8 devices in a mesh: dp: 1 (over z), cp: 8 (over y, x, core).
Axes of the slice: x: 2, y: 2, z: 1, core: 2. Of those that a mesh axis runs over, the one named last changes fastest.
Arguments:
- vis_feat: bfloat16 [8, 4096, 1152], P(('dp', 'cp'))
- text_emb: bfloat16 [4096, 3584], P(('dp', 'cp'))
- img_pos: int32 [8], P('dp')
- grad_y: bfloat16 [4096, 3584], P(('dp', 'cp'))
- pn_gain: bfloat16 [1152], replicated
- w_proj: bfloat16 [1152, 3584], replicated
- pre_gain: bfloat16 [3584], replicated
- w_query: bfloat16 [3584, 4096], replicated
- w_key: bfloat16 [3584, 2048], replicated
- w_value: bfloat16 [3584, 2048], replicated
- q_gain: bfloat16 [256], replicated
- k_gain: bfloat16 [256], replicated
- w_out: bfloat16 [4096, 3584], replicated
- post_gain: bfloat16 [3584], replicated
Outputs:
- output 1: bfloat16 [4096, 3584], P(('dp', 'cp'))
- output 2: bfloat16 [4096, 3584], P(('dp', 'cp'))
- output 3: bfloat16 [8, 4096, 1152], P(('dp', 'cp'))
- output 4: bfloat16 [1152], P('dp')
- output 5: bfloat16 [1152, 3584], P('dp')
- output 6: bfloat16 [3584], P('dp')
- output 7: bfloat16 [3584, 4096], P('dp')
- output 8: bfloat16 [3584, 2048], P('dp')
- output 9: bfloat16 [3584, 2048], P('dp')
- output 10: bfloat16 [256], P('dp')
- output 11: bfloat16 [256], P('dp')
- output 12: bfloat16 [4096, 3584], P('dp')
- output 13: bfloat16 [3584], P('dp')
All inputs are finite; a program needn't handle non-finite values.
Results may differ from the reference program's by a relative error of at most 0.02.
Values are sent between devices in bfloat16 or wider.
A program may use at most 1 GiB of HBM per device.

```python
import functools
import jax
import jax.numpy as jnp
from jax import lax

D = 3584
HEADS = 16
KV_HEADS = 8
HEAD = 256
DV = 1152
SEQ_DEV = 512
IMG_DEV = 1
GROUP = 8
GRID = 64
POOL = 4
SEQ = SEQ_DEV * GROUP
N_IMG = IMG_DEV * GROUP
SIDE = GRID // POOL
BLOCK = SIDE * SIDE
EPS = 1e-6
ROPE_BASE = 1000000.0
ROPE_SCALE = 8.0
NEG_BIG = -1e30


def place_images(rng_key):
    gap_key, perm_key = jax.random.split(rng_key)
    first_start = SEQ_DEV - BLOCK // 2
    spare = SEQ - N_IMG * BLOCK - first_start
    raw_gap = jax.random.randint(gap_key, (N_IMG,), 0, 8)
    weight = raw_gap * raw_gap * raw_gap
    gap_total = jnp.maximum(jnp.sum(weight), 1)
    gap_rows = spare * weight // gap_total
    slot_start = first_start + jnp.arange(N_IMG) * BLOCK + jnp.cumsum(gap_rows) - gap_rows
    slot_order = jax.random.permutation(perm_key, N_IMG)
    return slot_start[slot_order].astype(jnp.int32)


def draw_normal(rng_key, arr_shape, std_scale):
    return (jax.random.normal(rng_key, arr_shape, jnp.float32) * std_scale).astype(jnp.bfloat16)


def setup_inputs(seed: int = 0, part: int = 0) -> dict:
    base_key = jax.random.key(seed)
    part_keys = jax.random.split(jax.random.fold_in(base_key, part), 4)
    weight_keys = jax.random.split(jax.random.key(seed + 1), 10)
    return {
        'vis_feat': draw_normal(part_keys[0], (N_IMG, GRID * GRID, DV), 1.0),
        'text_emb': draw_normal(part_keys[1], (SEQ, D), 1.0),
        'img_pos': place_images(part_keys[2]),
        'grad_y': draw_normal(part_keys[3], (SEQ, D), 1.0),
        'pn_gain': draw_normal(weight_keys[0], (DV,), 0.3),
        'w_proj': draw_normal(weight_keys[1], (DV, D), DV ** -0.5),
        'pre_gain': draw_normal(weight_keys[2], (D,), 0.3),
        'w_query': draw_normal(weight_keys[3], (D, HEADS * HEAD), D ** -0.5),
        'w_key': draw_normal(weight_keys[4], (D, KV_HEADS * HEAD), D ** -0.5),
        'w_value': draw_normal(weight_keys[5], (D, KV_HEADS * HEAD), D ** -0.5),
        'q_gain': draw_normal(weight_keys[6], (HEAD,), 0.3),
        'k_gain': draw_normal(weight_keys[7], (HEAD,), 0.3),
        'w_out': draw_normal(weight_keys[8], (HEADS * HEAD, D), (HEADS * HEAD) ** -0.5),
        'post_gain': draw_normal(weight_keys[9], (D,), 0.3),
    }


def rms_scale(values, gain_vec):
    wide_vals = values.astype(jnp.float32)
    mean_sq = jnp.mean(wide_vals * wide_vals, axis=-1, keepdims=True)
    return wide_vals * lax.rsqrt(mean_sq + EPS) * (1.0 + gain_vec.astype(jnp.float32))


def rope_tables(positions):
    inv_freq = ROPE_BASE ** (-jnp.arange(0, HEAD, 2).astype(jnp.float32) / HEAD)
    rot_angle = (positions.astype(jnp.float32) / ROPE_SCALE)[:, None] * inv_freq[None, :]
    rot_angle = jnp.concatenate([rot_angle, rot_angle], axis=-1)
    return jnp.cos(rot_angle)[:, None, :], jnp.sin(rot_angle)[:, None, :]


def apply_rope(values, cos_t, sin_t):
    half_dim = values.shape[-1] // 2
    rotated = jnp.concatenate([-values[..., half_dim:], values[..., :half_dim]], axis=-1)
    return values * cos_t + rotated * sin_t


def project(vis_feat, pn_gain, w_proj):
    img_count = vis_feat.shape[0]
    patch_grid = vis_feat.reshape(img_count, SIDE, POOL, SIDE, POOL, DV).astype(jnp.float32)
    pooled = (jnp.sum(patch_grid, axis=(2, 4)) / (POOL * POOL)).astype(jnp.bfloat16)
    normed = rms_scale(pooled.reshape(img_count * BLOCK, DV), pn_gain).astype(jnp.bfloat16)
    return jnp.dot(normed, w_proj, preferred_element_type=jnp.float32).astype(jnp.bfloat16)


def attend_block(q_blk, start_blk, blk_index, k_heads, v_heads):
    groups = HEADS // KV_HEADS
    q_pos = blk_index * SEQ_DEV + jnp.arange(SEQ_DEV)
    key_pos = jnp.arange(SEQ)
    in_image = (start_blk[:, None] >= 0) & (key_pos[None, :] >= start_blk[:, None]) & (key_pos[None, :] < start_blk[:, None] + BLOCK)
    visible = (key_pos[None, :] <= q_pos[:, None]) | in_image
    q_grp = q_blk.reshape(SEQ_DEV, KV_HEADS, groups, HEAD).astype(jnp.float32)
    scores = jnp.einsum('qkgd,skd->kgqs', q_grp, k_heads.astype(jnp.float32)) * HEAD ** -0.5
    scores = jnp.where(visible[None, None], scores, NEG_BIG)
    prob_lo = jax.nn.softmax(scores, axis=-1).astype(jnp.bfloat16)
    attn_blk = jnp.einsum('kgqs,skd->qkgd', prob_lo.astype(jnp.float32), v_heads.astype(jnp.float32))
    return attn_blk.astype(jnp.bfloat16).reshape(SEQ_DEV, HEADS * HEAD)


def forward(vis_feat, text_emb, pn_gain, w_proj, pre_gain, w_query, w_key, w_value, q_gain, k_gain, w_out, post_gain, img_pos):
    soft_tok = project(vis_feat, pn_gain, w_proj)
    img_rows = (img_pos[:, None] + jnp.arange(BLOCK)[None, :]).reshape(-1)
    merged = text_emb.at[img_rows].set(soft_tok)
    starts = jnp.full((SEQ,), -1, jnp.int32).at[img_rows].set(jnp.repeat(img_pos, BLOCK))
    hidden = rms_scale(merged, pre_gain).astype(jnp.bfloat16)
    q_raw = jnp.dot(hidden, w_query, preferred_element_type=jnp.float32).astype(jnp.bfloat16).reshape(SEQ, HEADS, HEAD)
    k_raw = jnp.dot(hidden, w_key, preferred_element_type=jnp.float32).astype(jnp.bfloat16).reshape(SEQ, KV_HEADS, HEAD)
    v_heads = jnp.dot(hidden, w_value, preferred_element_type=jnp.float32).astype(jnp.bfloat16).reshape(SEQ, KV_HEADS, HEAD)
    cos_t, sin_t = rope_tables(jnp.arange(SEQ))
    q_heads = apply_rope(rms_scale(q_raw, q_gain), cos_t, sin_t).astype(jnp.bfloat16)
    k_heads = apply_rope(rms_scale(k_raw, k_gain), cos_t, sin_t).astype(jnp.bfloat16)
    block_fn = jax.checkpoint(attend_block)
    attn_out = lax.map(lambda blk_args: block_fn(blk_args[0], blk_args[1], blk_args[2], k_heads, v_heads), (q_heads.reshape(GROUP, SEQ_DEV, HEADS, HEAD), starts.reshape(GROUP, SEQ_DEV), jnp.arange(GROUP)))
    attn_out = attn_out.reshape(SEQ, HEADS * HEAD)
    proj_out = jnp.dot(attn_out, w_out, preferred_element_type=jnp.float32).astype(jnp.bfloat16)
    return (merged.astype(jnp.float32) + rms_scale(proj_out, post_gain)).astype(jnp.bfloat16)


def reference(vis_feat, text_emb, img_pos, grad_y, pn_gain, w_proj, pre_gain, w_query, w_key, w_value, q_gain, k_gain, w_out, post_gain):
    y_out, pullback = jax.vjp(functools.partial(forward, img_pos=img_pos), vis_feat, text_emb, pn_gain, w_proj, pre_gain, w_query, w_key, w_value, q_gain, k_gain, w_out, post_gain)
    grad_list = pullback(grad_y)
    return (y_out, grad_list[1], grad_list[0], grad_list[2], grad_list[3], grad_list[4], grad_list[5], grad_list[6], grad_list[7], grad_list[8], grad_list[9], grad_list[10], grad_list[11])
```

```python
import functools
import math
import jax
import jax.numpy as jnp
from jax import lax
from jax.experimental import pallas as pl
from jax.experimental.pallas import tpu as pltpu
from jax.sharding import PartitionSpec as P

GRID = 64
POOL = 4
SIDE = GRID // POOL
BLOCK = SIDE * SIDE
EPS = 1e-6
ROPE_BASE = 1000000.0
ROPE_SCALE = 8.0
NEG_BIG = -1e30
F32 = jnp.float32
BF16 = jnp.bfloat16
LOG2E = math.log2(math.e)


def rms_scale(values, gain_vec):
    wide_vals = values.astype(F32)
    mean_sq = jnp.mean(wide_vals * wide_vals, axis=-1, keepdims=True)
    return wide_vals * lax.rsqrt(mean_sq + EPS) * (1.0 + gain_vec)


def gain_norm(values, gain_vec):
    return rms_scale(values, gain_vec).astype(BF16)


def post_residual(merged, proj_out, gain_vec):
    return (merged.astype(F32) + rms_scale(proj_out, gain_vec)).astype(BF16)


def dot(a, b):
    return jnp.dot(a, b, preferred_element_type=F32)


def dot_nt(a, b):
    return lax.dot_general(a, b, (((1,), (1,)), ((), ())), preferred_element_type=F32)


def dot_tn(a, b):
    return lax.dot_general(a, b, (((0,), (0,)), ((), ())), preferred_element_type=F32)


def rope_tables(seq, head_dim):
    inv_freq = ROPE_BASE ** (-jnp.arange(0, head_dim, 2).astype(F32) / head_dim)
    rot_angle = (jnp.arange(seq).astype(F32) / ROPE_SCALE)[:, None] * inv_freq[None, :]
    return jnp.cos(rot_angle), jnp.sin(rot_angle)


def rope_fwd_kernel(hd, raw_ref, cos_ref, sin_ref, gq_ref, gk_ref, q_ref, k_ref, kt_ref):
    cos, sin = cos_ref[...], sin_ref[...]
    half = hd // 2
    n_q = q_ref.shape[1] // hd

    def one(col, gain):
        x = raw_ref[:, col:col + hd].astype(F32)
        r = lax.rsqrt(jnp.mean(x * x, axis=-1, keepdims=True) + EPS)
        x = x * r * (1.0 + gain)
        a, b = x[:, :half], x[:, half:]
        return (a * cos - b * sin), (b * cos + a * sin)

    for h in range(n_q):
        a, b = one(h * hd, gq_ref[...])
        q_ref[:, h * hd:h * hd + half] = a.astype(BF16)
        q_ref[:, h * hd + half:(h + 1) * hd] = b.astype(BF16)
    a, b = one(n_q * hd, gk_ref[...])
    k_ref[:, :half] = a.astype(BF16)
    k_ref[:, half:] = b.astype(BF16)
    kt_ref[:half, :] = a.T.astype(BF16)
    kt_ref[half:, :] = b.T.astype(BF16)


def rope_fwd(raw, cos, sin, gq, gk, hd, n_q):
    seq, width = raw.shape
    bm = 512
    row = lambda w: pl.BlockSpec((bm, w), lambda i: (i, 0))
    fix = pl.BlockSpec((1, hd), lambda i: (0, 0))
    return pl.pallas_call(
        functools.partial(rope_fwd_kernel, hd),
        grid=(seq // bm,),
        in_specs=[row(width), row(hd // 2), row(hd // 2), fix, fix],
        out_specs=[row(n_q * hd), row(hd), pl.BlockSpec((hd, bm), lambda i: (0, i))],
        out_shape=[jax.ShapeDtypeStruct((seq, n_q * hd), BF16), jax.ShapeDtypeStruct((seq, hd), BF16), jax.ShapeDtypeStruct((hd, seq), BF16)],
        cost_estimate=pl.CostEstimate(flops=20 * seq * width, bytes_accessed=4 * seq * width, transcendentals=0),
        name="rope_fwd",
    )(raw, cos, sin, gq, gk)


def rope_bwd_kernel(hd, raw_ref, dq_ref, dk_ref, dv_ref, cos_ref, sin_ref, gq_ref, gk_ref, out_ref, sq_ref, sk_ref):
    cos, sin = cos_ref[...], sin_ref[...]
    half = hd // 2
    n_q = dq_ref.shape[1] // hd

    @pl.when(pl.program_id(0) == 0)
    def _():
        sq_ref[...] = jnp.zeros_like(sq_ref)
        sk_ref[...] = jnp.zeros_like(sk_ref)

    def one(col, d_ref, dcol, gain, acc_ref):
        da = d_ref[:, dcol:dcol + half].astype(F32)
        db = d_ref[:, dcol + half:dcol + hd].astype(F32)
        d = jnp.concatenate([da * cos + db * sin, db * cos - da * sin], axis=1)
        x = raw_ref[:, col:col + hd].astype(F32)
        r = lax.rsqrt(jnp.mean(x * x, axis=-1, keepdims=True) + EPS)
        xr = x * r
        acc_ref[...] += jnp.sum(d * xr, axis=0, keepdims=True)
        gd = d * (1.0 + gain)
        dx = r * (gd - xr * jnp.mean(xr * gd, axis=-1, keepdims=True))
        out_ref[:, col:col + hd] = dx.astype(BF16)

    for h in range(n_q):
        one(h * hd, dq_ref, h * hd, gq_ref[...], sq_ref)
    one(n_q * hd, dk_ref, 0, gk_ref[...], sk_ref)
    out_ref[:, (n_q + 1) * hd:] = dv_ref[...]


def rope_bwd(raw, dq, dk, dv, cos, sin, gq, gk, hd, n_q):
    seq, width = raw.shape
    bm = 512
    row = lambda w: pl.BlockSpec((bm, w), lambda i: (i, 0))
    fix = pl.BlockSpec((1, hd), lambda i: (0, 0))
    return pl.pallas_call(
        functools.partial(rope_bwd_kernel, hd),
        grid=(seq // bm,),
        in_specs=[row(width), row(n_q * hd), row(hd), row(hd), row(hd // 2), row(hd // 2), fix, fix],
        out_specs=[row(width), fix, fix],
        out_shape=[jax.ShapeDtypeStruct((seq, width), BF16), jax.ShapeDtypeStruct((1, hd), F32), jax.ShapeDtypeStruct((1, hd), F32)],
        cost_estimate=pl.CostEstimate(flops=30 * seq * width, bytes_accessed=6 * seq * width, transcendentals=0),
        name="rope_bwd",
    )(raw, dq, dk, dv, cos, sin, gq, gk)


BQ = 256
KB = 512


def stack_heads(blk, hd):
    return jnp.concatenate([blk[:, h * hd:(h + 1) * hd] for h in range(blk.shape[1] // hd)], axis=0)


def fold_lanes(x, op):
    out = x[:, :128]
    for c in range(1, x.shape[1] // 128):
        out = op(out, x[:, c * 128:(c + 1) * 128])
    return out


def attn_fwd_kernel(hd, lim_ref, q_ref, kt_ref, v_ref, o_ref, o32_ref, lse_ref, s_ref):
    qb = pl.program_id(0)
    seq = kt_ref.shape[1]
    coef = hd ** -0.5 * LOG2E
    n_q = q_ref.shape[1] // hd
    rows = n_q * BQ
    q2 = stack_heads(q_ref[...], hd)
    lim = lim_ref[...]
    lim2 = jnp.concatenate([lim] * n_q, axis=0)
    n_full = (qb * BQ) // KB
    n_all = jnp.minimum((qb * BQ + BQ + BLOCK + KB - 1) // KB, seq // KB)

    def score(kb):
        cols = pl.ds(pl.multiple_of(kb * KB, KB), KB)
        return dot(q2, kt_ref[:, cols]), cols

    def full_body(kb, m):
        s, cols = score(kb)
        s_ref[:, cols] = s
        return jnp.maximum(m, fold_lanes(s, jnp.maximum))

    def mask_body(kb, m):
        s, cols = score(kb)
        key = kb * KB + lax.broadcasted_iota(jnp.int32, s.shape, 1)
        s = jnp.where(key <= lim2, s, NEG_BIG)
        s_ref[:, cols] = s
        return jnp.maximum(m, fold_lanes(s, jnp.maximum))

    m = lax.fori_loop(0, n_full, full_body, jnp.full((rows, 128), NEG_BIG, F32))
    m = lax.fori_loop(n_full, n_all, mask_body, m)
    m = jnp.max(m, axis=1, keepdims=True)

    def exp_body(kb, l):
        cols = pl.ds(pl.multiple_of(kb * KB, KB), KB)
        e = jnp.exp2((s_ref[:, cols] - m) * coef)
        s_ref[:, cols] = e
        return l + fold_lanes(e, jnp.add)

    l = lax.fori_loop(0, n_all, exp_body, jnp.zeros((rows, 128), F32))
    l = jnp.sum(l, axis=1, keepdims=True)
    inv = 1.0 / l

    def pv_body(kb, acc):
        cols = pl.ds(pl.multiple_of(kb * KB, KB), KB)
        p = (s_ref[:, cols] * inv).astype(BF16)
        return acc + dot(p, v_ref[cols, :])

    acc = lax.fori_loop(0, n_all, pv_body, jnp.zeros((rows, hd), F32))
    for h in range(n_q):
        part = acc[h * BQ:(h + 1) * BQ]
        o32_ref[:, h * hd:(h + 1) * hd] = part
        o_ref[:, h * hd:(h + 1) * hd] = part.astype(BF16)
    lse = jnp.broadcast_to(m * coef + jnp.log2(l), (rows, 128))
    lse_ref[0] = lse.T[:8, :]


def attn_fwd(lim, q, kt, raw, hd):
    seq, width = q.shape
    n_q = width // hd
    v_col = raw.shape[1] // hd - 1
    row = lambda w: pl.BlockSpec((BQ, w), lambda i: (i, 0))
    return pl.pallas_call(
        functools.partial(attn_fwd_kernel, hd),
        grid=(seq // BQ,),
        in_specs=[row(1), row(width), pl.BlockSpec((hd, seq), lambda i: (0, 0)), pl.BlockSpec((seq, hd), lambda i: (0, v_col))],
        out_specs=[row(width), row(width), pl.BlockSpec((1, 8, n_q * BQ), lambda i: (i, 0, 0))],
        out_shape=[jax.ShapeDtypeStruct((seq, width), BF16), jax.ShapeDtypeStruct((seq, width), F32), jax.ShapeDtypeStruct((seq // BQ, 8, n_q * BQ), F32)],
        scratch_shapes=[pltpu.VMEM((n_q * BQ, seq), F32)],
        cost_estimate=pl.CostEstimate(flops=int(2.2 * seq * seq * width), bytes_accessed=8 * seq * width, transcendentals=seq * seq),
        compiler_params=pltpu.CompilerParams(vmem_limit_bytes=40 * 1024 * 1024),
        name="attn_fwd",
    )(lim, q, kt, raw)


def attn_bwd_kernel(hd, lim_ref, q_ref, k_ref, kt_ref, v_ref, do_ref, o32_ref, lse_ref, dq_ref, dk_ref, dv_ref, dk_acc, dv_acc):
    qb = pl.program_id(0)
    seq = kt_ref.shape[1]
    scale = hd ** -0.5
    coef = scale * LOG2E
    n_q = q_ref.shape[1] // hd
    rows = n_q * BQ

    @pl.when(qb == 0)
    def _():
        dk_acc[...] = jnp.zeros_like(dk_acc)
        dv_acc[...] = jnp.zeros_like(dv_acc)

    q2 = stack_heads(q_ref[...], hd)
    do2 = stack_heads(do_ref[...], hd)
    o2 = stack_heads(o32_ref[...], hd)
    qt = q2.T
    dot_ = do2.T
    delta = jnp.sum(fold_lanes(do2.astype(F32) * o2, jnp.add).T, axis=0, keepdims=True)
    lse = lse_ref[0][0:1, :]
    lim = lim_ref[0]
    lim2 = jnp.concatenate([lim] * n_q, axis=1)
    n_full = (qb * BQ) // KB
    n_all = jnp.minimum((qb * BQ + BQ + BLOCK + KB - 1) // KB, seq // KB)

    def body(masked, kb, dqt):
        cols = pl.ds(pl.multiple_of(kb * KB, KB), KB)
        st = dot(k_ref[cols, :], qt)
        pt = jnp.exp2(st * coef - lse)
        if masked:
            key = kb * KB + lax.broadcasted_iota(jnp.int32, st.shape, 0)
            pt = jnp.where(key <= lim2, pt, 0.0)
        dpt = dot(v_ref[cols, :], dot_)
        dst = (pt * (dpt - delta) * scale).astype(BF16)
        dv_acc[cols, :] += dot(pt.astype(BF16), do2)
        dk_acc[cols, :] += dot(dst, q2)
        return dqt + dot(kt_ref[:, cols], dst)

    dqt = lax.fori_loop(0, n_full, functools.partial(body, False), jnp.zeros((hd, rows), F32))
    dqt = lax.fori_loop(n_full, n_all, functools.partial(body, True), dqt)
    dq = dqt.T.astype(BF16)
    for h in range(n_q):
        dq_ref[:, h * hd:(h + 1) * hd] = dq[h * BQ:(h + 1) * BQ]

    @pl.when(qb == pl.num_programs(0) - 1)
    def _():
        dk_ref[...] = dk_acc[...].astype(BF16)
        dv_ref[...] = dv_acc[...].astype(BF16)


def attn_bwd(lim_row, q, k, kt, raw, d_o, o32, lse, hd):
    seq, width = q.shape
    n_q = width // hd
    v_col = raw.shape[1] // hd - 1
    row = lambda w: pl.BlockSpec((BQ, w), lambda i: (i, 0))
    whole = pl.BlockSpec((seq, hd), lambda i: (0, 0))
    return pl.pallas_call(
        functools.partial(attn_bwd_kernel, hd),
        grid=(seq // BQ,),
        in_specs=[pl.BlockSpec((1, 1, BQ), lambda i: (i, 0, 0)), row(width), whole, pl.BlockSpec((hd, seq), lambda i: (0, 0)),
                  pl.BlockSpec((seq, hd), lambda i: (0, v_col)), row(width), row(width), pl.BlockSpec((1, 8, n_q * BQ), lambda i: (i, 0, 0))],
        out_specs=[row(width), whole, whole],
        out_shape=[jax.ShapeDtypeStruct((seq, width), BF16), jax.ShapeDtypeStruct((seq, hd), BF16), jax.ShapeDtypeStruct((seq, hd), BF16)],
        scratch_shapes=[pltpu.VMEM((seq, hd), F32), pltpu.VMEM((seq, hd), F32)],
        cost_estimate=pl.CostEstimate(flops=int(5.5 * seq * seq * width), bytes_accessed=12 * seq * width, transcendentals=seq * seq),
        compiler_params=pltpu.CompilerParams(vmem_limit_bytes=48 * 1024 * 1024),
        name="attn_bwd",
    )(lim_row, q, k, kt, raw, d_o, o32, lse)


def solution(mesh):
    n_dev = mesh.shape['cp']
    seq_spec = P(('dp', 'cp'))
    part_spec = P('dp')
    rep_spec = P()

    def gather_rows(x):
        return lax.all_gather(x, 'cp', tiled=True)

    def to_seq(x):
        return lax.all_to_all(x, 'cp', split_axis=0, concat_axis=1, tiled=True)

    def to_heads(x):
        return lax.all_to_all(x, 'cp', split_axis=1, concat_axis=0, tiled=True)

    def device_body(vis_loc, text_loc, img_pos, grad_y, pn_gain, w_proj, pre_gain, w_query, w_key, w_value, q_gain, k_gain, w_out, post_gain):
        rank = lax.axis_index('cp')
        seq_loc, d_model = text_loc.shape
        seq = seq_loc * n_dev
        img_loc, patches, dim_v = vis_loc.shape
        n_img = img_pos.shape[0]
        hd = q_gain.shape[0]
        wq_loc = w_query.shape[1] // n_dev
        wk_loc = w_key.shape[1] // n_dev
        n_q = wq_loc // hd
        pn32, pre32, post32 = pn_gain.astype(F32), pre_gain.astype(F32), post_gain.astype(F32)
        gq32 = q_gain.astype(F32)[None, :]
        gk32 = k_gain.astype(F32)[None, :]

        patch = jnp.arange(patches)
        patch_cell = (patch // (GRID * POOL)) * SIDE + (patch % GRID) // POOL
        pool_mat = (jnp.arange(BLOCK)[:, None] == patch_cell[None, :]).astype(BF16)
        pooled = jnp.einsum('cp,npd->ncd', pool_mat, vis_loc, preferred_element_type=F32) / (POOL * POOL)
        pooled = pooled.astype(BF16).reshape(img_loc * BLOCK, dim_v)
        normed, norm_pull = jax.vjp(gain_norm, pooled, pn32)
        normed_all = gather_rows(normed)

        q_pos = rank * seq_loc + jnp.arange(seq_loc)
        offset = q_pos[:, None] - img_pos[None, :]
        in_blk = (offset >= 0) & (offset < BLOCK)
        is_img = jnp.any(in_blk, axis=1)
        img_mask = is_img[:, None]
        flat_row = jnp.sum(jnp.where(in_blk, jnp.arange(n_img)[None, :] * BLOCK + offset, 0), axis=1)
        flat_row = jnp.where(is_img, flat_row, -1)
        select = (flat_row[:, None] == jnp.arange(n_img * BLOCK)[None, :]).astype(BF16)
        all_pos = jnp.arange(seq)
        all_off = all_pos[:, None] - img_pos[None, :]
        all_in = (all_off >= 0) & (all_off < BLOCK)
        limit = all_pos + jnp.sum(jnp.where(all_in, BLOCK - 1 - all_off, 0), axis=1)

        normed_rows = dot(select, normed_all).astype(BF16)
        soft_rows = dot(normed_rows, w_proj).astype(BF16)
        merged = jnp.where(img_mask, soft_rows, text_loc)
        hidden, pre_pull = jax.vjp(gain_norm, merged, pre32)
        hidden_all = gather_rows(hidden)

        w_qkv = jnp.concatenate([
            lax.dynamic_slice_in_dim(w_query, rank * wq_loc, wq_loc, 1),
            lax.dynamic_slice_in_dim(w_key, rank * wk_loc, wk_loc, 1),
            lax.dynamic_slice_in_dim(w_value, rank * wk_loc, wk_loc, 1)], axis=1)
        raw = dot(hidden_all, w_qkv).astype(BF16)
        cos_t, sin_t = rope_tables(seq, hd)
        q, k, kt = rope_fwd(raw, cos_t, sin_t, gq32, gk32, hd, n_q)
        o, o32, lse = attn_fwd(limit[:, None].astype(jnp.int32), q, kt, raw, hd)

        attn_seq = to_seq(o)
        proj_out = dot(attn_seq, w_out).astype(BF16)
        y_loc, post_pull = jax.vjp(post_residual, merged, proj_out, post32)
        d_resid, d_proj, g_post = post_pull(grad_y)
        d_attn = dot_nt(d_proj, w_out).astype(BF16)
        d_o = to_heads(d_attn)
        d_proj_all = gather_rows(d_proj)

        dq, dk, dv = attn_bwd(limit.astype(jnp.int32).reshape(seq // BQ, 1, BQ), q, k, kt, raw, d_o, o32, lse, hd)
        d_qkv, g_q_gain, g_k_gain = rope_bwd(raw, dq, dk, dv, cos_t, sin_t, gq32, gk32, hd, n_q)

        dq_seq = to_seq(d_qkv[:, :wq_loc])
        dk_seq = to_seq(d_qkv[:, wq_loc:wq_loc + wk_loc])
        dv_seq = to_seq(d_qkv[:, wq_loc + wk_loc:])
        d_hidden = dot_nt(dq_seq, w_query) + dot_nt(dk_seq, w_key)
        d_hidden = (d_hidden + dot_nt(dv_seq, w_value)).astype(BF16)
        d_merged_attn, g_pre = pre_pull(d_hidden)
        d_merged = (d_resid.astype(F32) + d_merged_attn.astype(F32)).astype(BF16)
        grad_text = jnp.where(img_mask, 0.0, d_merged).astype(BF16)

        d_soft_rows = jnp.where(img_mask, d_merged, 0.0).astype(BF16)
        d_normed_rows = dot_nt(d_soft_rows, w_proj).astype(BF16)
        d_normed_all = dot_tn(select, d_normed_rows).astype(BF16)
        d_normed = lax.psum_scatter(d_normed_all, 'cp', scatter_dimension=0, tiled=True)
        d_pooled, g_pn = norm_pull(d_normed)
        spread = (d_pooled.astype(F32) / (POOL * POOL)).astype(BF16).reshape(img_loc, SIDE, 1, SIDE, 1, dim_v)
        grad_vis = jnp.broadcast_to(spread, (img_loc, SIDE, POOL, SIDE, POOL, dim_v)).reshape(img_loc, patches, dim_v)

        g_proj_part = dot_tn(normed_rows, d_soft_rows)
        g_proj = gather_rows(lax.psum_scatter(g_proj_part, 'cp', scatter_dimension=0, tiled=True).astype(BF16))

        g_out = gather_rows(dot_tn(o, d_proj_all).astype(BF16))
        g_query = lax.all_gather(dot_tn(hidden_all, d_qkv[:, :wq_loc]).astype(BF16), 'cp', axis=1, tiled=True)
        g_key = lax.all_gather(dot_tn(hidden_all, d_qkv[:, wq_loc:wq_loc + wk_loc]).astype(BF16), 'cp', axis=1, tiled=True)
        g_value = lax.all_gather(dot_tn(hidden_all, d_qkv[:, wq_loc + wk_loc:]).astype(BF16), 'cp', axis=1, tiled=True)
        small = lax.psum((g_pn, g_pre, g_q_gain[0], g_k_gain[0], g_post), 'cp')
        g_pn, g_pre, g_q_gain, g_k_gain, g_post = [part.astype(BF16) for part in small]
        return (y_loc, grad_text, grad_vis, g_pn, g_proj, g_pre, g_query, g_key, g_value, g_q_gain, g_k_gain, g_out, g_post)

    in_specs = (seq_spec, seq_spec, part_spec, seq_spec) + (rep_spec,) * 10
    out_specs = (seq_spec, seq_spec, seq_spec) + (part_spec,) * 10
    return jax.shard_map(device_body, mesh=mesh, in_specs=in_specs, out_specs=out_specs, check_vma=False)
```

```python
import functools
import math
import jax
import jax.numpy as jnp
from jax import lax
from jax.experimental import pallas as pl
from jax.experimental.pallas import tpu as pltpu
from jax.sharding import PartitionSpec as P

GRID = 64
POOL = 4
SIDE = GRID // POOL
BLOCK = SIDE * SIDE
EPS = 1e-6
ROPE_BASE = 1000000.0
ROPE_SCALE = 8.0
NEG_BIG = -1e30
F32 = jnp.float32
BF16 = jnp.bfloat16
LOG2E = math.log2(math.e)


def rms_scale(values, gain_vec):
    wide_vals = values.astype(F32)
    mean_sq = jnp.mean(wide_vals * wide_vals, axis=-1, keepdims=True)
    return wide_vals * lax.rsqrt(mean_sq + EPS) * (1.0 + gain_vec)


def gain_norm(values, gain_vec):
    return rms_scale(values, gain_vec).astype(BF16)


def post_residual(merged, proj_out, gain_vec):
    return (merged.astype(F32) + rms_scale(proj_out, gain_vec)).astype(BF16)


def dot(a, b):
    return jnp.dot(a, b, preferred_element_type=F32)


def dot_nt(a, b):
    return lax.dot_general(a, b, (((1,), (1,)), ((), ())), preferred_element_type=F32)


def dot_tn(a, b):
    return lax.dot_general(a, b, (((0,), (0,)), ((), ())), preferred_element_type=F32)


def rope_tables(seq, head_dim):
    inv_freq = ROPE_BASE ** (-jnp.arange(0, head_dim, 2).astype(F32) / head_dim)
    rot_angle = (jnp.arange(seq).astype(F32) / ROPE_SCALE)[:, None] * inv_freq[None, :]
    return jnp.cos(rot_angle), jnp.sin(rot_angle)


def rope_fwd_kernel(hd, raw_ref, cos_ref, sin_ref, gq_ref, gk_ref, q_ref, k_ref, kt_ref, vt_ref):
    cos, sin = cos_ref[...], sin_ref[...]
    half = hd // 2
    n_q = q_ref.shape[1] // hd

    def one(col, gain):
        x = raw_ref[:, col:col + hd].astype(F32)
        r = lax.rsqrt(jnp.mean(x * x, axis=-1, keepdims=True) + EPS)
        x = x * r * (1.0 + gain)
        a, b = x[:, :half], x[:, half:]
        return (a * cos - b * sin), (b * cos + a * sin)

    for h in range(n_q):
        a, b = one(h * hd, gq_ref[...])
        q_ref[:, h * hd:h * hd + half] = a.astype(BF16)
        q_ref[:, h * hd + half:(h + 1) * hd] = b.astype(BF16)
    a, b = one(n_q * hd, gk_ref[...])
    k_ref[:, :half] = a.astype(BF16)
    k_ref[:, half:] = b.astype(BF16)
    kt_ref[:half, :] = a.T.astype(BF16)
    kt_ref[half:, :] = b.T.astype(BF16)
    vt_ref[...] = raw_ref[:, (n_q + 1) * hd:].T


def rope_fwd(raw, cos, sin, gq, gk, hd, n_q):
    seq, width = raw.shape
    bm = 512
    row = lambda w: pl.BlockSpec((bm, w), lambda i: (i, 0))
    fix = pl.BlockSpec((1, hd), lambda i: (0, 0))
    return pl.pallas_call(
        functools.partial(rope_fwd_kernel, hd),
        grid=(seq // bm,),
        in_specs=[row(width), row(hd // 2), row(hd // 2), fix, fix],
        out_specs=[row(n_q * hd), row(hd), pl.BlockSpec((hd, bm), lambda i: (0, i)), pl.BlockSpec((hd, bm), lambda i: (0, i))],
        out_shape=[jax.ShapeDtypeStruct((seq, n_q * hd), BF16), jax.ShapeDtypeStruct((seq, hd), BF16)] + [jax.ShapeDtypeStruct((hd, seq), BF16)] * 2,
        cost_estimate=pl.CostEstimate(flops=20 * seq * width, bytes_accessed=4 * seq * width, transcendentals=0),
        name="rope_fwd",
    )(raw, cos, sin, gq, gk)


def rope_bwd_kernel(hd, raw_ref, dq_ref, dk_ref, dv_ref, cos_ref, sin_ref, gq_ref, gk_ref, out_ref, qt_ref, kt_ref, vt_ref, sq_ref, sk_ref):
    cos, sin = cos_ref[...], sin_ref[...]
    half = hd // 2
    n_q = dq_ref.shape[1] // hd

    @pl.when(pl.program_id(0) == 0)
    def _():
        sq_ref[...] = jnp.zeros_like(sq_ref)
        sk_ref[...] = jnp.zeros_like(sk_ref)

    def one(col, d_ref, dcol, gain, acc_ref, t_ref):
        da = d_ref[:, dcol:dcol + half].astype(F32)
        db = d_ref[:, dcol + half:dcol + hd].astype(F32)
        d = jnp.concatenate([da * cos + db * sin, db * cos - da * sin], axis=1)
        x = raw_ref[:, col:col + hd].astype(F32)
        r = lax.rsqrt(jnp.mean(x * x, axis=-1, keepdims=True) + EPS)
        xr = x * r
        acc_ref[...] += jnp.sum(d * xr, axis=0, keepdims=True)
        gd = d * (1.0 + gain)
        dx = r * (gd - xr * jnp.mean(xr * gd, axis=-1, keepdims=True))
        dx = dx.astype(BF16)
        out_ref[:, col:col + hd] = dx
        t_ref[0, dcol:dcol + hd, :] = dx.T

    for h in range(n_q):
        one(h * hd, dq_ref, h * hd, gq_ref[...], sq_ref, qt_ref)
    one(n_q * hd, dk_ref, 0, gk_ref[...], sk_ref, kt_ref)
    out_ref[:, (n_q + 1) * hd:] = dv_ref[...]
    vt_ref[0] = dv_ref[...].T


def rope_bwd(raw, dq, dk, dv, cos, sin, gq, gk, hd, n_q, bm):
    seq, width = raw.shape
    tall = lambda w: pl.BlockSpec((1, w, bm), lambda i: (i, 0, 0))
    tshape = lambda w: jax.ShapeDtypeStruct((seq // bm, w, bm), BF16)
    row = lambda w: pl.BlockSpec((bm, w), lambda i: (i, 0))
    fix = pl.BlockSpec((1, hd), lambda i: (0, 0))
    return pl.pallas_call(
        functools.partial(rope_bwd_kernel, hd),
        grid=(seq // bm,),
        in_specs=[row(width), row(n_q * hd), row(hd), row(hd), row(hd // 2), row(hd // 2), fix, fix],
        out_specs=[row(width), tall(n_q * hd), tall(hd), tall(hd), fix, fix],
        out_shape=[jax.ShapeDtypeStruct((seq, width), BF16), tshape(n_q * hd), tshape(hd), tshape(hd), jax.ShapeDtypeStruct((1, hd), F32), jax.ShapeDtypeStruct((1, hd), F32)],
        cost_estimate=pl.CostEstimate(flops=30 * seq * width, bytes_accessed=6 * seq * width, transcendentals=0),
        name="rope_bwd",
    )(raw, dq, dk, dv, cos, sin, gq, gk)


BQ = 256
KB = 512


def stack_heads(blk, hd):
    return jnp.concatenate([blk[:, h * hd:(h + 1) * hd] for h in range(blk.shape[1] // hd)], axis=0)


def fold_rows(x, op):
    out = x[:8]
    for c in range(1, x.shape[0] // 8):
        out = op(out, x[c * 8:(c + 1) * 8])
    return out


def wide(blk, hd):
    return jnp.concatenate([blk[h * hd:(h + 1) * hd] for h in range(blk.shape[0] // hd)], axis=1)


def attn_fwd_kernel(hd, nkb_ref, lim_ref, q_ref, k_ref, vt_ref, o_ref, o32_ref, lse_ref, s_ref):
    qb = pl.program_id(0)
    coef = hd ** -0.5 * LOG2E
    n_q = q_ref.shape[1] // hd
    rows = n_q * BQ
    qt = stack_heads(q_ref[...], hd).T
    lim2 = jnp.concatenate([lim_ref[0]] * n_q, axis=1)
    n_full = (qb * BQ) // KB
    n_all = nkb_ref[qb]

    def score(kb):
        keys = pl.ds(pl.multiple_of(kb * KB, KB), KB)
        return dot(k_ref[keys, :], qt), keys

    def full_body(kb, m):
        s, keys = score(kb)
        s_ref[keys, :] = s
        return jnp.maximum(m, fold_rows(s, jnp.maximum))

    def mask_body(kb, m):
        s, keys = score(kb)
        key = kb * KB + lax.broadcasted_iota(jnp.int32, s.shape, 0)
        s = jnp.where(key <= lim2, s, NEG_BIG)
        s_ref[keys, :] = s
        return jnp.maximum(m, fold_rows(s, jnp.maximum))

    m = lax.fori_loop(0, n_full, full_body, jnp.full((8, rows), NEG_BIG, F32))
    m = lax.fori_loop(n_full, n_all, mask_body, m)
    m = jnp.max(m, axis=0, keepdims=True)

    def exp_body(kb, l):
        keys = pl.ds(pl.multiple_of(kb * KB, KB), KB)
        e = jnp.exp2((s_ref[keys, :] - m) * coef)
        s_ref[keys, :] = e
        return l + fold_rows(e, jnp.add)

    l = lax.fori_loop(0, n_all, exp_body, jnp.zeros((8, rows), F32))
    l = jnp.sum(l, axis=0, keepdims=True)
    inv = 1.0 / l

    def pv_body(kb, acc):
        keys = pl.ds(pl.multiple_of(kb * KB, KB), KB)
        p = (s_ref[keys, :] * inv).astype(BF16)
        return acc + dot(vt_ref[:, keys], p)

    acc = lax.fori_loop(0, n_all, pv_body, jnp.zeros((hd, rows), F32))
    for h in range(n_q):
        part = acc[:, h * BQ:(h + 1) * BQ]
        o32_ref[0, h * hd:(h + 1) * hd, :] = part
        o_ref[0, h * hd:(h + 1) * hd, :] = part.astype(BF16)
    lse_ref[0] = jnp.broadcast_to(m * coef + jnp.log2(l), (8, rows))


def attn_fwd(nkb, lim, q, k, vt, hd, seq_loc):
    seq, width = q.shape
    n_q = width // hd
    per = seq_loc // BQ
    tall = pl.BlockSpec((1, width, BQ), lambda i, *_: (i // per, 0, i % per))
    return pl.pallas_call(
        functools.partial(attn_fwd_kernel, hd),
        grid_spec=pltpu.PrefetchScalarGridSpec(
            num_scalar_prefetch=1,
            grid=(seq // BQ,),
            in_specs=[pl.BlockSpec((1, 1, BQ), lambda i, *_: (i, 0, 0)), pl.BlockSpec((BQ, width), lambda i, *_: (i, 0)),
                      pl.BlockSpec((seq, hd), lambda i, *_: (0, 0)), pl.BlockSpec((hd, seq), lambda i, *_: (0, 0))],
            out_specs=[tall, tall, pl.BlockSpec((1, 8, n_q * BQ), lambda i, *_: (i, 0, 0))],
            scratch_shapes=[pltpu.VMEM((seq, n_q * BQ), F32)]),
        out_shape=[jax.ShapeDtypeStruct((seq // seq_loc, width, seq_loc), BF16), jax.ShapeDtypeStruct((seq // seq_loc, width, seq_loc), F32),
                   jax.ShapeDtypeStruct((seq // BQ, 8, n_q * BQ), F32)],
        cost_estimate=pl.CostEstimate(flops=int(2.2 * seq * seq * width), bytes_accessed=8 * seq * width, transcendentals=seq * seq),
        compiler_params=pltpu.CompilerParams(vmem_limit_bytes=40 * 1024 * 1024),
        name="attn_fwd",
    )(nkb, lim, q, k, vt)


def attn_bwd_kernel(hd, nkb_ref, lim_ref, q_ref, k_ref, kt_ref, v_ref, do_ref, o32_ref, lse_ref, dq_ref, dk_ref, dv_ref, dk_acc, dv_acc):
    qb = pl.program_id(0)
    scale = hd ** -0.5
    coef = scale * LOG2E
    n_q = q_ref.shape[1] // hd
    rows = n_q * BQ

    @pl.when(qb == 0)
    def _():
        dk_acc[...] = jnp.zeros_like(dk_acc)
        dv_acc[...] = jnp.zeros_like(dv_acc)

    q2 = stack_heads(q_ref[...], hd)
    qt = q2.T
    dot_ = wide(do_ref[0], hd)
    do2 = dot_.T
    delta = jnp.sum(dot_.astype(F32) * wide(o32_ref[0], hd), axis=0, keepdims=True)
    lse = lse_ref[0][0:1, :]
    lim2 = jnp.concatenate([lim_ref[0]] * n_q, axis=1)
    n_full = (qb * BQ) // KB
    n_all = nkb_ref[qb]

    def body(masked, kb, dqt):
        keys = pl.ds(pl.multiple_of(kb * KB, KB), KB)
        st = dot(k_ref[keys, :], qt)
        pt = jnp.exp2(st * coef - lse)
        if masked:
            key = kb * KB + lax.broadcasted_iota(jnp.int32, st.shape, 0)
            pt = jnp.where(key <= lim2, pt, 0.0)
        dpt = dot(v_ref[keys, :], dot_)
        dst = (pt * (dpt - delta) * scale).astype(BF16)
        dv_acc[keys, :] += dot(pt.astype(BF16), do2)
        dk_acc[keys, :] += dot(dst, q2)
        return dqt + dot(kt_ref[:, keys], dst)

    dqt = lax.fori_loop(0, n_full, functools.partial(body, False), jnp.zeros((hd, rows), F32))
    dqt = lax.fori_loop(n_full, n_all, functools.partial(body, True), dqt)
    dq = dqt.T.astype(BF16)
    for h in range(n_q):
        dq_ref[:, h * hd:(h + 1) * hd] = dq[h * BQ:(h + 1) * BQ]

    @pl.when(qb == pl.num_programs(0) - 1)
    def _():
        dk_ref[...] = dk_acc[...].astype(BF16)
        dv_ref[...] = dv_acc[...].astype(BF16)


def attn_bwd(nkb, lim, q, k, kt, raw, d_o, o32, lse, hd):
    seq, width = q.shape
    n_q = width // hd
    v_col = raw.shape[1] // hd - 1
    per = d_o.shape[2] // BQ
    row = lambda w: pl.BlockSpec((BQ, w), lambda i, *_: (i, 0))
    tall = pl.BlockSpec((1, width, BQ), lambda i, *_: (i // per, 0, i % per))
    whole = pl.BlockSpec((seq, hd), lambda i, *_: (0, 0))
    return pl.pallas_call(
        functools.partial(attn_bwd_kernel, hd),
        grid_spec=pltpu.PrefetchScalarGridSpec(
            num_scalar_prefetch=1,
            grid=(seq // BQ,),
            in_specs=[pl.BlockSpec((1, 1, BQ), lambda i, *_: (i, 0, 0)), row(width), whole, pl.BlockSpec((hd, seq), lambda i, *_: (0, 0)),
                      pl.BlockSpec((seq, hd), lambda i, *_: (0, v_col)), tall, tall, pl.BlockSpec((1, 8, n_q * BQ), lambda i, *_: (i, 0, 0))],
            out_specs=[row(width), whole, whole],
            scratch_shapes=[pltpu.VMEM((seq, hd), F32), pltpu.VMEM((seq, hd), F32)]),
        out_shape=[jax.ShapeDtypeStruct((seq, width), BF16), jax.ShapeDtypeStruct((seq, hd), BF16), jax.ShapeDtypeStruct((seq, hd), BF16)],
        cost_estimate=pl.CostEstimate(flops=int(5.5 * seq * seq * width), bytes_accessed=12 * seq * width, transcendentals=seq * seq),
        compiler_params=pltpu.CompilerParams(vmem_limit_bytes=48 * 1024 * 1024),
        name="attn_bwd",
    )(nkb, lim, q, k, kt, raw, d_o, o32, lse)


def copy_kernel(x_ref, o_ref):
    o_ref[...] = x_ref[...]


def copy_out(x, cols):
    rows = x.shape[0]
    bm = 128
    spec = pl.BlockSpec((bm, cols), lambda i: (i, 0))
    return pl.pallas_call(
        copy_kernel,
        grid=(rows // bm,),
        in_specs=[spec],
        out_specs=spec,
        out_shape=jax.ShapeDtypeStruct((rows, cols), x.dtype),
        cost_estimate=pl.CostEstimate(flops=rows * cols, bytes_accessed=4 * rows * cols, transcendentals=0),
        name="copy_out",
    )(x)


def solution(mesh):
    n_dev = mesh.shape['cp']
    seq_spec = P(('dp', 'cp'))
    part_spec = P('dp')
    rep_spec = P()

    def gather(x, axis=0):
        return lax.all_gather(x, 'cp', axis=axis, tiled=True)

    def exchange(x):
        return lax.all_to_all(x, 'cp', split_axis=0, concat_axis=0, tiled=True)

    def device_step(vis_loc, text_loc, img_pos, grad_y, pn_gain, w_proj, pre_gain, w_query, w_key, w_value, q_gain, k_gain, w_out, post_gain):
        rank = lax.axis_index('cp')
        seq_loc, d_model = text_loc.shape
        seq = seq_loc * n_dev
        img_loc, patches, dim_v = vis_loc.shape
        n_img = img_pos.shape[0]
        hd = q_gain.shape[0]
        wq_loc = w_query.shape[1] // n_dev
        wk_loc = w_key.shape[1] // n_dev
        n_q = wq_loc // hd
        pn32, pre32, post32 = pn_gain.astype(F32), pre_gain.astype(F32), post_gain.astype(F32)
        gq32 = q_gain.astype(F32)[None, :]
        gk32 = k_gain.astype(F32)[None, :]

        patch = jnp.arange(patches)
        patch_cell = (patch // (GRID * POOL)) * SIDE + (patch % GRID) // POOL
        pool_mat = (jnp.arange(BLOCK)[:, None] == patch_cell[None, :]).astype(BF16)
        pooled = jnp.einsum('cp,npd->ncd', pool_mat, vis_loc, preferred_element_type=F32) / (POOL * POOL)
        pooled = pooled.astype(BF16).reshape(img_loc * BLOCK, dim_v)
        normed, norm_pull = jax.vjp(gain_norm, pooled, pn32)
        normed_all = gather(normed)

        q_pos = rank * seq_loc + jnp.arange(seq_loc)
        offset = q_pos[:, None] - img_pos[None, :]
        in_blk = (offset >= 0) & (offset < BLOCK)
        is_img = jnp.any(in_blk, axis=1)
        img_mask = is_img[:, None]
        flat_row = jnp.sum(jnp.where(in_blk, jnp.arange(n_img)[None, :] * BLOCK + offset, 0), axis=1)
        flat_row = jnp.where(is_img, flat_row, -1)
        select = (flat_row[:, None] == jnp.arange(n_img * BLOCK)[None, :]).astype(BF16)
        all_pos = jnp.arange(seq)
        all_off = all_pos[:, None] - img_pos[None, :]
        all_in = (all_off >= 0) & (all_off < BLOCK)
        limit = (all_pos + jnp.sum(jnp.where(all_in, BLOCK - 1 - all_off, 0), axis=1)).astype(jnp.int32).reshape(seq // BQ, 1, BQ)
        n_kb = (jnp.max(limit, axis=(1, 2)) // KB + 1).astype(jnp.int32)
        all_flat = jnp.sum(jnp.where(all_in, jnp.arange(n_img)[None, :] * BLOCK + all_off + 1, 0), axis=1) - 1
        select_all = (all_flat[:, None] == jnp.arange(n_img * BLOCK)[None, :]).astype(BF16)

        normed_rows = dot(select, normed_all).astype(BF16)
        soft_rows = dot(normed_rows, w_proj).astype(BF16)
        merged = jnp.where(img_mask, soft_rows, text_loc)
        hidden, pre_pull = jax.vjp(gain_norm, merged, pre32)
        hidden_all = gather(hidden)

        w_qkv = jnp.concatenate([
            lax.dynamic_slice_in_dim(w_query, rank * wq_loc, wq_loc, 1),
            lax.dynamic_slice_in_dim(w_key, rank * wk_loc, wk_loc, 1),
            lax.dynamic_slice_in_dim(w_value, rank * wk_loc, wk_loc, 1)], axis=1)
        raw = dot(hidden_all, w_qkv).astype(BF16)
        cos_t, sin_t = rope_tables(seq, hd)
        q, k, kt, vt = rope_fwd(raw, cos_t, sin_t, gq32, gk32, hd, n_q)
        o_t, o32_t, lse = attn_fwd(n_kb, limit, q, k, vt, hd, seq_loc)

        attn_t = exchange(o_t).reshape(n_dev * wq_loc, seq_loc)
        proj_out = dot_tn(attn_t, w_out).astype(BF16)
        y_loc, post_pull = jax.vjp(post_residual, merged, proj_out, post32)
        d_resid, d_proj, g_post = post_pull(grad_y)
        d_attn_t = dot_nt(w_out, d_proj).astype(BF16).reshape(n_dev, wq_loc, seq_loc)
        d_o = exchange(d_attn_t)
        d_proj_all = gather(d_proj)

        dq, dk, dv = attn_bwd(n_kb, limit, q, k, kt, raw, d_o, o32_t, lse, hd)
        d_qkv, dq_t, dk_t, dv_t, g_q_gain, g_k_gain = rope_bwd(raw, dq, dk, dv, cos_t, sin_t, gq32, gk32, hd, n_q, seq_loc)

        dk_seq = exchange(dk_t).reshape(-1, seq_loc)
        dv_seq = exchange(dv_t).reshape(-1, seq_loc)
        dq_seq = exchange(dq_t).reshape(-1, seq_loc)
        d_hidden = sum(lax.dot_general(d, w, (((0,), (1,)), ((), ())), preferred_element_type=F32)
                       for d, w in ((dk_seq, w_key), (dv_seq, w_value), (dq_seq, w_query))).astype(BF16)
        d_merged_attn, g_pre = pre_pull(d_hidden)
        d_merged = (d_resid.astype(F32) + d_merged_attn.astype(F32)).astype(BF16)
        grad_text = jnp.where(img_mask, 0.0, d_merged).astype(BF16)

        d_soft_rows = jnp.where(img_mask, d_merged, 0.0).astype(BF16)
        d_normed_rows = dot_nt(d_soft_rows, w_proj).astype(BF16)
        d_normed_all = dot_tn(select, d_normed_rows).astype(BF16)
        d_normed = lax.psum_scatter(d_normed_all, 'cp', scatter_dimension=0, tiled=True)
        d_pooled, g_pn = norm_pull(d_normed)
        spread = (d_pooled.astype(F32) / (POOL * POOL)).astype(BF16).reshape(img_loc, SIDE, 1, SIDE, 1, dim_v)
        grad_vis = jnp.broadcast_to(spread, (img_loc, SIDE, POOL, SIDE, POOL, dim_v)).reshape(img_loc, patches, dim_v)

        pad_cols = -(-d_model // (n_dev * 128)) * n_dev * 128
        d_soft_blk = jnp.pad(d_soft_rows, ((0, 0), (0, pad_cols - d_model))).T.reshape(n_dev, pad_cols // n_dev, seq_loc)
        d_soft_t = exchange(d_soft_blk)
        normed_pos = dot(select_all, normed_all).astype(BF16).reshape(n_dev, seq_loc, dim_v)
        g_proj = sum(lax.dot_general(normed_pos[i], d_soft_t[i], (((0,), (1,)), ((), ())), preferred_element_type=F32) for i in range(n_dev))
        g_proj = gather(g_proj.astype(BF16), 1)

        g_query = gather(dot_tn(hidden_all, d_qkv[:, :wq_loc]).astype(BF16), 1)
        o_rows = o_t.transpose(0, 2, 1).reshape(seq, wq_loc)
        g_out = gather(dot_tn(o_rows, d_proj_all).astype(BF16))
        g_value = gather(dot_tn(hidden_all, d_qkv[:, wq_loc + wk_loc:]).astype(BF16), 1)
        g_key = gather(dot_tn(hidden_all, d_qkv[:, wq_loc:wq_loc + wk_loc]).astype(BF16), 1)
        g_proj, g_query, g_out, g_value, g_key = [copy_out(g, c) for g, c in (
            (g_proj, d_model), (g_query, n_dev * wq_loc), (g_out, d_model), (g_value, n_dev * wk_loc), (g_key, n_dev * wk_loc))]
        small = lax.psum((g_pn, g_pre, g_q_gain[0], g_k_gain[0], g_post), 'cp')
        g_pn, g_pre, g_q_gain, g_k_gain, g_post = [part.astype(BF16) for part in small]
        return (y_loc, grad_text, grad_vis, g_pn, g_proj, g_pre, g_query, g_key, g_value, g_q_gain, g_k_gain, g_out, g_post)

    in_specs = (seq_spec, seq_spec, part_spec, seq_spec) + (rep_spec,) * 10
    out_specs = (seq_spec, seq_spec, seq_spec) + (part_spec,) * 10
    return jax.shard_map(device_step, mesh=mesh, in_specs=in_specs, out_specs=out_specs, check_vma=False)
```

```python
import functools
import math
import jax
import jax.numpy as jnp
from jax import lax
from jax.experimental import pallas as pl
from jax.experimental.pallas import tpu as pltpu
from jax.sharding import PartitionSpec as P

GRID = 64
POOL = 4
SIDE = GRID // POOL
BLOCK = SIDE * SIDE
EPS = 1e-6
ROPE_BASE = 1000000.0
ROPE_SCALE = 8.0
NEG_BIG = -1e30
F32 = jnp.float32
BF16 = jnp.bfloat16
LOG2E = math.log2(math.e)


def rms_scale(values, gain_vec):
    wide_vals = values.astype(F32)
    mean_sq = jnp.mean(wide_vals * wide_vals, axis=-1, keepdims=True)
    return wide_vals * lax.rsqrt(mean_sq + EPS) * (1.0 + gain_vec)


def gain_norm(values, gain_vec):
    return rms_scale(values, gain_vec).astype(BF16)


def post_residual(merged, proj_out, gain_vec):
    return (merged.astype(F32) + rms_scale(proj_out, gain_vec)).astype(BF16)


def dot(a, b):
    return jnp.dot(a, b, preferred_element_type=F32)


def dot_nt(a, b):
    return lax.dot_general(a, b, (((1,), (1,)), ((), ())), preferred_element_type=F32)


def dot_tn(a, b):
    return lax.dot_general(a, b, (((0,), (0,)), ((), ())), preferred_element_type=F32)


def rope_tables(seq, head_dim):
    inv_freq = ROPE_BASE ** (-jnp.arange(0, head_dim, 2).astype(F32) / head_dim)
    rot_angle = (jnp.arange(seq).astype(F32) / ROPE_SCALE)[:, None] * inv_freq[None, :]
    return jnp.cos(rot_angle), jnp.sin(rot_angle)


def rope_fwd_kernel(hd, raw_ref, cos_ref, sin_ref, gq_ref, gk_ref, q_ref, k_ref, kt_ref, vt_ref):
    cos, sin = cos_ref[...], sin_ref[...]
    half = hd // 2
    n_q = q_ref.shape[1] // hd

    def one(col, gain):
        x = raw_ref[:, col:col + hd].astype(F32)
        r = lax.rsqrt(jnp.mean(x * x, axis=-1, keepdims=True) + EPS)
        x = x * r * (1.0 + gain)
        a, b = x[:, :half], x[:, half:]
        return (a * cos - b * sin), (b * cos + a * sin)

    for h in range(n_q):
        a, b = one(h * hd, gq_ref[...])
        q_ref[:, h * hd:h * hd + half] = a.astype(BF16)
        q_ref[:, h * hd + half:(h + 1) * hd] = b.astype(BF16)
    a, b = one(n_q * hd, gk_ref[...])
    k_ref[:, :half] = a.astype(BF16)
    k_ref[:, half:] = b.astype(BF16)
    kt_ref[:half, :] = a.T.astype(BF16)
    kt_ref[half:, :] = b.T.astype(BF16)
    vt_ref[...] = raw_ref[:, (n_q + 1) * hd:].T


def rope_fwd(raw, cos, sin, gq, gk, hd, n_q):
    seq, width = raw.shape
    bm = 512
    row = lambda w: pl.BlockSpec((bm, w), lambda i: (i, 0))
    fix = pl.BlockSpec((1, hd), lambda i: (0, 0))
    return pl.pallas_call(
        functools.partial(rope_fwd_kernel, hd),
        grid=(seq // bm,),
        in_specs=[row(width), row(hd // 2), row(hd // 2), fix, fix],
        out_specs=[row(n_q * hd), row(hd), pl.BlockSpec((hd, bm), lambda i: (0, i)), pl.BlockSpec((hd, bm), lambda i: (0, i))],
        out_shape=[jax.ShapeDtypeStruct((seq, n_q * hd), BF16), jax.ShapeDtypeStruct((seq, hd), BF16)] + [jax.ShapeDtypeStruct((hd, seq), BF16)] * 2,
        cost_estimate=pl.CostEstimate(flops=20 * seq * width, bytes_accessed=4 * seq * width, transcendentals=0),
        name="rope_fwd",
    )(raw, cos, sin, gq, gk)


def rope_bwd_kernel(hd, raw_ref, dq0_ref, dq1_ref, dk_ref, dv_ref, cos_ref, sin_ref, gq_ref, gk_ref, out_ref, qt_ref, kt_ref, vt_ref, sq_ref, sk_ref):
    cos, sin = cos_ref[...], sin_ref[...]
    half = hd // 2
    n_q = dq0_ref.shape[1] // hd

    @pl.when(pl.program_id(0) == 0)
    def _():
        sq_ref[...] = jnp.zeros_like(sq_ref)
        sk_ref[...] = jnp.zeros_like(sk_ref)

    def load(refs, lo, hi):
        return jnp.concatenate([ref[:, lo:hi] for ref in refs], axis=0).astype(F32)

    def one(col, refs, dcol, gain, acc_ref, t_ref):
        da = load(refs, dcol, dcol + half)
        db = load(refs, dcol + half, dcol + hd)
        d = jnp.concatenate([da * cos + db * sin, db * cos - da * sin], axis=1)
        x = raw_ref[:, col:col + hd].astype(F32)
        r = lax.rsqrt(jnp.mean(x * x, axis=-1, keepdims=True) + EPS)
        xr = x * r
        acc_ref[...] += jnp.sum(d * xr, axis=0, keepdims=True)
        gd = d * (1.0 + gain)
        dx = r * (gd - xr * jnp.mean(xr * gd, axis=-1, keepdims=True))
        dx = dx.astype(BF16)
        out_ref[:, col:col + hd] = dx
        t_ref[0, dcol:dcol + hd, :] = dx.T

    for h in range(n_q):
        one(h * hd, (dq0_ref, dq1_ref), h * hd, gq_ref[...], sq_ref, qt_ref)
    one(n_q * hd, (dk_ref,), 0, gk_ref[...], sk_ref, kt_ref)
    out_ref[:, (n_q + 1) * hd:] = dv_ref[...]
    vt_ref[0] = dv_ref[...].T


def rope_bwd(raw, dq_halves, dk, dv, cos, sin, gq, gk, hd, n_q, bm):
    seq, width = raw.shape
    tall = lambda w: pl.BlockSpec((1, w, bm), lambda i: (i, 0, 0))
    tshape = lambda w: jax.ShapeDtypeStruct((seq // bm, w, bm), BF16)
    row = lambda w: pl.BlockSpec((bm, w), lambda i: (i, 0))
    fix = pl.BlockSpec((1, hd), lambda i: (0, 0))
    return pl.pallas_call(
        functools.partial(rope_bwd_kernel, hd),
        grid=(seq // bm,),
        in_specs=[row(width)] + [pl.BlockSpec((bm // 2, n_q * hd), lambda i: (i, 0))] * 2 + [row(hd), row(hd), row(hd // 2), row(hd // 2), fix, fix],
        out_specs=[row(width), tall(n_q * hd), tall(hd), tall(hd), fix, fix],
        out_shape=[jax.ShapeDtypeStruct((seq, width), BF16), tshape(n_q * hd), tshape(hd), tshape(hd), jax.ShapeDtypeStruct((1, hd), F32), jax.ShapeDtypeStruct((1, hd), F32)],
        cost_estimate=pl.CostEstimate(flops=30 * seq * width, bytes_accessed=6 * seq * width, transcendentals=0),
        name="rope_bwd",
    )(raw, *dq_halves, dk, dv, cos, sin, gq, gk)


BQ = 256
KB = 512
HALVES = 2
HALF_DEV = 4


def stack_heads(blk, hd):
    return jnp.concatenate([blk[:, h * hd:(h + 1) * hd] for h in range(blk.shape[1] // hd)], axis=0)


def fold_rows(x, op):
    out = x[:8]
    for c in range(1, x.shape[0] // 8):
        out = op(out, x[c * 8:(c + 1) * 8])
    return out


def wide(blk, hd):
    return jnp.concatenate([blk[h * hd:(h + 1) * hd] for h in range(blk.shape[0] // hd)], axis=1)


def attn_fwd_kernel(hd, part, nkb_ref, lim_ref, q_ref, k_ref, vt_ref, o_ref, o32_ref, lse_ref, s_ref):
    qb = HALVES * pl.program_id(0) + part
    coef = hd ** -0.5 * LOG2E
    n_q = q_ref.shape[1] // hd
    rows = n_q * BQ
    qt = stack_heads(q_ref[...], hd).T
    lim2 = jnp.concatenate([lim_ref[0]] * n_q, axis=1)
    n_full = (qb * BQ) // KB
    n_all = nkb_ref[qb]

    def score(kb):
        keys = pl.ds(pl.multiple_of(kb * KB, KB), KB)
        return dot(k_ref[keys, :], qt), keys

    def full_body(kb, m):
        s, keys = score(kb)
        s_ref[keys, :] = s
        return jnp.maximum(m, fold_rows(s, jnp.maximum))

    def mask_body(kb, m):
        s, keys = score(kb)
        key = kb * KB + lax.broadcasted_iota(jnp.int32, s.shape, 0)
        s = jnp.where(key <= lim2, s, NEG_BIG)
        s_ref[keys, :] = s
        return jnp.maximum(m, fold_rows(s, jnp.maximum))

    m = lax.fori_loop(0, n_full, full_body, jnp.full((8, rows), NEG_BIG, F32))
    m = lax.fori_loop(n_full, n_all, mask_body, m)
    m = jnp.max(m, axis=0, keepdims=True)

    def exp_body(kb, l):
        keys = pl.ds(pl.multiple_of(kb * KB, KB), KB)
        e = jnp.exp2((s_ref[keys, :] - m) * coef)
        s_ref[keys, :] = e
        return l + fold_rows(e, jnp.add)

    l = lax.fori_loop(0, n_all, exp_body, jnp.zeros((8, rows), F32))
    l = jnp.sum(l, axis=0, keepdims=True)
    inv = 1.0 / l

    def pv_body(kb, acc):
        keys = pl.ds(pl.multiple_of(kb * KB, KB), KB)
        p = (s_ref[keys, :] * inv).astype(BF16)
        return acc + dot(vt_ref[:, keys], p)

    acc = lax.fori_loop(0, n_all, pv_body, jnp.zeros((hd, rows), F32))
    for h in range(n_q):
        part = acc[:, h * BQ:(h + 1) * BQ]
        o32_ref[0, h * hd:(h + 1) * hd, :] = part
        o_ref[0, h * hd:(h + 1) * hd, :] = part.astype(BF16)
    lse_ref[0] = jnp.broadcast_to(m * coef + jnp.log2(l), (8, rows))


def attn_fwd(part, nkb, lim, q, k, vt, hd, n_dev):
    seq, width = q.shape
    n_q = width // hd
    tall = pl.BlockSpec((1, width, BQ), lambda i, *_: (i, 0, 0))
    at = lambda i, *_: HALVES * i + part
    return pl.pallas_call(
        functools.partial(attn_fwd_kernel, hd, part),
        grid_spec=pltpu.PrefetchScalarGridSpec(
            num_scalar_prefetch=1,
            grid=(n_dev,),
            in_specs=[pl.BlockSpec((1, 1, BQ), lambda i, *_: (at(i), 0, 0)), pl.BlockSpec((BQ, width), lambda i, *_: (at(i), 0)),
                      pl.BlockSpec((seq, hd), lambda i, *_: (0, 0)), pl.BlockSpec((hd, seq), lambda i, *_: (0, 0))],
            out_specs=[tall, tall, pl.BlockSpec((1, 8, n_q * BQ), lambda i, *_: (i, 0, 0))],
            scratch_shapes=[pltpu.VMEM((seq, n_q * BQ), F32)]),
        out_shape=[jax.ShapeDtypeStruct((n_dev, width, BQ), BF16), jax.ShapeDtypeStruct((n_dev, width, BQ), F32),
                   jax.ShapeDtypeStruct((n_dev, 8, n_q * BQ), F32)],
        cost_estimate=pl.CostEstimate(flops=int(1.1 * seq * seq * width), bytes_accessed=4 * seq * width, transcendentals=seq * seq),
        compiler_params=pltpu.CompilerParams(vmem_limit_bytes=40 * 1024 * 1024),
        name="attn_fwd",
    )(nkb, lim, q, k, vt)


def attn_bwd_kernel(hd, part, nkb_ref, lim_ref, q_ref, k_ref, kt_ref, v_ref, do_ref, o32_ref, lse_ref, *refs):
    step = pl.program_id(0)
    qb = HALVES * step + part
    scale = hd ** -0.5
    coef = scale * LOG2E
    n_q = q_ref.shape[1] // hd
    rows = n_q * BQ
    first, last = part == 0, part == HALVES - 1
    if not first:
        dk_in, dv_in, *refs = refs
    dq_ref, dk_ref, dv_ref, *refs = refs
    dk_acc, dv_acc = refs if last else (dk_ref, dv_ref)

    @pl.when(step == 0)
    def _():
        dk_acc[...] = jnp.zeros_like(dk_acc) if first else dk_in[...]
        dv_acc[...] = jnp.zeros_like(dv_acc) if first else dv_in[...]

    q2 = stack_heads(q_ref[...], hd)
    qt = q2.T
    dot_ = wide(do_ref[0], hd)
    do2 = dot_.T
    delta = jnp.sum(dot_.astype(F32) * wide(o32_ref[0], hd), axis=0, keepdims=True)
    lse = lse_ref[0][0:1, :]
    lim2 = jnp.concatenate([lim_ref[0]] * n_q, axis=1)
    n_full = (qb * BQ) // KB
    n_all = nkb_ref[qb]

    def body(masked, kb, dqt):
        keys = pl.ds(pl.multiple_of(kb * KB, KB), KB)
        st = dot(k_ref[keys, :], qt)
        pt = jnp.exp2(st * coef - lse)
        if masked:
            key = kb * KB + lax.broadcasted_iota(jnp.int32, st.shape, 0)
            pt = jnp.where(key <= lim2, pt, 0.0)
        dpt = dot(v_ref[keys, :], dot_)
        dst = (pt * (dpt - delta) * scale).astype(BF16)
        dv_acc[keys, :] += dot(pt.astype(BF16), do2)
        dk_acc[keys, :] += dot(dst, q2)
        return dqt + dot(kt_ref[:, keys], dst)

    dqt = lax.fori_loop(0, n_full, functools.partial(body, False), jnp.zeros((hd, rows), F32))
    dqt = lax.fori_loop(n_full, n_all, functools.partial(body, True), dqt)
    dq = dqt.T.astype(BF16)
    for h in range(n_q):
        dq_ref[:, h * hd:(h + 1) * hd] = dq[h * BQ:(h + 1) * BQ]

    if last:
        @pl.when(step == pl.num_programs(0) - 1)
        def _():
            dk_ref[...] = dk_acc[...].astype(BF16)
            dv_ref[...] = dv_acc[...].astype(BF16)


def attn_bwd(part, nkb, lim, q, k, kt, raw, d_o, o32, lse, carried, hd, n_dev):
    seq, width = q.shape
    n_q = width // hd
    v_col = raw.shape[1] // hd - 1
    at = lambda i, *_: HALVES * i + part
    tall = pl.BlockSpec((1, width, BQ), lambda i, *_: (i, 0, 0))
    whole = pl.BlockSpec((seq, hd), lambda i, *_: (0, 0))
    last = part == HALVES - 1
    acc_type = BF16 if last else F32
    return pl.pallas_call(
        functools.partial(attn_bwd_kernel, hd, part),
        grid_spec=pltpu.PrefetchScalarGridSpec(
            num_scalar_prefetch=1,
            grid=(n_dev,),
            in_specs=[pl.BlockSpec((1, 1, BQ), lambda i, *_: (at(i), 0, 0)), pl.BlockSpec((BQ, width), lambda i, *_: (at(i), 0)), whole,
                      pl.BlockSpec((hd, seq), lambda i, *_: (0, 0)), pl.BlockSpec((seq, hd), lambda i, *_: (0, v_col)), tall, tall,
                      pl.BlockSpec((1, 8, n_q * BQ), lambda i, *_: (i, 0, 0))] + [whole] * len(carried),
            out_specs=[pl.BlockSpec((BQ, width), lambda i, *_: (i, 0)), whole, whole],
            scratch_shapes=[pltpu.VMEM((seq, hd), F32)] * 2 if last else []),
        out_shape=[jax.ShapeDtypeStruct((n_dev * BQ, width), BF16), jax.ShapeDtypeStruct((seq, hd), acc_type), jax.ShapeDtypeStruct((seq, hd), acc_type)],
        cost_estimate=pl.CostEstimate(flops=int(2.7 * seq * seq * width), bytes_accessed=6 * seq * width, transcendentals=seq * seq),
        compiler_params=pltpu.CompilerParams(vmem_limit_bytes=56 * 1024 * 1024),
        name="attn_bwd",
    )(nkb, lim, q, k, kt, raw, d_o, o32, lse, *carried)


def by_core(core_ref, own_ref, par_ref, store):
    @pl.when(core_ref[0] == 0)
    def _():
        store(own_ref, par_ref)

    @pl.when(core_ref[0] != 0)
    def _():
        store(par_ref, own_ref)


def merge_cols_kernel(core_ref, own_ref, par_ref, o_ref):
    n = HALF_DEV
    w = own_ref.shape[1] // n

    def store(even, odd):
        for j in range(n):
            o_ref[:, 2 * j * w:(2 * j + 1) * w] = even[:, j * w:(j + 1) * w]
            o_ref[:, (2 * j + 1) * w:(2 * j + 2) * w] = odd[:, j * w:(j + 1) * w]

    by_core(core_ref, own_ref, par_ref, store)


def merge_rows_kernel(core_ref, own_ref, par_ref, o_ref):
    b = own_ref.shape[0]

    def store(even, odd):
        o_ref[:b] = even[...]
        o_ref[b:] = odd[...]

    by_core(core_ref, own_ref, par_ref, store)


def merge_rows_t_kernel(core_ref, own_ref, par_ref, o_ref):
    def store(even, odd):
        o_ref[...] = jnp.concatenate([even[...], odd[...]], axis=0).T

    by_core(core_ref, own_ref, par_ref, store)


def merge_call(body, core, own, par, grid, in_block, in_map, out_shape, out_block, out_map):
    return pl.pallas_call(
        body,
        grid_spec=pltpu.PrefetchScalarGridSpec(
            num_scalar_prefetch=1, grid=(grid,),
            in_specs=[pl.BlockSpec(in_block, in_map)] * 2,
            out_specs=pl.BlockSpec(out_block, out_map)),
        out_shape=jax.ShapeDtypeStruct(out_shape, own.dtype),
        cost_estimate=pl.CostEstimate(flops=out_shape[0] * out_shape[1], bytes_accessed=4 * out_shape[0] * out_shape[1], transcendentals=0),
        compiler_params=pltpu.CompilerParams(vmem_limit_bytes=40 * 1024 * 1024),
        name="merge",
    )(core, own, par)


def merge_cols(core, own, par):
    rows, cols = own.shape
    bm = 512
    return merge_call(merge_cols_kernel, core, own, par, rows // bm, (bm, cols), lambda i, *_: (i, 0), (rows, 2 * cols), (bm, 2 * cols), lambda i, *_: (i, 0))


def merge_rows(core, own, par, n):
    rows, cols = own.shape
    bm = rows // n
    return merge_call(merge_rows_kernel, core, own, par, n, (bm, cols), lambda i, *_: (i, 0), (2 * rows, cols), (2 * bm, cols), lambda i, *_: (i, 0))


def merge_rows_t(core, own, par, n):
    rows, cols = own.shape
    bm = rows // n
    return merge_call(merge_rows_t_kernel, core, own, par, n, (bm, cols), lambda i, *_: (i, 0), (cols, 2 * rows), (cols, 2 * bm), lambda i, *_: (0, i))


def solution(mesh):
    n_dev = mesh.shape['cp']
    seq_spec = P(('dp', 'cp'))
    part_spec = P('dp')
    rep_spec = P()

    def gather(x, axis=0):
        return lax.all_gather(x, 'cp', axis=axis, tiled=True)

    def exchange(x, after=None):
        if after is not None:
            x, _ = lax.optimization_barrier((x, after))
        return lax.all_to_all(x, 'cp', split_axis=0, concat_axis=0, tiled=True)

    def gather_pair(x, axis=0):
        own = lax.all_gather(x, 'cp', axis=axis, tiled=True, axis_index_groups=[list(range(c, n_dev, 2)) for c in range(2)])
        return own, lax.ppermute(own, 'cp', [(i, i ^ 1) for i in range(n_dev)])

    def device_step(vis_loc, text_loc, img_pos, grad_y, pn_gain, w_proj, pre_gain, w_query, w_key, w_value, q_gain, k_gain, w_out, post_gain):
        rank = lax.axis_index('cp')
        seq_loc, d_model = text_loc.shape
        seq = seq_loc * n_dev
        img_loc, patches, dim_v = vis_loc.shape
        n_img = img_pos.shape[0]
        hd = q_gain.shape[0]
        wq_loc = w_query.shape[1] // n_dev
        wk_loc = w_key.shape[1] // n_dev
        n_q = wq_loc // hd
        pn32, pre32, post32 = pn_gain.astype(F32), pre_gain.astype(F32), post_gain.astype(F32)
        gq32 = q_gain.astype(F32)[None, :]
        gk32 = k_gain.astype(F32)[None, :]

        patch = jnp.arange(patches)
        patch_cell = (patch // (GRID * POOL)) * SIDE + (patch % GRID) // POOL
        pool_mat = (jnp.arange(BLOCK)[:, None] == patch_cell[None, :]).astype(BF16)
        pooled = jnp.einsum('cp,npd->ncd', pool_mat, vis_loc, preferred_element_type=F32) / (POOL * POOL)
        pooled = pooled.astype(BF16).reshape(img_loc * BLOCK, dim_v)
        normed, norm_pull = jax.vjp(gain_norm, pooled, pn32)
        normed_all = gather(normed)

        q_pos = rank * seq_loc + jnp.arange(seq_loc)
        offset = q_pos[:, None] - img_pos[None, :]
        in_blk = (offset >= 0) & (offset < BLOCK)
        is_img = jnp.any(in_blk, axis=1)
        img_mask = is_img[:, None]
        flat_row = jnp.sum(jnp.where(in_blk, jnp.arange(n_img)[None, :] * BLOCK + offset, 0), axis=1)
        flat_row = jnp.where(is_img, flat_row, -1)
        select = (flat_row[:, None] == jnp.arange(n_img * BLOCK)[None, :]).astype(BF16)
        all_pos = jnp.arange(seq)
        all_off = all_pos[:, None] - img_pos[None, :]
        all_in = (all_off >= 0) & (all_off < BLOCK)
        limit = (all_pos + jnp.sum(jnp.where(all_in, BLOCK - 1 - all_off, 0), axis=1)).astype(jnp.int32).reshape(seq // BQ, 1, BQ)
        n_kb = (jnp.max(limit, axis=(1, 2)) // KB + 1).astype(jnp.int32)
        all_flat = jnp.sum(jnp.where(all_in, jnp.arange(n_img)[None, :] * BLOCK + all_off + 1, 0), axis=1) - 1
        select_all = (all_flat[:, None] == jnp.arange(n_img * BLOCK)[None, :]).astype(BF16)

        normed_rows = dot(select, normed_all).astype(BF16)
        soft_rows = dot(normed_rows, w_proj).astype(BF16)
        merged = jnp.where(img_mask, soft_rows, text_loc)
        hidden, pre_pull = jax.vjp(gain_norm, merged, pre32)
        hidden_all = gather(hidden)

        w_qkv = jnp.concatenate([
            lax.dynamic_slice_in_dim(w_query, rank * wq_loc, wq_loc, 1),
            lax.dynamic_slice_in_dim(w_key, rank * wk_loc, wk_loc, 1),
            lax.dynamic_slice_in_dim(w_value, rank * wk_loc, wk_loc, 1)], axis=1)
        raw = dot(hidden_all, w_qkv).astype(BF16)
        cos_t, sin_t = rope_tables(seq, hd)
        q, k, kt, vt = rope_fwd(raw, cos_t, sin_t, gq32, gk32, hd, n_q)
        core = rank % 2
        rows_of = lambda x, c: x[c * BQ:(c + 1) * BQ]
        fwd = []
        for c in range(HALVES):
            fwd.append(attn_fwd(c, n_kb, limit, q, k, vt, hd, n_dev))
        y_parts, d_o, d_proj_all, g_post = [], [], [], 0.0
        attn_t = []
        for c in range(HALVES):
            attn_t.append(exchange(fwd[c][0], attn_t[-1] if c else None))
        prev = attn_t[-1]
        for c in range(HALVES):
            attn_c = attn_t[c]
            if c:
                attn_c, _ = lax.optimization_barrier((attn_c, d_attn_t))
            proj_out = dot_tn(attn_c.reshape(n_dev * wq_loc, BQ), w_out).astype(BF16)
            y_part, post_pull = jax.vjp(post_residual, rows_of(merged, c), proj_out, post32)
            _, d_proj, g_post_part = post_pull(rows_of(grad_y, c))
            d_attn_t = dot_nt(w_out, d_proj).astype(BF16).reshape(n_dev, wq_loc, BQ)
            y_parts.append(y_part)
            g_post = g_post + g_post_part
            prev = exchange(d_attn_t, prev)
            d_o.append(prev)
            d_proj_all.append(gather_pair(d_proj))
        y_loc = jnp.concatenate(y_parts, axis=0)

        dq_halves, carried = [], []
        for c in range(HALVES):
            dq, *carried = attn_bwd(c, n_kb, limit, q, k, kt, raw, d_o[c], fwd[c][1], fwd[c][2], carried, hd, n_dev)
            dq_halves.append(dq)
        dk, dv = carried
        g_value = gather_pair(dot_tn(hidden_all, dv).astype(BF16), 1)
        d_qkv, dq_t, dk_t, dv_t, g_q_gain, g_k_gain = rope_bwd(raw, dq_halves, dk, dv, cos_t, sin_t, gq32, gk32, hd, n_q, seq_loc)

        dk_seq = exchange(dk_t, prev)
        dv_seq = exchange(dv_t, dk_seq)
        dq_seq = exchange(dq_t, dv_seq)
        dk_seq, dv_seq, dq_last = [x.reshape(-1, seq_loc) for x in (dk_seq, dv_seq, dq_seq)]
        d_hidden = sum(lax.dot_general(d, w, (((0,), (1,)), ((), ())), preferred_element_type=F32)
                       for d, w in ((dk_seq, w_key), (dv_seq, w_value), (dq_last, w_query))).astype(BF16)
        d_merged_attn, g_pre = pre_pull(d_hidden)
        d_merged = (grad_y.astype(F32) + d_merged_attn.astype(F32)).astype(BF16)
        grad_text = jnp.where(img_mask, 0.0, d_merged).astype(BF16)

        d_soft_rows = jnp.where(img_mask, d_merged, 0.0).astype(BF16)
        d_normed_rows = dot_nt(d_soft_rows, w_proj).astype(BF16)
        d_normed_all = dot_tn(select, d_normed_rows).astype(BF16)
        d_normed = lax.psum_scatter(d_normed_all, 'cp', scatter_dimension=0, tiled=True)
        d_pooled, g_pn = norm_pull(d_normed)
        spread = (d_pooled.astype(F32) / (POOL * POOL)).astype(BF16).reshape(img_loc, SIDE, 1, SIDE, 1, dim_v)
        grad_vis = jnp.broadcast_to(spread, (img_loc, SIDE, POOL, SIDE, POOL, dim_v)).reshape(img_loc, patches, dim_v)

        d_soft_t = exchange(d_soft_rows.T.reshape(n_dev, d_model // n_dev, seq_loc), dq_seq)
        normed_pos = dot(select_all, normed_all).astype(BF16).reshape(n_dev, seq_loc, dim_v)
        g_proj = sum(dot(d_soft_t[i], normed_pos[i]) for i in range(n_dev)).astype(BF16)
        g_proj = gather_pair(g_proj)

        g_query = gather_pair(dot_tn(hidden_all, d_qkv[:, :wq_loc]).astype(BF16), 1)
        g_key = gather_pair(dot_tn(hidden_all, d_qkv[:, wq_loc:wq_loc + wk_loc]).astype(BF16), 1)
        g_out = 0.0
        for c in range(HALVES):
            o_rows = fwd[c][0].transpose(0, 2, 1).reshape(HALF_DEV, 2, BQ, wq_loc)
            for side, d_part in zip((core, 1 - core), d_proj_all[c]):
                g_out = g_out + dot_tn(lax.dynamic_index_in_dim(o_rows, side, 1, False).reshape(-1, wq_loc), d_part)
        g_out = gather_pair(g_out.astype(BF16))
        core_arr = core.astype(jnp.int32).reshape(1)
        g_value = merge_cols(core_arr, *g_value)
        g_key = merge_cols(core_arr, *g_key)
        g_query = merge_cols(core_arr, *g_query)
        g_out = merge_rows(core_arr, *g_out, HALF_DEV)
        g_proj = merge_rows_t(core_arr, *g_proj, HALF_DEV)
        small = lax.psum((g_pn, g_pre, g_q_gain[0], g_k_gain[0], g_post), 'cp')
        g_pn, g_pre, g_q_gain, g_k_gain, g_post = [part.astype(BF16) for part in small]
        return (y_loc, grad_text, grad_vis, g_pn, g_proj, g_pre, g_query, g_key, g_value, g_q_gain, g_k_gain, g_out, g_post)

    in_specs = (seq_spec, seq_spec, part_spec, seq_spec) + (rep_spec,) * 10
    out_specs = (seq_spec, seq_spec, seq_spec) + (part_spec,) * 10
    return jax.shard_map(device_step, mesh=mesh, in_specs=in_specs, out_specs=out_specs, check_vma=False)
```

```python
import functools
import math
import jax
import jax.numpy as jnp
from jax import lax
from jax.experimental import pallas as pl
from jax.experimental.pallas import tpu as pltpu
from jax.sharding import PartitionSpec as P

GRID = 64
POOL = 4
SIDE = GRID // POOL
BLOCK = SIDE * SIDE
EPS = 1e-6
ROPE_BASE = 1000000.0
ROPE_SCALE = 8.0
NEG_BIG = -1e30
F32 = jnp.float32
BF16 = jnp.bfloat16
LOG2E = math.log2(math.e)


def rms_scale(values, gain_vec):
    wide_vals = values.astype(F32)
    mean_sq = jnp.mean(wide_vals * wide_vals, axis=-1, keepdims=True)
    return wide_vals * lax.rsqrt(mean_sq + EPS) * (1.0 + gain_vec)


def gain_norm(values, gain_vec):
    return rms_scale(values, gain_vec).astype(BF16)


def post_residual(merged, proj_out, gain_vec):
    return (merged.astype(F32) + rms_scale(proj_out, gain_vec)).astype(BF16)


def dot(a, b):
    return jnp.dot(a, b, preferred_element_type=F32)


def dot_nt(a, b):
    return lax.dot_general(a, b, (((1,), (1,)), ((), ())), preferred_element_type=F32)


def dot_tn(a, b):
    return lax.dot_general(a, b, (((0,), (0,)), ((), ())), preferred_element_type=F32)


def rope_tables(seq, head_dim):
    inv_freq = ROPE_BASE ** (-jnp.arange(0, head_dim, 2).astype(F32) / head_dim)
    rot_angle = (jnp.arange(seq).astype(F32) / ROPE_SCALE)[:, None] * inv_freq[None, :]
    return jnp.cos(rot_angle), jnp.sin(rot_angle)


def rope_fwd_kernel(hd, raw_ref, cos_ref, sin_ref, gq_ref, gk_ref, q_ref, k_ref, kt_ref, vt_ref):
    cos, sin = cos_ref[...], sin_ref[...]
    half = hd // 2
    n_q = q_ref.shape[1] // hd

    def one(col, gain):
        x = raw_ref[:, col:col + hd].astype(F32)
        r = lax.rsqrt(jnp.mean(x * x, axis=-1, keepdims=True) + EPS)
        x = x * r * (1.0 + gain)
        a, b = x[:, :half], x[:, half:]
        return (a * cos - b * sin), (b * cos + a * sin)

    for h in range(n_q):
        a, b = one(h * hd, gq_ref[...])
        q_ref[:, h * hd:h * hd + half] = a.astype(BF16)
        q_ref[:, h * hd + half:(h + 1) * hd] = b.astype(BF16)
    a, b = one(n_q * hd, gk_ref[...])
    k_ref[:, :half] = a.astype(BF16)
    k_ref[:, half:] = b.astype(BF16)
    kt_ref[:half, :] = a.T.astype(BF16)
    kt_ref[half:, :] = b.T.astype(BF16)
    vt_ref[...] = raw_ref[:, (n_q + 1) * hd:].T


def rope_fwd(raw, cos, sin, gq, gk, hd, n_q):
    seq, width = raw.shape
    bm = 512
    row = lambda w: pl.BlockSpec((bm, w), lambda i: (i, 0))
    fix = pl.BlockSpec((1, hd), lambda i: (0, 0))
    return pl.pallas_call(
        functools.partial(rope_fwd_kernel, hd),
        grid=(seq // bm,),
        in_specs=[row(width), row(hd // 2), row(hd // 2), fix, fix],
        out_specs=[row(n_q * hd), row(hd), pl.BlockSpec((hd, bm), lambda i: (0, i)), pl.BlockSpec((hd, bm), lambda i: (0, i))],
        out_shape=[jax.ShapeDtypeStruct((seq, n_q * hd), BF16), jax.ShapeDtypeStruct((seq, hd), BF16)] + [jax.ShapeDtypeStruct((hd, seq), BF16)] * 2,
        cost_estimate=pl.CostEstimate(flops=20 * seq * width, bytes_accessed=4 * seq * width, transcendentals=0),
        name="rope_fwd",
    )(raw, cos, sin, gq, gk)


def rope_bwd_kernel(hd, raw_ref, dq0_ref, dq1_ref, dk_ref, dv_ref, cos_ref, sin_ref, gq_ref, gk_ref, out_ref, qt_ref, kt_ref, vt_ref, sq_ref, sk_ref):
    cos, sin = cos_ref[...], sin_ref[...]
    half = hd // 2
    n_q = dq0_ref.shape[1] // hd

    @pl.when(pl.program_id(0) == 0)
    def _():
        sq_ref[...] = jnp.zeros_like(sq_ref)
        sk_ref[...] = jnp.zeros_like(sk_ref)

    def load(refs, lo, hi):
        return jnp.concatenate([ref[:, lo:hi] for ref in refs], axis=0).astype(F32)

    def one(col, refs, dcol, gain, acc_ref, t_ref):
        da = load(refs, dcol, dcol + half)
        db = load(refs, dcol + half, dcol + hd)
        d = jnp.concatenate([da * cos + db * sin, db * cos - da * sin], axis=1)
        x = raw_ref[:, col:col + hd].astype(F32)
        r = lax.rsqrt(jnp.mean(x * x, axis=-1, keepdims=True) + EPS)
        xr = x * r
        acc_ref[...] += jnp.sum(d * xr, axis=0, keepdims=True)
        gd = d * (1.0 + gain)
        dx = r * (gd - xr * jnp.mean(xr * gd, axis=-1, keepdims=True))
        dx = dx.astype(BF16)
        out_ref[:, col:col + hd] = dx
        t_ref[0, dcol:dcol + hd, :] = dx.T

    for h in range(n_q):
        one(h * hd, (dq0_ref, dq1_ref), h * hd, gq_ref[...], sq_ref, qt_ref)
    one(n_q * hd, (dk_ref,), 0, gk_ref[...], sk_ref, kt_ref)
    out_ref[:, (n_q + 1) * hd:] = dv_ref[...]
    vt_ref[0] = dv_ref[...].T


def rope_bwd(raw, dq_halves, dk, dv, cos, sin, gq, gk, hd, n_q, bm):
    seq, width = raw.shape
    tall = lambda w: pl.BlockSpec((1, w, bm), lambda i: (i, 0, 0))
    tshape = lambda w: jax.ShapeDtypeStruct((seq // bm, w, bm), BF16)
    row = lambda w: pl.BlockSpec((bm, w), lambda i: (i, 0))
    fix = pl.BlockSpec((1, hd), lambda i: (0, 0))
    return pl.pallas_call(
        functools.partial(rope_bwd_kernel, hd),
        grid=(seq // bm,),
        in_specs=[row(width)] + [pl.BlockSpec((bm // 2, n_q * hd), lambda i: (i, 0))] * 2 + [row(hd), row(hd), row(hd // 2), row(hd // 2), fix, fix],
        out_specs=[row(width), tall(n_q * hd), tall(hd), tall(hd), fix, fix],
        out_shape=[jax.ShapeDtypeStruct((seq, width), BF16), tshape(n_q * hd), tshape(hd), tshape(hd), jax.ShapeDtypeStruct((1, hd), F32), jax.ShapeDtypeStruct((1, hd), F32)],
        cost_estimate=pl.CostEstimate(flops=30 * seq * width, bytes_accessed=6 * seq * width, transcendentals=0),
        name="rope_bwd",
    )(raw, *dq_halves, dk, dv, cos, sin, gq, gk)


BQ = 256
KB = 512
HALVES = 2


def stack_heads(blk, hd):
    return jnp.concatenate([blk[:, h * hd:(h + 1) * hd] for h in range(blk.shape[1] // hd)], axis=0)


def wide(blk, hd):
    return jnp.concatenate([blk[h * hd:(h + 1) * hd] for h in range(blk.shape[0] // hd)], axis=1)


def attn_fwd_kernel(hd, part, nkb_ref, lim_ref, q_ref, k_ref, vt_ref, o_ref, o32_ref, lse_ref, s_ref):
    qb = HALVES * pl.program_id(0) + part
    coef = hd ** -0.5 * LOG2E
    n_q = q_ref.shape[1] // hd
    rows = n_q * BQ
    qt = stack_heads(q_ref[...], hd).T
    lim2 = jnp.concatenate([lim_ref[0]] * n_q, axis=1)
    n_full = (qb * BQ) // KB
    n_all = nkb_ref[qb]

    def body(masked, kb, stats):
        m, l = stats
        keys = pl.ds(pl.multiple_of(kb * KB, KB), KB)
        t = dot(k_ref[keys, :], qt) * coef
        if masked:
            key = kb * KB + lax.broadcasted_iota(jnp.int32, t.shape, 0)
            t = jnp.where(key <= lim2, t, NEG_BIG)
        s_ref[keys, :] = t
        t = t.reshape(KB // 8, 8, rows)
        m_new = jnp.maximum(m, jnp.max(t, axis=0))
        return m_new, l * jnp.exp2(m - m_new) + jnp.sum(jnp.exp2(t - m_new), axis=0)

    stats = (jnp.full((8, rows), NEG_BIG, F32), jnp.zeros((8, rows), F32))
    stats = lax.fori_loop(0, n_full, functools.partial(body, False), stats)
    m8, l8 = lax.fori_loop(n_full, n_all, functools.partial(body, True), stats)
    m = jnp.max(m8, axis=0, keepdims=True)
    lse = m + jnp.log2(jnp.sum(l8 * jnp.exp2(m8 - m), axis=0, keepdims=True))

    def pv_body(kb, acc):
        keys = pl.ds(pl.multiple_of(kb * KB, KB), KB)
        p = jnp.exp2(s_ref[keys, :] - lse).astype(BF16)
        return acc + dot(vt_ref[:, keys], p)

    acc = lax.fori_loop(0, n_all, pv_body, jnp.zeros((hd, rows), F32))
    for h in range(n_q):
        part = acc[:, h * BQ:(h + 1) * BQ]
        o32_ref[0, h * hd:(h + 1) * hd, :] = part
        o_ref[0, h * hd:(h + 1) * hd, :] = part.astype(BF16)
    lse_ref[0] = jnp.broadcast_to(lse, (8, rows))


def attn_fwd(part, nkb, lim, q, k, vt, hd, n_dev):
    seq, width = q.shape
    n_q = width // hd
    tall = pl.BlockSpec((1, width, BQ), lambda i, *_: (i, 0, 0))
    at = lambda i, *_: HALVES * i + part
    return pl.pallas_call(
        functools.partial(attn_fwd_kernel, hd, part),
        grid_spec=pltpu.PrefetchScalarGridSpec(
            num_scalar_prefetch=1,
            grid=(n_dev,),
            in_specs=[pl.BlockSpec((1, 1, BQ), lambda i, *_: (at(i), 0, 0)), pl.BlockSpec((BQ, width), lambda i, *_: (at(i), 0)),
                      pl.BlockSpec((seq, hd), lambda i, *_: (0, 0)), pl.BlockSpec((hd, seq), lambda i, *_: (0, 0))],
            out_specs=[tall, tall, pl.BlockSpec((1, 8, n_q * BQ), lambda i, *_: (i, 0, 0))],
            scratch_shapes=[pltpu.VMEM((seq, n_q * BQ), F32)]),
        out_shape=[jax.ShapeDtypeStruct((n_dev, width, BQ), BF16), jax.ShapeDtypeStruct((n_dev, width, BQ), F32),
                   jax.ShapeDtypeStruct((n_dev, 8, n_q * BQ), F32)],
        cost_estimate=pl.CostEstimate(flops=int(1.1 * seq * seq * width), bytes_accessed=4 * seq * width, transcendentals=seq * seq),
        compiler_params=pltpu.CompilerParams(vmem_limit_bytes=40 * 1024 * 1024),
        name="attn_fwd",
    )(nkb, lim, q, k, vt)


def attn_bwd_kernel(hd, part, nkb_ref, lim_ref, q_ref, k_ref, kt_ref, v_ref, do_ref, o32_ref, lse_ref, *refs):
    step = pl.program_id(0)
    qb = HALVES * step + part
    scale = hd ** -0.5
    coef = scale * LOG2E
    n_q = q_ref.shape[1] // hd
    rows = n_q * BQ
    first, last = part == 0, part == HALVES - 1
    if not first:
        dk_in, dv_in, *refs = refs
    dq_ref, dk_ref, dv_ref, *refs = refs
    dk_acc, dv_acc = refs if last else (dk_ref, dv_ref)

    @pl.when(step == 0)
    def _():
        dk_acc[...] = jnp.zeros_like(dk_acc) if first else dk_in[...]
        dv_acc[...] = jnp.zeros_like(dv_acc) if first else dv_in[...]

    q2 = stack_heads(q_ref[...], hd)
    qt = q2.T
    dot_ = wide(do_ref[0], hd)
    do2 = dot_.T
    delta = jnp.sum(dot_.astype(F32) * wide(o32_ref[0], hd), axis=0, keepdims=True)
    lse = lse_ref[0][0:1, :]
    lim2 = jnp.concatenate([lim_ref[0]] * n_q, axis=1)
    n_full = (qb * BQ) // KB
    n_all = nkb_ref[qb]

    def body(masked, kb, dqt):
        keys = pl.ds(pl.multiple_of(kb * KB, KB), KB)
        st = dot(k_ref[keys, :], qt)
        pt = jnp.exp2(st * coef - lse)
        if masked:
            key = kb * KB + lax.broadcasted_iota(jnp.int32, st.shape, 0)
            pt = jnp.where(key <= lim2, pt, 0.0)
        dpt = dot(v_ref[keys, :], dot_)
        dst = (pt * (dpt - delta)).astype(BF16)
        dv_acc[keys, :] += dot(pt.astype(BF16), do2)
        dk_acc[keys, :] += dot(dst, q2)
        return dqt + dot(kt_ref[:, keys], dst)

    dqt = lax.fori_loop(0, n_full, functools.partial(body, False), jnp.zeros((hd, rows), F32))
    dqt = lax.fori_loop(n_full, n_all, functools.partial(body, True), dqt)
    dq = (dqt * scale).T.astype(BF16)
    for h in range(n_q):
        dq_ref[:, h * hd:(h + 1) * hd] = dq[h * BQ:(h + 1) * BQ]

    if last:
        @pl.when(step == pl.num_programs(0) - 1)
        def _():
            dk_ref[...] = (dk_acc[...] * scale).astype(BF16)
            dv_ref[...] = dv_acc[...].astype(BF16)


def attn_bwd(part, nkb, lim, q, k, kt, raw, d_o, o32, lse, carried, hd, n_dev):
    seq, width = q.shape
    n_q = width // hd
    v_col = raw.shape[1] // hd - 1
    at = lambda i, *_: HALVES * i + part
    tall = pl.BlockSpec((1, width, BQ), lambda i, *_: (i, 0, 0))
    whole = pl.BlockSpec((seq, hd), lambda i, *_: (0, 0))
    last = part == HALVES - 1
    acc_type = BF16 if last else F32
    return pl.pallas_call(
        functools.partial(attn_bwd_kernel, hd, part),
        grid_spec=pltpu.PrefetchScalarGridSpec(
            num_scalar_prefetch=1,
            grid=(n_dev,),
            in_specs=[pl.BlockSpec((1, 1, BQ), lambda i, *_: (at(i), 0, 0)), pl.BlockSpec((BQ, width), lambda i, *_: (at(i), 0)), whole,
                      pl.BlockSpec((hd, seq), lambda i, *_: (0, 0)), pl.BlockSpec((seq, hd), lambda i, *_: (0, v_col)), tall, tall,
                      pl.BlockSpec((1, 8, n_q * BQ), lambda i, *_: (i, 0, 0))] + [whole] * len(carried),
            out_specs=[pl.BlockSpec((BQ, width), lambda i, *_: (i, 0)), whole, whole],
            scratch_shapes=[pltpu.VMEM((seq, hd), F32)] * 2 if last else []),
        out_shape=[jax.ShapeDtypeStruct((n_dev * BQ, width), BF16), jax.ShapeDtypeStruct((seq, hd), acc_type), jax.ShapeDtypeStruct((seq, hd), acc_type)],
        cost_estimate=pl.CostEstimate(flops=int(2.7 * seq * seq * width), bytes_accessed=6 * seq * width, transcendentals=seq * seq),
        compiler_params=pltpu.CompilerParams(vmem_limit_bytes=56 * 1024 * 1024),
        name="attn_bwd",
    )(nkb, lim, q, k, kt, raw, d_o, o32, lse, *carried)


def split_kernel(n_dev, x_ref, *o_refs):
    width = x_ref.shape[1] // n_dev
    for g in range(n_dev):
        col = g * width
        for o_ref in o_refs:
            w = o_ref.shape[1] // n_dev
            o_ref[:, g * w:(g + 1) * w] = x_ref[:, col:col + w]
            col += w


def copy_kernel(x_ref, o_ref):
    o_ref[...] = x_ref[...]


def transpose_kernel(x_ref, o_ref):
    o_ref[...] = x_ref[...].T


def stream(body, x, in_spec, shapes, out_specs, grid):
    return pl.pallas_call(
        body,
        grid=(grid,),
        in_specs=[in_spec],
        out_specs=out_specs,
        out_shape=[jax.ShapeDtypeStruct(shape, x.dtype) for shape in shapes],
        cost_estimate=pl.CostEstimate(flops=x.size, bytes_accessed=4 * x.size, transcendentals=0),
        compiler_params=pltpu.CompilerParams(vmem_limit_bytes=40 * 1024 * 1024),
        name="copy_out",
    )(x)


def split_cols(x, n_dev, widths):
    bm = 256
    row = lambda w: pl.BlockSpec((bm, w), lambda i: (i, 0))
    return stream(functools.partial(split_kernel, n_dev), x, row(x.shape[1]), [(x.shape[0], w) for w in widths], [row(w) for w in widths], x.shape[0] // bm)


def copy_rows(x):
    spec = pl.BlockSpec((512, x.shape[1]), lambda i: (i, 0))
    return stream(copy_kernel, x, spec, [x.shape], [spec], x.shape[0] // 512)[0]


def transpose_rows(x):
    rows, cols = x.shape
    return stream(transpose_kernel, x, pl.BlockSpec((512, cols), lambda i: (i, 0)), [(cols, rows)], [pl.BlockSpec((cols, 512), lambda i: (0, i))], rows // 512)[0]


def solution(mesh):
    n_dev = mesh.shape['cp']
    seq_spec = P(('dp', 'cp'))
    part_spec = P('dp')
    rep_spec = P()

    def gather(x, axis=0):
        return lax.all_gather(x, 'cp', axis=axis, tiled=True)

    def exchange(x, after=None):
        if after is not None:
            x, _ = lax.optimization_barrier((x, after))
        return lax.all_to_all(x, 'cp', split_axis=0, concat_axis=0, tiled=True)

    def device_step(vis_loc, text_loc, img_pos, grad_y, pn_gain, w_proj, pre_gain, w_query, w_key, w_value, q_gain, k_gain, w_out, post_gain):
        rank = lax.axis_index('cp')
        seq_loc, d_model = text_loc.shape
        seq = seq_loc * n_dev
        img_loc, patches, dim_v = vis_loc.shape
        n_img = img_pos.shape[0]
        hd = q_gain.shape[0]
        wq_loc = w_query.shape[1] // n_dev
        wk_loc = w_key.shape[1] // n_dev
        n_q = wq_loc // hd
        pn32, pre32, post32 = pn_gain.astype(F32), pre_gain.astype(F32), post_gain.astype(F32)
        gq32 = q_gain.astype(F32)[None, :]
        gk32 = k_gain.astype(F32)[None, :]

        patch = jnp.arange(patches)
        patch_cell = (patch // (GRID * POOL)) * SIDE + (patch % GRID) // POOL
        pool_mat = (jnp.arange(BLOCK)[:, None] == patch_cell[None, :]).astype(BF16)
        pooled = jnp.einsum('cp,npd->ncd', pool_mat, vis_loc, preferred_element_type=F32) / (POOL * POOL)
        pooled = pooled.astype(BF16).reshape(img_loc * BLOCK, dim_v)
        normed, norm_pull = jax.vjp(gain_norm, pooled, pn32)
        normed_all = gather(normed)

        q_pos = rank * seq_loc + jnp.arange(seq_loc)
        offset = q_pos[:, None] - img_pos[None, :]
        in_blk = (offset >= 0) & (offset < BLOCK)
        is_img = jnp.any(in_blk, axis=1)
        img_mask = is_img[:, None]
        flat_row = jnp.sum(jnp.where(in_blk, jnp.arange(n_img)[None, :] * BLOCK + offset, 0), axis=1)
        flat_row = jnp.where(is_img, flat_row, -1)
        select = (flat_row[:, None] == jnp.arange(n_img * BLOCK)[None, :]).astype(BF16)
        all_pos = jnp.arange(seq)
        all_off = all_pos[:, None] - img_pos[None, :]
        all_in = (all_off >= 0) & (all_off < BLOCK)
        limit = (all_pos + jnp.sum(jnp.where(all_in, BLOCK - 1 - all_off, 0), axis=1)).astype(jnp.int32).reshape(seq // BQ, 1, BQ)
        n_kb = (jnp.max(limit, axis=(1, 2)) // KB + 1).astype(jnp.int32)
        all_flat = jnp.sum(jnp.where(all_in, jnp.arange(n_img)[None, :] * BLOCK + all_off + 1, 0), axis=1) - 1
        select_all = (all_flat[:, None] == jnp.arange(n_img * BLOCK)[None, :]).astype(BF16)

        normed_rows = dot(select, normed_all).astype(BF16)
        soft_rows = dot(normed_rows, w_proj).astype(BF16)
        merged = jnp.where(img_mask, soft_rows, text_loc)
        hidden, pre_pull = jax.vjp(gain_norm, merged, pre32)
        hidden_all = gather(hidden)

        w_qkv = jnp.concatenate([
            lax.dynamic_slice_in_dim(w_query, rank * wq_loc, wq_loc, 1),
            lax.dynamic_slice_in_dim(w_key, rank * wk_loc, wk_loc, 1),
            lax.dynamic_slice_in_dim(w_value, rank * wk_loc, wk_loc, 1)], axis=1)
        raw = dot(hidden_all, w_qkv).astype(BF16)
        cos_t, sin_t = rope_tables(seq, hd)
        q, k, kt, vt = rope_fwd(raw, cos_t, sin_t, gq32, gk32, hd, n_q)
        rows_of = lambda x, c: x[c * BQ:(c + 1) * BQ]
        fwd = []
        for c in range(HALVES):
            fwd.append(attn_fwd(c, n_kb, limit, q, k, vt, hd, n_dev))
        y_parts, d_o, d_proj_parts, g_post = [], [], [], 0.0
        attn_t = []
        for c in range(HALVES):
            attn_t.append(exchange(fwd[c][0], attn_t[-1] if c else None))
        prev = attn_t[-1]
        for c in range(HALVES):
            attn_c = attn_t[c]
            if c:
                attn_c, _ = lax.optimization_barrier((attn_c, d_attn_t))
            proj_out = dot_tn(attn_c.reshape(n_dev * wq_loc, BQ), w_out).astype(BF16)
            y_part, post_pull = jax.vjp(post_residual, rows_of(merged, c), proj_out, post32)
            _, d_proj, g_post_part = post_pull(rows_of(grad_y, c))
            d_attn_t = dot_nt(w_out, d_proj).astype(BF16).reshape(n_dev, wq_loc, BQ)
            y_parts.append(y_part)
            g_post = g_post + g_post_part
            prev = exchange(d_attn_t, prev)
            d_o.append(prev)
            d_proj_parts.append(d_proj)
        d_proj_all = gather(jnp.concatenate(d_proj_parts, axis=0))
        y_loc = jnp.concatenate(y_parts, axis=0)

        dq_halves, carried = [], []
        for c in range(HALVES):
            dq, *carried = attn_bwd(c, n_kb, limit, q, k, kt, raw, d_o[c], fwd[c][1], fwd[c][2], carried, hd, n_dev)
            dq_halves.append(dq)
        dk, dv = carried
        d_qkv, dq_t, dk_t, dv_t, g_q_gain, g_k_gain = rope_bwd(raw, dq_halves, dk, dv, cos_t, sin_t, gq32, gk32, hd, n_q, seq_loc)

        g_qkv = dot_tn(hidden_all, d_qkv).astype(BF16)
        g_qkv = gather(g_qkv, 1)

        dq_seq = exchange(dq_t, prev)
        dk_seq = exchange(dk_t, dq_seq)
        dv_last = exchange(dv_t, dk_seq)
        dq_seq, dk_seq, dv_seq = [x.reshape(-1, seq_loc) for x in (dq_seq, dk_seq, dv_last)]
        d_hidden = sum(lax.dot_general(d, w, (((0,), (1,)), ((), ())), preferred_element_type=F32)
                       for d, w in ((dq_seq, w_query), (dk_seq, w_key), (dv_seq, w_value))).astype(BF16)
        d_merged_attn, g_pre = pre_pull(d_hidden)
        d_merged = (grad_y.astype(F32) + d_merged_attn.astype(F32)).astype(BF16)
        grad_text = jnp.where(img_mask, 0.0, d_merged).astype(BF16)

        d_soft_rows = jnp.where(img_mask, d_merged, 0.0).astype(BF16)
        d_normed_rows = dot_nt(d_soft_rows, w_proj).astype(BF16)
        d_normed_all = dot_tn(select, d_normed_rows).astype(BF16)
        d_normed = lax.psum_scatter(d_normed_all, 'cp', scatter_dimension=0, tiled=True)
        d_pooled, g_pn = norm_pull(d_normed)
        spread = (d_pooled.astype(F32) / (POOL * POOL)).astype(BF16).reshape(img_loc, SIDE, 1, SIDE, 1, dim_v)
        grad_vis = jnp.broadcast_to(spread, (img_loc, SIDE, POOL, SIDE, POOL, dim_v)).reshape(img_loc, patches, dim_v)

        d_soft_t = exchange(d_soft_rows.T.reshape(n_dev, d_model // n_dev, seq_loc), dv_last)
        normed_pos = dot(select_all, normed_all).astype(BF16).reshape(n_dev, seq_loc, dim_v)
        g_proj = sum(dot(d_soft_t[i], normed_pos[i]) for i in range(n_dev)).astype(BF16)
        g_proj = gather(g_proj)

        o_rows = jnp.stack([part[0] for part in fwd], axis=1).transpose(0, 1, 3, 2).reshape(seq, wq_loc)
        g_out = dot_tn(o_rows, d_proj_all).astype(BF16)
        g_out = gather(g_out)
        g_query, g_key, g_value = split_cols(g_qkv, n_dev, (n_dev * wq_loc, n_dev * wk_loc, n_dev * wk_loc))
        g_out = copy_rows(g_out)
        g_proj = transpose_rows(g_proj)
        small = lax.psum((g_pn, g_pre, g_q_gain[0], g_k_gain[0], g_post), 'cp')
        g_pn, g_pre, g_q_gain, g_k_gain, g_post = [part.astype(BF16) for part in small]
        return (y_loc, grad_text, grad_vis, g_pn, g_proj, g_pre, g_query, g_key, g_value, g_q_gain, g_k_gain, g_out, g_post)

    in_specs = (seq_spec, seq_spec, part_spec, seq_spec) + (rep_spec,) * 10
    out_specs = (seq_spec, seq_spec, seq_spec) + (part_spec,) * 10
    return jax.shard_map(device_step, mesh=mesh, in_specs=in_specs, out_specs=out_specs, check_vma=False)
```

```python
import functools
import math
import jax
import jax.numpy as jnp
from jax import lax
from jax.experimental import pallas as pl
from jax.experimental.pallas import tpu as pltpu
from jax.sharding import PartitionSpec as P

GRID = 64
POOL = 4
SIDE = GRID // POOL
BLOCK = SIDE * SIDE
EPS = 1e-6
ROPE_BASE = 1000000.0
ROPE_SCALE = 8.0
NEG_BIG = -1e30
F32 = jnp.float32
BF16 = jnp.bfloat16
LOG2E = math.log2(math.e)


def rms_scale(values, gain_vec):
    wide_vals = values.astype(F32)
    mean_sq = jnp.mean(wide_vals * wide_vals, axis=-1, keepdims=True)
    return wide_vals * lax.rsqrt(mean_sq + EPS) * (1.0 + gain_vec)


def gain_norm(values, gain_vec):
    return rms_scale(values, gain_vec).astype(BF16)


def post_residual(merged, proj_out, gain_vec):
    return (merged.astype(F32) + rms_scale(proj_out, gain_vec)).astype(BF16)


def dot(a, b):
    return jnp.dot(a, b, preferred_element_type=F32)


def dot_nt(a, b):
    return lax.dot_general(a, b, (((1,), (1,)), ((), ())), preferred_element_type=F32)


def dot_tn(a, b):
    return lax.dot_general(a, b, (((0,), (0,)), ((), ())), preferred_element_type=F32)


def rope_tables(seq, head_dim):
    inv_freq = ROPE_BASE ** (-jnp.arange(0, head_dim, 2).astype(F32) / head_dim)
    rot_angle = (jnp.arange(seq).astype(F32) / ROPE_SCALE)[:, None] * inv_freq[None, :]
    return jnp.cos(rot_angle), jnp.sin(rot_angle)


def rope_fwd_kernel(hd, raw_ref, cos_ref, sin_ref, gq_ref, gk_ref, q_ref, k_ref, kt_ref, vt_ref):
    cos, sin = cos_ref[...], sin_ref[...]
    half = hd // 2
    n_q = q_ref.shape[1] // hd

    def one(col, gain):
        x = raw_ref[:, col:col + hd].astype(F32)
        r = lax.rsqrt(jnp.mean(x * x, axis=-1, keepdims=True) + EPS)
        x = x * r * (1.0 + gain)
        a, b = x[:, :half], x[:, half:]
        return (a * cos - b * sin), (b * cos + a * sin)

    for h in range(n_q):
        a, b = one(h * hd, gq_ref[...])
        q_ref[:, h * hd:h * hd + half] = a.astype(BF16)
        q_ref[:, h * hd + half:(h + 1) * hd] = b.astype(BF16)
    a, b = one(n_q * hd, gk_ref[...])
    k_ref[:, :half] = a.astype(BF16)
    k_ref[:, half:] = b.astype(BF16)
    kt_ref[:half, :] = a.T.astype(BF16)
    kt_ref[half:, :] = b.T.astype(BF16)
    vt_ref[...] = raw_ref[:, (n_q + 1) * hd:].T


def rope_fwd(raw, cos, sin, gq, gk, hd, n_q):
    seq, width = raw.shape
    bm = 512
    row = lambda w: pl.BlockSpec((bm, w), lambda i: (i, 0))
    fix = pl.BlockSpec((1, hd), lambda i: (0, 0))
    return pl.pallas_call(
        functools.partial(rope_fwd_kernel, hd),
        grid=(seq // bm,),
        in_specs=[row(width), row(hd // 2), row(hd // 2), fix, fix],
        out_specs=[row(n_q * hd), row(hd), pl.BlockSpec((hd, bm), lambda i: (0, i)), pl.BlockSpec((hd, bm), lambda i: (0, i))],
        out_shape=[jax.ShapeDtypeStruct((seq, n_q * hd), BF16), jax.ShapeDtypeStruct((seq, hd), BF16)] + [jax.ShapeDtypeStruct((hd, seq), BF16)] * 2,
        cost_estimate=pl.CostEstimate(flops=20 * seq * width, bytes_accessed=4 * seq * width, transcendentals=0),
        name="rope_fwd",
    )(raw, cos, sin, gq, gk)


def rope_bwd_kernel(hd, raw_ref, dq0_ref, dq1_ref, dk_ref, dv_ref, cos_ref, sin_ref, gq_ref, gk_ref, out_ref, qt_ref, kt_ref, vt_ref, sq_ref, sk_ref):
    cos, sin = cos_ref[...], sin_ref[...]
    half = hd // 2
    n_q = dq0_ref.shape[1] // hd

    @pl.when(pl.program_id(0) == 0)
    def _():
        sq_ref[...] = jnp.zeros_like(sq_ref)
        sk_ref[...] = jnp.zeros_like(sk_ref)

    def load(refs, lo, hi):
        return jnp.concatenate([ref[:, lo:hi] for ref in refs], axis=0).astype(F32)

    def one(col, refs, dcol, gain, acc_ref, t_ref):
        da = load(refs, dcol, dcol + half)
        db = load(refs, dcol + half, dcol + hd)
        d = jnp.concatenate([da * cos + db * sin, db * cos - da * sin], axis=1)
        x = raw_ref[:, col:col + hd].astype(F32)
        r = lax.rsqrt(jnp.mean(x * x, axis=-1, keepdims=True) + EPS)
        xr = x * r
        acc_ref[...] += jnp.sum(d * xr, axis=0, keepdims=True)
        gd = d * (1.0 + gain)
        dx = r * (gd - xr * jnp.mean(xr * gd, axis=-1, keepdims=True))
        dx = dx.astype(BF16)
        out_ref[:, col:col + hd] = dx
        t_ref[0, dcol:dcol + hd, :] = dx.T

    for h in range(n_q):
        one(h * hd, (dq0_ref, dq1_ref), h * hd, gq_ref[...], sq_ref, qt_ref)
    one(n_q * hd, (dk_ref,), 0, gk_ref[...], sk_ref, kt_ref)
    out_ref[:, (n_q + 1) * hd:] = dv_ref[...]
    vt_ref[0] = dv_ref[...].T


def rope_bwd(raw, dq_halves, dk, dv, cos, sin, gq, gk, hd, n_q, bm):
    seq, width = raw.shape
    tall = lambda w: pl.BlockSpec((1, w, bm), lambda i: (i, 0, 0))
    tshape = lambda w: jax.ShapeDtypeStruct((seq // bm, w, bm), BF16)
    row = lambda w: pl.BlockSpec((bm, w), lambda i: (i, 0))
    fix = pl.BlockSpec((1, hd), lambda i: (0, 0))
    return pl.pallas_call(
        functools.partial(rope_bwd_kernel, hd),
        grid=(seq // bm,),
        in_specs=[row(width)] + [pl.BlockSpec((bm // 2, n_q * hd), lambda i: (i, 0))] * 2 + [row(hd), row(hd), row(hd // 2), row(hd // 2), fix, fix],
        out_specs=[row(width), tall(n_q * hd), tall(hd), tall(hd), fix, fix],
        out_shape=[jax.ShapeDtypeStruct((seq, width), BF16), tshape(n_q * hd), tshape(hd), tshape(hd), jax.ShapeDtypeStruct((1, hd), F32), jax.ShapeDtypeStruct((1, hd), F32)],
        cost_estimate=pl.CostEstimate(flops=30 * seq * width, bytes_accessed=6 * seq * width, transcendentals=0),
        name="rope_bwd",
    )(raw, *dq_halves, dk, dv, cos, sin, gq, gk)


BQ = 256
KB = 512
HALVES = 2


def stack_heads(blk, hd):
    return jnp.concatenate([blk[:, h * hd:(h + 1) * hd] for h in range(blk.shape[1] // hd)], axis=0)


def wide(blk, hd):
    return jnp.concatenate([blk[h * hd:(h + 1) * hd] for h in range(blk.shape[0] // hd)], axis=1)


def attn_fwd_kernel(hd, part, nkb_ref, lim_ref, q_ref, k_ref, vt_ref, o_ref, o32_ref, lse_ref, s_ref, p_ref):
    qb = HALVES * pl.program_id(0) + part
    coef = hd ** -0.5 * LOG2E
    n_q = q_ref.shape[1] // hd
    rows = n_q * BQ
    qt = stack_heads(q_ref[...], hd).T
    lim2 = jnp.concatenate([lim_ref[0]] * n_q, axis=1)
    n_full = (qb * BQ) // KB
    n_all = nkb_ref[qb]

    @pl.when(pl.program_id(0) == 0)
    def _():
        s_ref[:KB, :] = jnp.full((KB, rows), NEG_BIG, F32)

    def add_sum(m_prev, m, l, t):
        return l * jnp.exp2(m_prev - m) + jnp.sum(jnp.exp2(t.reshape(KB // 8, 8, rows) - m), axis=0)

    def body(masked, kb, stats):
        m_prev, m, l = stats
        pair = s_ref.at[pl.ds(pl.multiple_of(kb * KB, KB), 2 * KB)]
        l = add_sum(m_prev, m, l, pair[:KB])
        t = dot(k_ref[pl.ds(pl.multiple_of(kb * KB, KB), KB), :], qt) * coef
        if masked:
            key = kb * KB + lax.broadcasted_iota(jnp.int32, t.shape, 0)
            t = jnp.where(key <= lim2, t, NEG_BIG)
        pair[KB:] = t
        return m, jnp.maximum(m, jnp.max(t.reshape(KB // 8, 8, rows), axis=0)), l

    low = s_ref[:8, :]
    stats = lax.fori_loop(0, n_full, functools.partial(body, False), (low, low, jnp.zeros((8, rows), F32)))
    m_prev, m8, l8 = lax.fori_loop(n_full, n_all, functools.partial(body, True), stats)
    l8 = add_sum(m_prev, m8, l8, s_ref[pl.ds(pl.multiple_of(n_all * KB, KB), KB), :])
    m = jnp.max(m8, axis=0, keepdims=True)
    lse = m + jnp.log2(jnp.sum(l8 * jnp.exp2(m8 - m), axis=0, keepdims=True))

    def prob(kb):
        return jnp.exp2(s_ref[pl.ds(pl.multiple_of((kb + 1) * KB, KB), KB), :] - lse).astype(BF16)

    def pv(kb, p):
        return dot(vt_ref[:, pl.ds(pl.multiple_of(kb * KB, KB), KB)], p)

    p_ref[:KB] = prob(0)

    def pv_body(kb, acc):
        pair = p_ref.at[pl.ds(pl.multiple_of((kb - 1) * KB, KB), 2 * KB)]
        acc = acc + pv(kb - 1, pair[:KB])
        pair[KB:] = prob(kb)
        return acc

    acc = lax.fori_loop(1, n_all, pv_body, jnp.zeros((hd, rows), F32))
    acc = acc + pv(n_all - 1, p_ref[pl.ds(pl.multiple_of((n_all - 1) * KB, KB), KB), :])
    for h in range(n_q):
        part = acc[:, h * BQ:(h + 1) * BQ]
        o32_ref[0, h * hd:(h + 1) * hd, :] = part
        o_ref[0, h * hd:(h + 1) * hd, :] = part.astype(BF16)
    lse_ref[0] = jnp.broadcast_to(lse, (8, rows))


def attn_fwd(part, nkb, lim, q, k, vt, hd, n_dev):
    seq, width = q.shape
    n_q = width // hd
    tall = pl.BlockSpec((1, width, BQ), lambda i, *_: (i, 0, 0))
    at = lambda i, *_: HALVES * i + part
    return pl.pallas_call(
        functools.partial(attn_fwd_kernel, hd, part),
        grid_spec=pltpu.PrefetchScalarGridSpec(
            num_scalar_prefetch=1,
            grid=(n_dev,),
            in_specs=[pl.BlockSpec((1, 1, BQ), lambda i, *_: (at(i), 0, 0)), pl.BlockSpec((BQ, width), lambda i, *_: (at(i), 0)),
                      pl.BlockSpec((seq, hd), lambda i, *_: (0, 0)), pl.BlockSpec((hd, seq), lambda i, *_: (0, 0))],
            out_specs=[tall, tall, pl.BlockSpec((1, 8, n_q * BQ), lambda i, *_: (i, 0, 0))],
            scratch_shapes=[pltpu.VMEM((seq + KB, n_q * BQ), F32), pltpu.VMEM((seq, n_q * BQ), BF16)]),
        out_shape=[jax.ShapeDtypeStruct((n_dev, width, BQ), BF16), jax.ShapeDtypeStruct((n_dev, width, BQ), F32),
                   jax.ShapeDtypeStruct((n_dev, 8, n_q * BQ), F32)],
        cost_estimate=pl.CostEstimate(flops=int(1.1 * seq * seq * width), bytes_accessed=4 * seq * width, transcendentals=seq * seq),
        compiler_params=pltpu.CompilerParams(vmem_limit_bytes=40 * 1024 * 1024),
        name="attn_fwd",
    )(nkb, lim, q, k, vt)


def attn_bwd_kernel(hd, part, nkb_ref, lim_ref, q_ref, k_ref, kt_ref, v_ref, do_ref, o32_ref, lse_ref, *refs):
    step = pl.program_id(0)
    qb = HALVES * step + part
    scale = hd ** -0.5
    coef = scale * LOG2E
    n_q = q_ref.shape[1] // hd
    rows = n_q * BQ
    first, last = part == 0, part == HALVES - 1
    if not first:
        dk_in, dv_in, *refs = refs
    dq_ref, dk_ref, dv_ref, *refs = refs
    dk_acc, dv_acc = refs if last else (dk_ref, dv_ref)

    @pl.when(step == 0)
    def _():
        dk_acc[...] = jnp.zeros_like(dk_acc) if first else dk_in[...]
        dv_acc[...] = jnp.zeros_like(dv_acc) if first else dv_in[...]

    q2 = stack_heads(q_ref[...], hd)
    qt = q2.T
    dot_ = wide(do_ref[0], hd)
    do2 = dot_.T
    delta = jnp.sum(dot_.astype(F32) * wide(o32_ref[0], hd), axis=0, keepdims=True)
    lse = lse_ref[0][0:1, :]
    lim2 = jnp.concatenate([lim_ref[0]] * n_q, axis=1)
    n_full = (qb * BQ) // KB
    n_all = nkb_ref[qb]

    def body(masked, kb, dqt):
        keys = pl.ds(pl.multiple_of(kb * KB, KB), KB)
        st = dot(k_ref[keys, :], qt)
        pt = jnp.exp2(st * coef - lse)
        if masked:
            key = kb * KB + lax.broadcasted_iota(jnp.int32, st.shape, 0)
            pt = jnp.where(key <= lim2, pt, 0.0)
        dpt = dot(v_ref[keys, :], dot_)
        dst = (pt * (dpt - delta)).astype(BF16)
        dv_acc[keys, :] += dot(pt.astype(BF16), do2)
        dk_acc[keys, :] += dot(dst, q2)
        return dqt + dot(kt_ref[:, keys], dst)

    dqt = lax.fori_loop(0, n_full, functools.partial(body, False), jnp.zeros((hd, rows), F32))
    dqt = lax.fori_loop(n_full, n_all, functools.partial(body, True), dqt)
    dq = (dqt * scale).T.astype(BF16)
    for h in range(n_q):
        dq_ref[:, h * hd:(h + 1) * hd] = dq[h * BQ:(h + 1) * BQ]

    if last:
        @pl.when(step == pl.num_programs(0) - 1)
        def _():
            dk_ref[...] = (dk_acc[...] * scale).astype(BF16)
            dv_ref[...] = dv_acc[...].astype(BF16)


def attn_bwd(part, nkb, lim, q, k, kt, raw, d_o, o32, lse, carried, hd, n_dev):
    seq, width = q.shape
    n_q = width // hd
    v_col = raw.shape[1] // hd - 1
    at = lambda i, *_: HALVES * i + part
    tall = pl.BlockSpec((1, width, BQ), lambda i, *_: (i, 0, 0))
    whole = pl.BlockSpec((seq, hd), lambda i, *_: (0, 0))
    last = part == HALVES - 1
    acc_type = BF16 if last else F32
    return pl.pallas_call(
        functools.partial(attn_bwd_kernel, hd, part),
        grid_spec=pltpu.PrefetchScalarGridSpec(
            num_scalar_prefetch=1,
            grid=(n_dev,),
            in_specs=[pl.BlockSpec((1, 1, BQ), lambda i, *_: (at(i), 0, 0)), pl.BlockSpec((BQ, width), lambda i, *_: (at(i), 0)), whole,
                      pl.BlockSpec((hd, seq), lambda i, *_: (0, 0)), pl.BlockSpec((seq, hd), lambda i, *_: (0, v_col)), tall, tall,
                      pl.BlockSpec((1, 8, n_q * BQ), lambda i, *_: (i, 0, 0))] + [whole] * len(carried),
            out_specs=[pl.BlockSpec((BQ, width), lambda i, *_: (i, 0)), whole, whole],
            scratch_shapes=[pltpu.VMEM((seq, hd), F32)] * 2 if last else []),
        out_shape=[jax.ShapeDtypeStruct((n_dev * BQ, width), BF16), jax.ShapeDtypeStruct((seq, hd), acc_type), jax.ShapeDtypeStruct((seq, hd), acc_type)],
        cost_estimate=pl.CostEstimate(flops=int(2.7 * seq * seq * width), bytes_accessed=6 * seq * width, transcendentals=seq * seq),
        compiler_params=pltpu.CompilerParams(vmem_limit_bytes=56 * 1024 * 1024),
        name="attn_bwd",
    )(nkb, lim, q, k, kt, raw, d_o, o32, lse, *carried)


def split_kernel(n_dev, x_ref, *o_refs):
    width = x_ref.shape[1] // n_dev
    for g in range(n_dev):
        col = g * width
        for o_ref in o_refs:
            w = o_ref.shape[1] // n_dev
            o_ref[:, g * w:(g + 1) * w] = x_ref[:, col:col + w]
            col += w


def copy_kernel(x_ref, o_ref):
    o_ref[...] = x_ref[...]


def transpose_kernel(x_ref, o_ref):
    o_ref[...] = x_ref[...].T


def stream(body, x, in_spec, shapes, out_specs, grid):
    return pl.pallas_call(
        body,
        grid=(grid,),
        in_specs=[in_spec],
        out_specs=out_specs,
        out_shape=[jax.ShapeDtypeStruct(shape, x.dtype) for shape in shapes],
        cost_estimate=pl.CostEstimate(flops=x.size, bytes_accessed=4 * x.size, transcendentals=0),
        compiler_params=pltpu.CompilerParams(vmem_limit_bytes=40 * 1024 * 1024),
        name="copy_out",
    )(x)


def split_cols(x, n_dev, widths):
    bm = 256
    row = lambda w: pl.BlockSpec((bm, w), lambda i: (i, 0))
    return stream(functools.partial(split_kernel, n_dev), x, row(x.shape[1]), [(x.shape[0], w) for w in widths], [row(w) for w in widths], x.shape[0] // bm)


def copy_rows(x):
    spec = pl.BlockSpec((512, x.shape[1]), lambda i: (i, 0))
    return stream(copy_kernel, x, spec, [x.shape], [spec], x.shape[0] // 512)[0]


def transpose_rows(x):
    rows, cols = x.shape
    return stream(transpose_kernel, x, pl.BlockSpec((512, cols), lambda i: (i, 0)), [(cols, rows)], [pl.BlockSpec((cols, 512), lambda i: (0, i))], rows // 512)[0]


def solution(mesh):
    n_dev = mesh.shape['cp']
    seq_spec = P(('dp', 'cp'))
    part_spec = P('dp')
    rep_spec = P()

    def gather(x, axis=0):
        return lax.all_gather(x, 'cp', axis=axis, tiled=True)

    def exchange(x, after=None):
        if after is not None:
            x, _ = lax.optimization_barrier((x, after))
        return lax.all_to_all(x, 'cp', split_axis=0, concat_axis=0, tiled=True)

    def device_step(vis_loc, text_loc, img_pos, grad_y, pn_gain, w_proj, pre_gain, w_query, w_key, w_value, q_gain, k_gain, w_out, post_gain):
        rank = lax.axis_index('cp')
        seq_loc, d_model = text_loc.shape
        seq = seq_loc * n_dev
        img_loc, patches, dim_v = vis_loc.shape
        n_img = img_pos.shape[0]
        hd = q_gain.shape[0]
        wq_loc = w_query.shape[1] // n_dev
        wk_loc = w_key.shape[1] // n_dev
        n_q = wq_loc // hd
        pn32, pre32, post32 = pn_gain.astype(F32), pre_gain.astype(F32), post_gain.astype(F32)
        gq32 = q_gain.astype(F32)[None, :]
        gk32 = k_gain.astype(F32)[None, :]

        patch = jnp.arange(patches)
        patch_cell = (patch // (GRID * POOL)) * SIDE + (patch % GRID) // POOL
        pool_mat = (jnp.arange(BLOCK)[:, None] == patch_cell[None, :]).astype(BF16)
        pooled = jnp.einsum('cp,npd->ncd', pool_mat, vis_loc, preferred_element_type=F32) / (POOL * POOL)
        pooled = pooled.astype(BF16).reshape(img_loc * BLOCK, dim_v)
        normed, norm_pull = jax.vjp(gain_norm, pooled, pn32)
        normed_all = gather(normed)

        q_pos = rank * seq_loc + jnp.arange(seq_loc)
        offset = q_pos[:, None] - img_pos[None, :]
        in_blk = (offset >= 0) & (offset < BLOCK)
        is_img = jnp.any(in_blk, axis=1)
        img_mask = is_img[:, None]
        flat_row = jnp.sum(jnp.where(in_blk, jnp.arange(n_img)[None, :] * BLOCK + offset, 0), axis=1)
        flat_row = jnp.where(is_img, flat_row, -1)
        select = (flat_row[:, None] == jnp.arange(n_img * BLOCK)[None, :]).astype(BF16)
        all_pos = jnp.arange(seq)
        all_off = all_pos[:, None] - img_pos[None, :]
        all_in = (all_off >= 0) & (all_off < BLOCK)
        limit = (all_pos + jnp.sum(jnp.where(all_in, BLOCK - 1 - all_off, 0), axis=1)).astype(jnp.int32).reshape(seq // BQ, 1, BQ)
        n_kb = (jnp.max(limit, axis=(1, 2)) // KB + 1).astype(jnp.int32)
        all_flat = jnp.sum(jnp.where(all_in, jnp.arange(n_img)[None, :] * BLOCK + all_off + 1, 0), axis=1) - 1
        select_all = (all_flat[:, None] == jnp.arange(n_img * BLOCK)[None, :]).astype(BF16)

        normed_rows = dot(select, normed_all).astype(BF16)
        soft_rows = dot(normed_rows, w_proj).astype(BF16)
        merged = jnp.where(img_mask, soft_rows, text_loc)
        hidden, pre_pull = jax.vjp(gain_norm, merged, pre32)
        hidden_all = gather(hidden)

        w_qkv = jnp.concatenate([
            lax.dynamic_slice_in_dim(w_query, rank * wq_loc, wq_loc, 1),
            lax.dynamic_slice_in_dim(w_key, rank * wk_loc, wk_loc, 1),
            lax.dynamic_slice_in_dim(w_value, rank * wk_loc, wk_loc, 1)], axis=1)
        raw = dot(hidden_all, w_qkv).astype(BF16)
        cos_t, sin_t = rope_tables(seq, hd)
        q, k, kt, vt = rope_fwd(raw, cos_t, sin_t, gq32, gk32, hd, n_q)
        rows_of = lambda x, c: x[c * BQ:(c + 1) * BQ]
        fwd = []
        for c in range(HALVES):
            fwd.append(attn_fwd(c, n_kb, limit, q, k, vt, hd, n_dev))
        y_parts, d_o, d_proj_parts, g_post = [], [], [], 0.0
        attn_t = []
        for c in range(HALVES):
            attn_t.append(exchange(fwd[c][0], attn_t[-1] if c else None))
        prev = attn_t[-1]
        for c in range(HALVES):
            attn_c = attn_t[c]
            if c:
                attn_c, _ = lax.optimization_barrier((attn_c, d_attn_t))
            proj_out = dot_tn(attn_c.reshape(n_dev * wq_loc, BQ), w_out).astype(BF16)
            y_part, post_pull = jax.vjp(post_residual, rows_of(merged, c), proj_out, post32)
            _, d_proj, g_post_part = post_pull(rows_of(grad_y, c))
            d_attn_t = dot_nt(w_out, d_proj).astype(BF16).reshape(n_dev, wq_loc, BQ)
            y_parts.append(y_part)
            g_post = g_post + g_post_part
            prev = exchange(d_attn_t, prev)
            d_o.append(prev)
            d_proj_parts.append(gather(d_proj))
        y_loc = jnp.concatenate(y_parts, axis=0)

        dq_halves, carried = [], []
        for c in range(HALVES):
            dq, *carried = attn_bwd(c, n_kb, limit, q, k, kt, raw, d_o[c], fwd[c][1], fwd[c][2], carried, hd, n_dev)
            dq_halves.append(dq)
        dk, dv = carried
        d_qkv, dq_t, dk_t, dv_t, g_q_gain, g_k_gain = rope_bwd(raw, dq_halves, dk, dv, cos_t, sin_t, gq32, gk32, hd, n_q, seq_loc)

        g_qkv = dot_tn(hidden_all, d_qkv).astype(BF16)
        g_qkv = gather(g_qkv, 1)

        dq_seq = exchange(dq_t, prev)
        dk_seq = exchange(dk_t, dq_seq)
        dv_last = exchange(dv_t, dk_seq)
        dq_seq, dk_seq, dv_seq = [x.reshape(-1, seq_loc) for x in (dq_seq, dk_seq, dv_last)]
        d_hidden = sum(lax.dot_general(d, w, (((0,), (1,)), ((), ())), preferred_element_type=F32)
                       for d, w in ((dq_seq, w_query), (dk_seq, w_key), (dv_seq, w_value))).astype(BF16)
        d_merged_attn, g_pre = pre_pull(d_hidden)
        d_merged = (grad_y.astype(F32) + d_merged_attn.astype(F32)).astype(BF16)
        grad_text = jnp.where(img_mask, 0.0, d_merged).astype(BF16)

        d_soft_rows = jnp.where(img_mask, d_merged, 0.0).astype(BF16)
        d_normed_rows = dot_nt(d_soft_rows, w_proj).astype(BF16)
        d_normed_all = dot_tn(select, d_normed_rows).astype(BF16)
        d_normed = lax.psum_scatter(d_normed_all, 'cp', scatter_dimension=0, tiled=True)
        d_pooled, g_pn = norm_pull(d_normed)
        spread = (d_pooled.astype(F32) / (POOL * POOL)).astype(BF16).reshape(img_loc, SIDE, 1, SIDE, 1, dim_v)
        grad_vis = jnp.broadcast_to(spread, (img_loc, SIDE, POOL, SIDE, POOL, dim_v)).reshape(img_loc, patches, dim_v)

        d_soft_t = exchange(d_soft_rows.T.reshape(n_dev, d_model // n_dev, seq_loc), dv_last)
        normed_pos = dot(select_all, normed_all).astype(BF16).reshape(n_dev, seq_loc, dim_v)
        g_proj = sum(dot(d_soft_t[i], normed_pos[i]) for i in range(n_dev)).astype(BF16)
        g_proj = gather(g_proj)

        g_out = sum(dot_tn(fwd[c][0].transpose(0, 2, 1).reshape(-1, wq_loc), d_proj_parts[c]) for c in range(HALVES)).astype(BF16)
        g_out = gather(g_out)
        g_query, g_key, g_value = split_cols(g_qkv, n_dev, (n_dev * wq_loc, n_dev * wk_loc, n_dev * wk_loc))
        g_out = copy_rows(g_out)
        g_proj = transpose_rows(g_proj)
        small = lax.psum((g_pn, g_pre, g_q_gain[0], g_k_gain[0], g_post), 'cp')
        g_pn, g_pre, g_q_gain, g_k_gain, g_post = [part.astype(BF16) for part in small]
        return (y_loc, grad_text, grad_vis, g_pn, g_proj, g_pre, g_query, g_key, g_value, g_q_gain, g_k_gain, g_out, g_post)

    in_specs = (seq_spec, seq_spec, part_spec, seq_spec) + (rep_spec,) * 10
    out_specs = (seq_spec, seq_spec, seq_spec) + (part_spec,) * 10
    return jax.shard_map(device_step, mesh=mesh, in_specs=in_specs, out_specs=out_specs, check_vma=False)
```

```python
import functools
import math
import jax
import jax.numpy as jnp
from jax import lax
from jax.experimental import pallas as pl
from jax.experimental.pallas import tpu as pltpu
from jax.sharding import PartitionSpec as P

GRID = 64
POOL = 4
SIDE = GRID // POOL
BLOCK = SIDE * SIDE
EPS = 1e-6
ROPE_BASE = 1000000.0
ROPE_SCALE = 8.0
NEG_BIG = -1e30
F32 = jnp.float32
BF16 = jnp.bfloat16
LOG2E = math.log2(math.e)


def rms_scale(values, gain_vec):
    wide_vals = values.astype(F32)
    mean_sq = jnp.mean(wide_vals * wide_vals, axis=-1, keepdims=True)
    return wide_vals * lax.rsqrt(mean_sq + EPS) * (1.0 + gain_vec)


def gain_norm(values, gain_vec):
    return rms_scale(values, gain_vec).astype(BF16)


def post_residual(merged, proj_out, gain_vec):
    return (merged.astype(F32) + rms_scale(proj_out, gain_vec)).astype(BF16)


def dot(a, b):
    return jnp.dot(a, b, preferred_element_type=F32)


def dot_nt(a, b):
    return lax.dot_general(a, b, (((1,), (1,)), ((), ())), preferred_element_type=F32)


def dot_tn(a, b):
    return lax.dot_general(a, b, (((0,), (0,)), ((), ())), preferred_element_type=F32)


def rope_tables(seq, head_dim):
    inv_freq = ROPE_BASE ** (-jnp.arange(0, head_dim, 2).astype(F32) / head_dim)
    rot_angle = (jnp.arange(seq).astype(F32) / ROPE_SCALE)[:, None] * inv_freq[None, :]
    return jnp.cos(rot_angle), jnp.sin(rot_angle)


def rope_fwd_kernel(hd, raw_ref, cos_ref, sin_ref, gq_ref, gk_ref, q_ref, k_ref, kt_ref, vt_ref):
    cos, sin = cos_ref[...], sin_ref[...]
    half = hd // 2
    n_q = q_ref.shape[1] // hd

    def one(col, gain):
        x = raw_ref[:, col:col + hd].astype(F32)
        r = lax.rsqrt(jnp.mean(x * x, axis=-1, keepdims=True) + EPS)
        x = x * r * (1.0 + gain)
        a, b = x[:, :half], x[:, half:]
        return (a * cos - b * sin), (b * cos + a * sin)

    for h in range(n_q):
        a, b = one(h * hd, gq_ref[...])
        q_ref[:, h * hd:h * hd + half] = a.astype(BF16)
        q_ref[:, h * hd + half:(h + 1) * hd] = b.astype(BF16)
    a, b = one(n_q * hd, gk_ref[...])
    k_ref[:, :half] = a.astype(BF16)
    k_ref[:, half:] = b.astype(BF16)
    kt_ref[:half, :] = a.T.astype(BF16)
    kt_ref[half:, :] = b.T.astype(BF16)
    vt_ref[...] = raw_ref[:, (n_q + 1) * hd:].T


def rope_fwd(raw, cos, sin, gq, gk, hd, n_q):
    seq, width = raw.shape
    bm = 512
    row = lambda w: pl.BlockSpec((bm, w), lambda i: (i, 0))
    fix = pl.BlockSpec((1, hd), lambda i: (0, 0))
    return pl.pallas_call(
        functools.partial(rope_fwd_kernel, hd),
        grid=(seq // bm,),
        in_specs=[row(width), row(hd // 2), row(hd // 2), fix, fix],
        out_specs=[row(n_q * hd), row(hd), pl.BlockSpec((hd, bm), lambda i: (0, i)), pl.BlockSpec((hd, bm), lambda i: (0, i))],
        out_shape=[jax.ShapeDtypeStruct((seq, n_q * hd), BF16), jax.ShapeDtypeStruct((seq, hd), BF16)] + [jax.ShapeDtypeStruct((hd, seq), BF16)] * 2,
        cost_estimate=pl.CostEstimate(flops=20 * seq * width, bytes_accessed=4 * seq * width, transcendentals=0),
        name="rope_fwd",
    )(raw, cos, sin, gq, gk)


def rope_bwd_kernel(hd, raw_ref, dq0_ref, dq1_ref, dk_ref, dv_ref, cos_ref, sin_ref, gq_ref, gk_ref, out_ref, qt_ref, kt_ref, vt_ref, sq_ref, sk_ref):
    cos, sin = cos_ref[...], sin_ref[...]
    half = hd // 2
    n_q = dq0_ref.shape[1] // hd

    @pl.when(pl.program_id(0) == 0)
    def _():
        sq_ref[...] = jnp.zeros_like(sq_ref)
        sk_ref[...] = jnp.zeros_like(sk_ref)

    def load(refs, lo, hi):
        return jnp.concatenate([ref[:, lo:hi] for ref in refs], axis=0).astype(F32)

    def one(col, refs, dcol, gain, acc_ref, t_ref):
        da = load(refs, dcol, dcol + half)
        db = load(refs, dcol + half, dcol + hd)
        d = jnp.concatenate([da * cos + db * sin, db * cos - da * sin], axis=1)
        x = raw_ref[:, col:col + hd].astype(F32)
        r = lax.rsqrt(jnp.mean(x * x, axis=-1, keepdims=True) + EPS)
        xr = x * r
        acc_ref[...] += jnp.sum(d * xr, axis=0, keepdims=True)
        gd = d * (1.0 + gain)
        dx = r * (gd - xr * jnp.mean(xr * gd, axis=-1, keepdims=True))
        dx = dx.astype(BF16)
        out_ref[:, col:col + hd] = dx
        t_ref[0, dcol:dcol + hd, :] = dx.T

    for h in range(n_q):
        one(h * hd, (dq0_ref, dq1_ref), h * hd, gq_ref[...], sq_ref, qt_ref)
    one(n_q * hd, (dk_ref,), 0, gk_ref[...], sk_ref, kt_ref)
    out_ref[:, (n_q + 1) * hd:] = dv_ref[...]
    vt_ref[0] = dv_ref[...].T


def rope_bwd(raw, dq_halves, dk, dv, cos, sin, gq, gk, hd, n_q, bm):
    seq, width = raw.shape
    tall = lambda w: pl.BlockSpec((1, w, bm), lambda i: (i, 0, 0))
    tshape = lambda w: jax.ShapeDtypeStruct((seq // bm, w, bm), BF16)
    row = lambda w: pl.BlockSpec((bm, w), lambda i: (i, 0))
    fix = pl.BlockSpec((1, hd), lambda i: (0, 0))
    return pl.pallas_call(
        functools.partial(rope_bwd_kernel, hd),
        grid=(seq // bm,),
        in_specs=[row(width)] + [pl.BlockSpec((bm // 2, n_q * hd), lambda i: (i, 0))] * 2 + [row(hd), row(hd), row(hd // 2), row(hd // 2), fix, fix],
        out_specs=[row(width), tall(n_q * hd), tall(hd), tall(hd), fix, fix],
        out_shape=[jax.ShapeDtypeStruct((seq, width), BF16), tshape(n_q * hd), tshape(hd), tshape(hd), jax.ShapeDtypeStruct((1, hd), F32), jax.ShapeDtypeStruct((1, hd), F32)],
        cost_estimate=pl.CostEstimate(flops=30 * seq * width, bytes_accessed=6 * seq * width, transcendentals=0),
        name="rope_bwd",
    )(raw, *dq_halves, dk, dv, cos, sin, gq, gk)


BQ = 256
KB = 512
HALVES = 2


def stack_heads(blk, hd):
    return jnp.concatenate([blk[:, h * hd:(h + 1) * hd] for h in range(blk.shape[1] // hd)], axis=0)


def wide(blk, hd):
    return jnp.concatenate([blk[h * hd:(h + 1) * hd] for h in range(blk.shape[0] // hd)], axis=1)


def attn_fwd_kernel(hd, part, nkb_ref, lim_ref, q_ref, k_ref, vt_ref, o_ref, o32_ref, lse_ref, s_ref, p_ref, acc_ref):
    qb = HALVES * pl.program_id(0) + part
    coef = hd ** -0.5 * LOG2E
    n_q = q_ref.shape[1] // hd
    rows = n_q * BQ
    qt = stack_heads(q_ref[...], hd).T
    lim2 = jnp.concatenate([lim_ref[0]] * n_q, axis=1)
    n_full = (qb * BQ) // KB
    n_all = nkb_ref[qb]

    @pl.when(pl.program_id(0) == 0)
    def _():
        s_ref[:KB, :] = jnp.full((KB, rows), NEG_BIG, F32)

    def add_sum(m_prev, m, l, t):
        return l * jnp.exp2(m_prev - m) + jnp.sum(jnp.exp2(t.reshape(KB // 8, 8, rows) - m), axis=0)

    def body(masked, kb, stats):
        m_prev, m, l = stats
        pair = s_ref.at[pl.ds(pl.multiple_of(kb * KB, KB), 2 * KB)]
        l = add_sum(m_prev, m, l, pair[:KB])
        t = dot(k_ref[pl.ds(pl.multiple_of(kb * KB, KB), KB), :], qt) * coef
        if masked:
            key = kb * KB + lax.broadcasted_iota(jnp.int32, t.shape, 0)
            t = jnp.where(key <= lim2, t, NEG_BIG)
        pair[KB:] = t
        return m, jnp.maximum(m, jnp.max(t.reshape(KB // 8, 8, rows), axis=0)), l

    low = s_ref[:8, :]
    stats = lax.fori_loop(0, n_full, functools.partial(body, False), (low, low, jnp.zeros((8, rows), F32)))
    m_prev, m8, l8 = lax.fori_loop(n_full, n_all, functools.partial(body, True), stats)
    l8 = add_sum(m_prev, m8, l8, s_ref[pl.ds(pl.multiple_of(n_all * KB, KB), KB), :])
    m = jnp.max(m8, axis=0, keepdims=True)
    lse = m + jnp.log2(jnp.sum(l8 * jnp.exp2(m8 - m), axis=0, keepdims=True))

    def prob(kb):
        return jnp.exp2(s_ref[pl.ds(pl.multiple_of((kb + 1) * KB, KB), KB), :] - lse).astype(BF16)

    def pv(kb, p):
        return dot(vt_ref[:, pl.ds(pl.multiple_of(kb * KB, KB), KB)], p)

    p_ref[:KB] = prob(0)
    acc_ref[...] = jnp.zeros_like(acc_ref)

    def pv_body(kb, carry):
        pair = p_ref.at[pl.ds(pl.multiple_of((kb - 1) * KB, KB), 2 * KB)]
        acc_ref[...] += pv(kb - 1, pair[:KB])
        pair[KB:] = prob(kb)
        return carry

    lax.fori_loop(1, n_all, pv_body, 0)
    acc = acc_ref[...] + pv(n_all - 1, p_ref[pl.ds(pl.multiple_of((n_all - 1) * KB, KB), KB), :])
    for h in range(n_q):
        part = acc[:, h * BQ:(h + 1) * BQ]
        o32_ref[0, h * hd:(h + 1) * hd, :] = part
        o_ref[0, h * hd:(h + 1) * hd, :] = part.astype(BF16)
    lse_ref[0] = jnp.broadcast_to(lse, (8, rows))


def attn_fwd(part, nkb, lim, q, k, vt, hd, n_dev):
    seq, width = q.shape
    n_q = width // hd
    tall = pl.BlockSpec((1, width, BQ), lambda i, *_: (i, 0, 0))
    at = lambda i, *_: HALVES * i + part
    return pl.pallas_call(
        functools.partial(attn_fwd_kernel, hd, part),
        grid_spec=pltpu.PrefetchScalarGridSpec(
            num_scalar_prefetch=1,
            grid=(n_dev,),
            in_specs=[pl.BlockSpec((1, 1, BQ), lambda i, *_: (at(i), 0, 0)), pl.BlockSpec((BQ, width), lambda i, *_: (at(i), 0)),
                      pl.BlockSpec((seq, hd), lambda i, *_: (0, 0)), pl.BlockSpec((hd, seq), lambda i, *_: (0, 0))],
            out_specs=[tall, tall, pl.BlockSpec((1, 8, n_q * BQ), lambda i, *_: (i, 0, 0))],
            scratch_shapes=[pltpu.VMEM((seq + KB, n_q * BQ), F32), pltpu.VMEM((seq, n_q * BQ), BF16), pltpu.VMEM((hd, n_q * BQ), F32)]),
        out_shape=[jax.ShapeDtypeStruct((n_dev, width, BQ), BF16), jax.ShapeDtypeStruct((n_dev, width, BQ), F32),
                   jax.ShapeDtypeStruct((n_dev, 8, n_q * BQ), F32)],
        cost_estimate=pl.CostEstimate(flops=int(1.1 * seq * seq * width), bytes_accessed=4 * seq * width, transcendentals=seq * seq),
        compiler_params=pltpu.CompilerParams(vmem_limit_bytes=40 * 1024 * 1024),
        name="attn_fwd",
    )(nkb, lim, q, k, vt)


def attn_bwd_kernel(hd, part, nkb_ref, lim_ref, q_ref, k_ref, kt_ref, v_ref, do_ref, o32_ref, lse_ref, *refs):
    step = pl.program_id(0)
    qb = HALVES * step + part
    scale = hd ** -0.5
    coef = scale * LOG2E
    n_q = q_ref.shape[1] // hd
    rows = n_q * BQ
    first, last = part == 0, part == HALVES - 1
    if not first:
        dk_in, dv_in, *refs = refs
    dq_ref, dk_ref, dv_ref, *refs = refs
    dk_acc, dv_acc = refs if last else (dk_ref, dv_ref)

    @pl.when(step == 0)
    def _():
        dk_acc[...] = jnp.zeros_like(dk_acc) if first else dk_in[...]
        dv_acc[...] = jnp.zeros_like(dv_acc) if first else dv_in[...]

    q2 = stack_heads(q_ref[...], hd)
    qt = q2.T
    dot_ = wide(do_ref[0], hd)
    do2 = dot_.T
    delta = jnp.sum(dot_.astype(F32) * wide(o32_ref[0], hd), axis=0, keepdims=True)
    lse = lse_ref[0][0:1, :]
    lim2 = jnp.concatenate([lim_ref[0]] * n_q, axis=1)
    n_full = (qb * BQ) // KB
    n_all = nkb_ref[qb]

    def body(masked, kb, dqt):
        keys = pl.ds(pl.multiple_of(kb * KB, KB), KB)
        st = dot(k_ref[keys, :], qt)
        pt = jnp.exp2(st * coef - lse)
        if masked:
            key = kb * KB + lax.broadcasted_iota(jnp.int32, st.shape, 0)
            pt = jnp.where(key <= lim2, pt, 0.0)
        dpt = dot(v_ref[keys, :], dot_)
        dst = (pt * (dpt - delta)).astype(BF16)
        dv_acc[keys, :] += dot(pt.astype(BF16), do2)
        dk_acc[keys, :] += dot(dst, q2)
        return dqt + dot(kt_ref[:, keys], dst)

    dqt = lax.fori_loop(0, n_full, functools.partial(body, False), jnp.zeros((hd, rows), F32))
    dqt = lax.fori_loop(n_full, n_all, functools.partial(body, True), dqt)
    dq = (dqt * scale).T.astype(BF16)
    for h in range(n_q):
        dq_ref[:, h * hd:(h + 1) * hd] = dq[h * BQ:(h + 1) * BQ]

    if last:
        @pl.when(step == pl.num_programs(0) - 1)
        def _():
            dk_ref[...] = (dk_acc[...] * scale).astype(BF16)
            dv_ref[...] = dv_acc[...].astype(BF16)


def attn_bwd(part, nkb, lim, q, k, kt, raw, d_o, o32, lse, carried, hd, n_dev):
    seq, width = q.shape
    n_q = width // hd
    v_col = raw.shape[1] // hd - 1
    at = lambda i, *_: HALVES * i + part
    tall = pl.BlockSpec((1, width, BQ), lambda i, *_: (i, 0, 0))
    whole = pl.BlockSpec((seq, hd), lambda i, *_: (0, 0))
    last = part == HALVES - 1
    acc_type = BF16 if last else F32
    return pl.pallas_call(
        functools.partial(attn_bwd_kernel, hd, part),
        grid_spec=pltpu.PrefetchScalarGridSpec(
            num_scalar_prefetch=1,
            grid=(n_dev,),
            in_specs=[pl.BlockSpec((1, 1, BQ), lambda i, *_: (at(i), 0, 0)), pl.BlockSpec((BQ, width), lambda i, *_: (at(i), 0)), whole,
                      pl.BlockSpec((hd, seq), lambda i, *_: (0, 0)), pl.BlockSpec((seq, hd), lambda i, *_: (0, v_col)), tall, tall,
                      pl.BlockSpec((1, 8, n_q * BQ), lambda i, *_: (i, 0, 0))] + [whole] * len(carried),
            out_specs=[pl.BlockSpec((BQ, width), lambda i, *_: (i, 0)), whole, whole],
            scratch_shapes=[pltpu.VMEM((seq, hd), F32)] * 2 if last else []),
        out_shape=[jax.ShapeDtypeStruct((n_dev * BQ, width), BF16), jax.ShapeDtypeStruct((seq, hd), acc_type), jax.ShapeDtypeStruct((seq, hd), acc_type)],
        cost_estimate=pl.CostEstimate(flops=int(2.7 * seq * seq * width), bytes_accessed=6 * seq * width, transcendentals=seq * seq),
        compiler_params=pltpu.CompilerParams(vmem_limit_bytes=56 * 1024 * 1024),
        name="attn_bwd",
    )(nkb, lim, q, k, kt, raw, d_o, o32, lse, *carried)


def split_kernel(n_dev, x_ref, *o_refs):
    width = x_ref.shape[1] // n_dev
    for g in range(n_dev):
        col = g * width
        for o_ref in o_refs:
            w = o_ref.shape[1] // n_dev
            o_ref[:, g * w:(g + 1) * w] = x_ref[:, col:col + w]
            col += w


def copy_kernel(x_ref, o_ref):
    o_ref[...] = x_ref[...]


def transpose_kernel(x_ref, o_ref):
    o_ref[...] = x_ref[...].T


def stream(body, x, in_spec, shapes, out_specs, grid):
    return pl.pallas_call(
        body,
        grid=(grid,),
        in_specs=[in_spec],
        out_specs=out_specs,
        out_shape=[jax.ShapeDtypeStruct(shape, x.dtype) for shape in shapes],
        cost_estimate=pl.CostEstimate(flops=x.size, bytes_accessed=4 * x.size, transcendentals=0),
        compiler_params=pltpu.CompilerParams(vmem_limit_bytes=40 * 1024 * 1024),
        name="copy_out",
    )(x)


def split_cols(x, n_dev, widths):
    bm = 256
    row = lambda w: pl.BlockSpec((bm, w), lambda i: (i, 0))
    return stream(functools.partial(split_kernel, n_dev), x, row(x.shape[1]), [(x.shape[0], w) for w in widths], [row(w) for w in widths], x.shape[0] // bm)


def copy_rows(x):
    spec = pl.BlockSpec((512, x.shape[1]), lambda i: (i, 0))
    return stream(copy_kernel, x, spec, [x.shape], [spec], x.shape[0] // 512)[0]


def transpose_rows(x):
    rows, cols = x.shape
    return stream(transpose_kernel, x, pl.BlockSpec((512, cols), lambda i: (i, 0)), [(cols, rows)], [pl.BlockSpec((cols, 512), lambda i: (0, i))], rows // 512)[0]


def solution(mesh):
    n_dev = mesh.shape['cp']
    seq_spec = P(('dp', 'cp'))
    part_spec = P('dp')
    rep_spec = P()

    def gather(x, axis=0):
        return lax.all_gather(x, 'cp', axis=axis, tiled=True)

    def exchange(x, after=None):
        if after is not None:
            x, _ = lax.optimization_barrier((x, after))
        return lax.all_to_all(x, 'cp', split_axis=0, concat_axis=0, tiled=True)

    def reduce_to_owner(x, rank):
        bits = [rank // 4, (rank // 2) % 2, rank % 2]

        def halve(x, dim, bit):
            pick = lambda b: lax.dynamic_index_in_dim(x, b, dim, keepdims=False)
            got = lax.ppermute(pick(1 - bits[bit]), 'cp', [(i, i ^ (4 >> bit)) for i in range(n_dev)])
            return pick(bits[bit]) + got

        rows, cols = x.shape[0] // n_dev, x.shape[1]
        x = halve(x.reshape(2, 2, 2, rows, cols), 2, 2)
        cut = cols // 256 * 128
        first = halve(halve(x[..., :cut], 1, 1), 0, 0)
        second = halve(halve(x[..., cut:], 0, 0), 0, 1)
        return jnp.concatenate([first, second], axis=-1)

    def device_step(vis_loc, text_loc, img_pos, grad_y, pn_gain, w_proj, pre_gain, w_query, w_key, w_value, q_gain, k_gain, w_out, post_gain):
        rank = lax.axis_index('cp')
        seq_loc, d_model = text_loc.shape
        seq = seq_loc * n_dev
        img_loc, patches, dim_v = vis_loc.shape
        n_img = img_pos.shape[0]
        hd = q_gain.shape[0]
        wq_loc = w_query.shape[1] // n_dev
        wk_loc = w_key.shape[1] // n_dev
        n_q = wq_loc // hd
        pn32, pre32, post32 = pn_gain.astype(F32), pre_gain.astype(F32), post_gain.astype(F32)
        gq32 = q_gain.astype(F32)[None, :]
        gk32 = k_gain.astype(F32)[None, :]

        patch = jnp.arange(patches)
        patch_cell = (patch // (GRID * POOL)) * SIDE + (patch % GRID) // POOL
        pool_mat = (jnp.arange(BLOCK)[:, None] == patch_cell[None, :]).astype(BF16)
        pooled = jnp.einsum('cp,npd->ncd', pool_mat, vis_loc, preferred_element_type=F32) / (POOL * POOL)
        pooled = pooled.astype(BF16).reshape(img_loc * BLOCK, dim_v)
        normed, norm_pull = jax.vjp(gain_norm, pooled, pn32)
        normed_all = gather(normed)

        q_pos = rank * seq_loc + jnp.arange(seq_loc)
        offset = q_pos[:, None] - img_pos[None, :]
        in_blk = (offset >= 0) & (offset < BLOCK)
        is_img = jnp.any(in_blk, axis=1)
        img_mask = is_img[:, None]
        flat_row = jnp.sum(jnp.where(in_blk, jnp.arange(n_img)[None, :] * BLOCK + offset, 0), axis=1)
        flat_row = jnp.where(is_img, flat_row, -1)
        select = (flat_row[:, None] == jnp.arange(n_img * BLOCK)[None, :]).astype(BF16)
        all_pos = jnp.arange(seq)
        all_off = all_pos[:, None] - img_pos[None, :]
        all_in = (all_off >= 0) & (all_off < BLOCK)
        limit = (all_pos + jnp.sum(jnp.where(all_in, BLOCK - 1 - all_off, 0), axis=1)).astype(jnp.int32).reshape(seq // BQ, 1, BQ)
        n_kb = (jnp.max(limit, axis=(1, 2)) // KB + 1).astype(jnp.int32)
        all_flat = jnp.sum(jnp.where(all_in, jnp.arange(n_img)[None, :] * BLOCK + all_off + 1, 0), axis=1) - 1
        select_all = (all_flat[:, None] == jnp.arange(n_img * BLOCK)[None, :]).astype(BF16)

        normed_rows = dot(select, normed_all).astype(BF16)
        soft_rows = dot(normed_rows, w_proj).astype(BF16)
        merged = jnp.where(img_mask, soft_rows, text_loc)
        hidden, pre_pull = jax.vjp(gain_norm, merged, pre32)
        hidden_all = gather(hidden)

        w_qkv = jnp.concatenate([
            lax.dynamic_slice_in_dim(w_query, rank * wq_loc, wq_loc, 1),
            lax.dynamic_slice_in_dim(w_key, rank * wk_loc, wk_loc, 1),
            lax.dynamic_slice_in_dim(w_value, rank * wk_loc, wk_loc, 1)], axis=1)
        raw = dot(hidden_all, w_qkv).astype(BF16)
        cos_t, sin_t = rope_tables(seq, hd)
        q, k, kt, vt = rope_fwd(raw, cos_t, sin_t, gq32, gk32, hd, n_q)
        rows_of = lambda x, c: x[c * BQ:(c + 1) * BQ]
        fwd = []
        for c in range(HALVES):
            fwd.append(attn_fwd(c, n_kb, limit, q, k, vt, hd, n_dev))
        y_parts, d_o, d_proj_parts, g_post = [], [], [], 0.0
        attn_t = []
        for c in range(HALVES):
            attn_t.append(exchange(fwd[c][0], attn_t[-1] if c else None))
        prev = attn_t[-1]
        for c in range(HALVES):
            attn_c = attn_t[c]
            if c:
                attn_c, _ = lax.optimization_barrier((attn_c, d_attn_t))
            proj_out = dot_tn(attn_c.reshape(n_dev * wq_loc, BQ), w_out).astype(BF16)
            y_part, post_pull = jax.vjp(post_residual, rows_of(merged, c), proj_out, post32)
            _, d_proj, g_post_part = post_pull(rows_of(grad_y, c))
            d_attn_t = dot_nt(w_out, d_proj).astype(BF16).reshape(n_dev, wq_loc, BQ)
            y_parts.append(y_part)
            g_post = g_post + g_post_part
            prev = exchange(d_attn_t, prev)
            d_o.append(prev)
            d_proj_parts.append(gather(d_proj))
        y_loc = jnp.concatenate(y_parts, axis=0)

        dq_halves, carried = [], []
        for c in range(HALVES):
            dq, *carried = attn_bwd(c, n_kb, limit, q, k, kt, raw, d_o[c], fwd[c][1], fwd[c][2], carried, hd, n_dev)
            dq_halves.append(dq)
        dk, dv = carried
        d_qkv, dq_t, dk_t, dv_t, g_q_gain, g_k_gain = rope_bwd(raw, dq_halves, dk, dv, cos_t, sin_t, gq32, gk32, hd, n_q, seq_loc)

        g_qkv = dot_tn(hidden_all, d_qkv).astype(BF16)
        g_qkv = gather(g_qkv, 1)

        dq_seq = exchange(dq_t, prev)
        dk_seq = exchange(dk_t, dq_seq)
        dv_last = exchange(dv_t, dk_seq)
        dq_seq, dk_seq, dv_seq = [x.reshape(-1, seq_loc) for x in (dq_seq, dk_seq, dv_last)]
        d_hidden = sum(lax.dot_general(d, w, (((0,), (1,)), ((), ())), preferred_element_type=F32)
                       for d, w in ((dq_seq, w_query), (dk_seq, w_key), (dv_seq, w_value))).astype(BF16)
        d_merged_attn, g_pre = pre_pull(d_hidden)
        d_merged = (grad_y.astype(F32) + d_merged_attn.astype(F32)).astype(BF16)
        grad_text = jnp.where(img_mask, 0.0, d_merged).astype(BF16)

        d_soft_rows = jnp.where(img_mask, d_merged, 0.0).astype(BF16)
        d_normed_rows = dot_nt(d_soft_rows, w_proj).astype(BF16)
        d_normed_all = dot_tn(select, d_normed_rows).astype(BF16)
        d_normed = reduce_to_owner(d_normed_all, rank)
        d_pooled, g_pn = norm_pull(d_normed)
        spread = (d_pooled.astype(F32) / (POOL * POOL)).astype(BF16).reshape(img_loc, SIDE, 1, SIDE, 1, dim_v)
        grad_vis = jnp.broadcast_to(spread, (img_loc, SIDE, POOL, SIDE, POOL, dim_v)).reshape(img_loc, patches, dim_v)

        d_soft_t = exchange(d_soft_rows.T.reshape(n_dev, d_model // n_dev, seq_loc), dv_last)
        normed_pos = dot(select_all, normed_all).astype(BF16).reshape(n_dev, seq_loc, dim_v)
        g_proj = sum(dot(d_soft_t[i], normed_pos[i]) for i in range(n_dev)).astype(BF16)
        g_proj = gather(g_proj)

        g_out = sum(dot_tn(fwd[c][0].transpose(0, 2, 1).reshape(-1, wq_loc), d_proj_parts[c]) for c in range(HALVES)).astype(BF16)
        g_out = gather(g_out)
        g_query, g_key, g_value = split_cols(g_qkv, n_dev, (n_dev * wq_loc, n_dev * wk_loc, n_dev * wk_loc))
        g_out = copy_rows(g_out)
        g_proj = transpose_rows(g_proj)
        small = lax.psum((g_pn, g_pre, g_q_gain[0], g_k_gain[0], g_post), 'cp')
        g_pn, g_pre, g_q_gain, g_k_gain, g_post = [part.astype(BF16) for part in small]
        return (y_loc, grad_text, grad_vis, g_pn, g_proj, g_pre, g_query, g_key, g_value, g_q_gain, g_k_gain, g_out, g_post)

    in_specs = (seq_spec, seq_spec, part_spec, seq_spec) + (rep_spec,) * 10
    out_specs = (seq_spec, seq_spec, seq_spec) + (part_spec,) * 10
    return jax.shard_map(device_step, mesh=mesh, in_specs=in_specs, out_specs=out_specs, check_vma=False)
```

```python
import functools
import math
import jax
import jax.numpy as jnp
from jax import lax
from jax.experimental import pallas as pl
from jax.experimental.pallas import tpu as pltpu
from jax.sharding import PartitionSpec as P

GRID = 64
POOL = 4
SIDE = GRID // POOL
BLOCK = SIDE * SIDE
EPS = 1e-6
ROPE_BASE = 1000000.0
ROPE_SCALE = 8.0
NEG_BIG = -1e30
F32 = jnp.float32
BF16 = jnp.bfloat16
LOG2E = math.log2(math.e)


def rms_scale(values, gain_vec):
    wide_vals = values.astype(F32)
    mean_sq = jnp.mean(wide_vals * wide_vals, axis=-1, keepdims=True)
    return wide_vals * lax.rsqrt(mean_sq + EPS) * (1.0 + gain_vec)


def gain_norm(values, gain_vec):
    return rms_scale(values, gain_vec).astype(BF16)


def post_residual(merged, proj_out, gain_vec):
    return (merged.astype(F32) + rms_scale(proj_out, gain_vec)).astype(BF16)


def dot(a, b):
    return jnp.dot(a, b, preferred_element_type=F32)


def dot_nt(a, b):
    return lax.dot_general(a, b, (((1,), (1,)), ((), ())), preferred_element_type=F32)


def dot_tn(a, b):
    return lax.dot_general(a, b, (((0,), (0,)), ((), ())), preferred_element_type=F32)


def rope_tables(seq, head_dim):
    inv_freq = ROPE_BASE ** (-jnp.arange(0, head_dim, 2).astype(F32) / head_dim)
    rot_angle = (jnp.arange(seq).astype(F32) / ROPE_SCALE)[:, None] * inv_freq[None, :]
    return jnp.cos(rot_angle), jnp.sin(rot_angle)


def rope_fwd_kernel(hd, raw_ref, cos_ref, sin_ref, gq_ref, gk_ref, q_ref, k_ref, kt_ref, vt_ref):
    cos, sin = cos_ref[...], sin_ref[...]
    half = hd // 2
    n_q = q_ref.shape[1] // hd

    def one(col, gain):
        x = raw_ref[:, col:col + hd].astype(F32)
        r = lax.rsqrt(jnp.mean(x * x, axis=-1, keepdims=True) + EPS)
        x = x * r * (1.0 + gain)
        a, b = x[:, :half], x[:, half:]
        return (a * cos - b * sin), (b * cos + a * sin)

    for h in range(n_q):
        a, b = one(h * hd, gq_ref[...])
        q_ref[:, h * hd:h * hd + half] = a.astype(BF16)
        q_ref[:, h * hd + half:(h + 1) * hd] = b.astype(BF16)
    a, b = one(n_q * hd, gk_ref[...])
    k_ref[:, :half] = a.astype(BF16)
    k_ref[:, half:] = b.astype(BF16)
    kt_ref[:half, :] = a.T.astype(BF16)
    kt_ref[half:, :] = b.T.astype(BF16)
    vt_ref[...] = raw_ref[:, (n_q + 1) * hd:].T


def rope_fwd(raw, cos, sin, gq, gk, hd, n_q):
    seq, width = raw.shape
    bm = 512
    row = lambda w: pl.BlockSpec((bm, w), lambda i: (i, 0))
    fix = pl.BlockSpec((1, hd), lambda i: (0, 0))
    return pl.pallas_call(
        functools.partial(rope_fwd_kernel, hd),
        grid=(seq // bm,),
        in_specs=[row(width), row(hd // 2), row(hd // 2), fix, fix],
        out_specs=[row(n_q * hd), row(hd), pl.BlockSpec((hd, bm), lambda i: (0, i)), pl.BlockSpec((hd, bm), lambda i: (0, i))],
        out_shape=[jax.ShapeDtypeStruct((seq, n_q * hd), BF16), jax.ShapeDtypeStruct((seq, hd), BF16)] + [jax.ShapeDtypeStruct((hd, seq), BF16)] * 2,
        cost_estimate=pl.CostEstimate(flops=20 * seq * width, bytes_accessed=4 * seq * width, transcendentals=0),
        name="rope_fwd",
    )(raw, cos, sin, gq, gk)


def rope_bwd_kernel(hd, raw_ref, dq0_ref, dq1_ref, dk_ref, cos_ref, sin_ref, gq_ref, gk_ref, q_ref, k_ref, qt_ref, sq_ref, sk_ref):
    cos, sin = cos_ref[...], sin_ref[...]
    half = hd // 2
    n_q = dq0_ref.shape[1] // hd

    @pl.when(pl.program_id(0) == 0)
    def _():
        sq_ref[...] = jnp.zeros_like(sq_ref)
        sk_ref[...] = jnp.zeros_like(sk_ref)

    def load(refs, lo, hi):
        return jnp.concatenate([ref[:, lo:hi] for ref in refs], axis=0).astype(F32)

    def one(col, refs, dcol, gain, acc_ref, out_ref, t_ref=None):
        da = load(refs, dcol, dcol + half)
        db = load(refs, dcol + half, dcol + hd)
        d = jnp.concatenate([da * cos + db * sin, db * cos - da * sin], axis=1)
        x = raw_ref[:, col:col + hd].astype(F32)
        r = lax.rsqrt(jnp.mean(x * x, axis=-1, keepdims=True) + EPS)
        xr = x * r
        acc_ref[...] += jnp.sum(d * xr, axis=0, keepdims=True)
        gd = d * (1.0 + gain)
        dx = r * (gd - xr * jnp.mean(xr * gd, axis=-1, keepdims=True))
        dx = dx.astype(BF16)
        out_ref[:, dcol:dcol + hd] = dx
        if t_ref is not None:
            t_ref[0, dcol:dcol + hd, :] = dx.T

    for h in range(n_q):
        one(h * hd, (dq0_ref, dq1_ref), h * hd, gq_ref[...], sq_ref, q_ref, qt_ref)
    one(n_q * hd, (dk_ref,), 0, gk_ref[...], sk_ref, k_ref)


def rope_bwd(raw, dq_halves, dk, cos, sin, gq, gk, hd, n_q, bm):
    seq, width = raw.shape
    tall = lambda w: pl.BlockSpec((1, w, bm), lambda i: (i, 0, 0))
    tshape = lambda w: jax.ShapeDtypeStruct((seq // bm, w, bm), BF16)
    row = lambda w: pl.BlockSpec((bm, w), lambda i: (i, 0))
    fix = pl.BlockSpec((1, hd), lambda i: (0, 0))
    return pl.pallas_call(
        functools.partial(rope_bwd_kernel, hd),
        grid=(seq // bm,),
        in_specs=[row(width)] + [pl.BlockSpec((bm // 2, n_q * hd), lambda i: (i, 0))] * 2 + [row(hd), row(hd // 2), row(hd // 2), fix, fix],
        out_specs=[row(n_q * hd), row(hd), tall(n_q * hd), fix, fix],
        out_shape=[jax.ShapeDtypeStruct((seq, n_q * hd), BF16), jax.ShapeDtypeStruct((seq, hd), BF16), tshape(n_q * hd), jax.ShapeDtypeStruct((1, hd), F32), jax.ShapeDtypeStruct((1, hd), F32)],
        cost_estimate=pl.CostEstimate(flops=30 * seq * width, bytes_accessed=6 * seq * width, transcendentals=0),
        name="rope_bwd",
    )(raw, *dq_halves, dk, cos, sin, gq, gk)


BQ = 256
KB = 512
HALVES = 2


def stack_heads(blk, hd):
    return jnp.concatenate([blk[:, h * hd:(h + 1) * hd] for h in range(blk.shape[1] // hd)], axis=0)


def wide(blk, hd):
    return jnp.concatenate([blk[h * hd:(h + 1) * hd] for h in range(blk.shape[0] // hd)], axis=1)


def attn_fwd_kernel(hd, part, nkb_ref, lim_ref, q_ref, k_ref, vt_ref, o_ref, o32_ref, lse_ref, s_ref, p_ref, acc_ref):
    qb = HALVES * pl.program_id(0) + part
    coef = hd ** -0.5 * LOG2E
    n_q = q_ref.shape[1] // hd
    rows = n_q * BQ
    qt = stack_heads(q_ref[...], hd).T
    lim2 = jnp.concatenate([lim_ref[0]] * n_q, axis=1)
    n_full = (qb * BQ) // KB
    n_all = nkb_ref[qb]

    @pl.when(pl.program_id(0) == 0)
    def _():
        s_ref[:KB, :] = jnp.full((KB, rows), NEG_BIG, F32)

    def add_sum(m_prev, m, l, t):
        return l * jnp.exp2(m_prev - m) + jnp.sum(jnp.exp2(t.reshape(KB // 8, 8, rows) - m), axis=0)

    def body(masked, kb, stats):
        m_prev, m, l = stats
        pair = s_ref.at[pl.ds(pl.multiple_of(kb * KB, KB), 2 * KB)]
        l = add_sum(m_prev, m, l, pair[:KB])
        t = dot(k_ref[pl.ds(pl.multiple_of(kb * KB, KB), KB), :], qt) * coef
        if masked:
            key = kb * KB + lax.broadcasted_iota(jnp.int32, t.shape, 0)
            t = jnp.where(key <= lim2, t, NEG_BIG)
        pair[KB:] = t
        return m, jnp.maximum(m, jnp.max(t.reshape(KB // 8, 8, rows), axis=0)), l

    low = s_ref[:8, :]
    stats = lax.fori_loop(0, n_full, functools.partial(body, False), (low, low, jnp.zeros((8, rows), F32)))
    m_prev, m8, l8 = lax.fori_loop(n_full, n_all, functools.partial(body, True), stats)
    l8 = add_sum(m_prev, m8, l8, s_ref[pl.ds(pl.multiple_of(n_all * KB, KB), KB), :])
    m = jnp.max(m8, axis=0, keepdims=True)
    lse = m + jnp.log2(jnp.sum(l8 * jnp.exp2(m8 - m), axis=0, keepdims=True))

    def prob(kb):
        return jnp.exp2(s_ref[pl.ds(pl.multiple_of((kb + 1) * KB, KB), KB), :] - lse).astype(BF16)

    def pv(kb, p):
        return dot(vt_ref[:, pl.ds(pl.multiple_of(kb * KB, KB), KB)], p)

    p_ref[:KB] = prob(0)
    acc_ref[...] = jnp.zeros_like(acc_ref)

    def pv_body(kb, carry):
        pair = p_ref.at[pl.ds(pl.multiple_of((kb - 1) * KB, KB), 2 * KB)]
        acc_ref[...] += pv(kb - 1, pair[:KB])
        pair[KB:] = prob(kb)
        return carry

    lax.fori_loop(1, n_all, pv_body, 0)
    acc = acc_ref[...] + pv(n_all - 1, p_ref[pl.ds(pl.multiple_of((n_all - 1) * KB, KB), KB), :])
    for h in range(n_q):
        part = acc[:, h * BQ:(h + 1) * BQ]
        o32_ref[0, h * hd:(h + 1) * hd, :] = part
        o_ref[0, h * hd:(h + 1) * hd, :] = part.astype(BF16)
    lse_ref[0] = jnp.broadcast_to(lse, (8, rows))


def attn_fwd(part, nkb, lim, q, k, vt, hd, n_dev):
    seq, width = q.shape
    n_q = width // hd
    tall = pl.BlockSpec((1, width, BQ), lambda i, *_: (i, 0, 0))
    at = lambda i, *_: HALVES * i + part
    return pl.pallas_call(
        functools.partial(attn_fwd_kernel, hd, part),
        grid_spec=pltpu.PrefetchScalarGridSpec(
            num_scalar_prefetch=1,
            grid=(n_dev,),
            in_specs=[pl.BlockSpec((1, 1, BQ), lambda i, *_: (at(i), 0, 0)), pl.BlockSpec((BQ, width), lambda i, *_: (at(i), 0)),
                      pl.BlockSpec((seq, hd), lambda i, *_: (0, 0)), pl.BlockSpec((hd, seq), lambda i, *_: (0, 0))],
            out_specs=[tall, tall, pl.BlockSpec((1, 8, n_q * BQ), lambda i, *_: (i, 0, 0))],
            scratch_shapes=[pltpu.VMEM((seq + KB, n_q * BQ), F32), pltpu.VMEM((seq, n_q * BQ), BF16), pltpu.VMEM((hd, n_q * BQ), F32)]),
        out_shape=[jax.ShapeDtypeStruct((n_dev, width, BQ), BF16), jax.ShapeDtypeStruct((n_dev, width, BQ), F32),
                   jax.ShapeDtypeStruct((n_dev, 8, n_q * BQ), F32)],
        cost_estimate=pl.CostEstimate(flops=int(1.1 * seq * seq * width), bytes_accessed=4 * seq * width, transcendentals=seq * seq),
        compiler_params=pltpu.CompilerParams(vmem_limit_bytes=40 * 1024 * 1024),
        name="attn_fwd",
    )(nkb, lim, q, k, vt)


def attn_bwd_kernel(hd, part, nkb_ref, lim_ref, q_ref, k_ref, kt_ref, v_ref, do_ref, o32_ref, lse_ref, *refs):
    step = pl.program_id(0)
    qb = HALVES * step + part
    scale = hd ** -0.5
    coef = scale * LOG2E
    n_q = q_ref.shape[1] // hd
    rows = n_q * BQ
    first, last = part == 0, part == HALVES - 1
    if not first:
        dk_in, dv_in, *refs = refs
    dq_ref, dk_ref, dv_ref, *refs = refs
    dk_acc, dv_acc = refs if last else (dk_ref, dv_ref)

    @pl.when(step == 0)
    def _():
        dk_acc[...] = jnp.zeros_like(dk_acc) if first else dk_in[...]
        dv_acc[...] = jnp.zeros_like(dv_acc) if first else dv_in[...]

    q2 = stack_heads(q_ref[...], hd)
    qt = q2.T
    dot_ = wide(do_ref[0], hd)
    do2 = dot_.T
    delta = jnp.sum(dot_.astype(F32) * wide(o32_ref[0], hd), axis=0, keepdims=True)
    lse = lse_ref[0][0:1, :]
    lim2 = jnp.concatenate([lim_ref[0]] * n_q, axis=1)
    n_full = (qb * BQ) // KB
    n_all = nkb_ref[qb]

    def body(masked, kb, dqt):
        keys = pl.ds(pl.multiple_of(kb * KB, KB), KB)
        st = dot(k_ref[keys, :], qt)
        pt = jnp.exp2(st * coef - lse)
        if masked:
            key = kb * KB + lax.broadcasted_iota(jnp.int32, st.shape, 0)
            pt = jnp.where(key <= lim2, pt, 0.0)
        dpt = dot(v_ref[keys, :], dot_)
        dst = (pt * (dpt - delta)).astype(BF16)
        dv_acc[keys, :] += dot(pt.astype(BF16), do2)
        dk_acc[keys, :] += dot(dst, q2)
        return dqt + dot(kt_ref[:, keys], dst)

    dqt = lax.fori_loop(0, n_full, functools.partial(body, False), jnp.zeros((hd, rows), F32))
    dqt = lax.fori_loop(n_full, n_all, functools.partial(body, True), dqt)
    dq = (dqt * scale).T.astype(BF16)
    for h in range(n_q):
        dq_ref[:, h * hd:(h + 1) * hd] = dq[h * BQ:(h + 1) * BQ]

    if last:
        @pl.when(step == pl.num_programs(0) - 1)
        def _():
            dk_ref[...] = (dk_acc[...] * scale).astype(BF16)
            dv_ref[...] = dv_acc[...].astype(BF16)


def attn_bwd(part, nkb, lim, q, k, kt, raw, d_o, o32, lse, carried, hd, n_dev):
    seq, width = q.shape
    n_q = width // hd
    v_col = raw.shape[1] // hd - 1
    at = lambda i, *_: HALVES * i + part
    tall = pl.BlockSpec((1, width, BQ), lambda i, *_: (i, 0, 0))
    whole = pl.BlockSpec((seq, hd), lambda i, *_: (0, 0))
    last = part == HALVES - 1
    acc_type = BF16 if last else F32
    return pl.pallas_call(
        functools.partial(attn_bwd_kernel, hd, part),
        grid_spec=pltpu.PrefetchScalarGridSpec(
            num_scalar_prefetch=1,
            grid=(n_dev,),
            in_specs=[pl.BlockSpec((1, 1, BQ), lambda i, *_: (at(i), 0, 0)), pl.BlockSpec((BQ, width), lambda i, *_: (at(i), 0)), whole,
                      pl.BlockSpec((hd, seq), lambda i, *_: (0, 0)), pl.BlockSpec((seq, hd), lambda i, *_: (0, v_col)), tall, tall,
                      pl.BlockSpec((1, 8, n_q * BQ), lambda i, *_: (i, 0, 0))] + [whole] * len(carried),
            out_specs=[pl.BlockSpec((BQ, width), lambda i, *_: (i, 0)), whole, whole],
            scratch_shapes=[pltpu.VMEM((seq, hd), F32)] * 2 if last else []),
        out_shape=[jax.ShapeDtypeStruct((n_dev * BQ, width), BF16), jax.ShapeDtypeStruct((seq, hd), acc_type), jax.ShapeDtypeStruct((seq, hd), acc_type)],
        cost_estimate=pl.CostEstimate(flops=int(2.7 * seq * seq * width), bytes_accessed=6 * seq * width, transcendentals=seq * seq),
        compiler_params=pltpu.CompilerParams(vmem_limit_bytes=56 * 1024 * 1024),
        name="attn_bwd",
    )(nkb, lim, q, k, kt, raw, d_o, o32, lse, *carried)


def copy_kernel(x_ref, o_ref):
    o_ref[...] = x_ref[...]


def transpose_kernel(x_ref, o_ref):
    o_ref[...] = x_ref[...].T


def stream(body, x, in_spec, shapes, out_specs, grid):
    return pl.pallas_call(
        body,
        grid=(grid,),
        in_specs=[in_spec],
        out_specs=out_specs,
        out_shape=[jax.ShapeDtypeStruct(shape, x.dtype) for shape in shapes],
        cost_estimate=pl.CostEstimate(flops=x.size, bytes_accessed=4 * x.size, transcendentals=0),
        compiler_params=pltpu.CompilerParams(vmem_limit_bytes=40 * 1024 * 1024),
        name="copy_out",
    )(x)


def copy_rows(x):
    spec = pl.BlockSpec((512, x.shape[1]), lambda i: (i, 0))
    return stream(copy_kernel, x, spec, [x.shape], [spec], x.shape[0] // 512)[0]


def spread_kernel(x_ref, o_ref):
    cell, col = (lax.broadcasted_iota(jnp.int32, (GRID, SIDE), d) for d in (0, 1))
    y = dot((cell // POOL == col).astype(BF16), x_ref[...]).astype(BF16)
    for t in range(POOL):
        o_ref[t * GRID:(t + 1) * GRID, :] = y


def spread_rows(x):
    cols = x.shape[1]
    step = GRID * POOL
    n = x.shape[0] // SIDE
    return stream(spread_kernel, x, pl.BlockSpec((SIDE, cols), lambda i: (i, 0)), [(n * step, cols)], [pl.BlockSpec((step, cols), lambda i: (i, 0))], n)[0]


def transpose_rows(x):
    rows, cols = x.shape
    return stream(transpose_kernel, x, pl.BlockSpec((512, cols), lambda i: (i, 0)), [(cols, rows)], [pl.BlockSpec((cols, 512), lambda i: (0, i))], rows // 512)[0]


def solution(mesh):
    n_dev = mesh.shape['cp']
    seq_spec = P(('dp', 'cp'))
    part_spec = P('dp')
    rep_spec = P()

    def gather(x, axis=0):
        return lax.all_gather(x, 'cp', axis=axis, tiled=True)

    def exchange(x, after=None):
        if after is not None:
            x, _ = lax.optimization_barrier((x, after))
        return lax.all_to_all(x, 'cp', split_axis=0, concat_axis=0, tiled=True)

    def reduce_to_owner(x, rank):
        bits = [rank // 4, (rank // 2) % 2, rank % 2]

        def halve(x, dim, bit):
            pick = lambda b: lax.dynamic_index_in_dim(x, b, dim, keepdims=False)
            got = lax.ppermute(pick(1 - bits[bit]), 'cp', [(i, i ^ (4 >> bit)) for i in range(n_dev)])
            return pick(bits[bit]) + got

        rows, cols = x.shape[0] // n_dev, x.shape[1]
        x = halve(x.reshape(2, 2, 2, rows, cols), 2, 2)
        cut = cols // 256 * 128
        first = halve(halve(x[..., :cut], 1, 1), 0, 0)
        second = halve(halve(x[..., cut:], 0, 0), 0, 1)
        return jnp.concatenate([first, second], axis=-1)

    def device_step(vis_loc, text_loc, img_pos, grad_y, pn_gain, w_proj, pre_gain, w_query, w_key, w_value, q_gain, k_gain, w_out, post_gain):
        rank = lax.axis_index('cp')
        seq_loc, d_model = text_loc.shape
        seq = seq_loc * n_dev
        img_loc, patches, dim_v = vis_loc.shape
        n_img = img_pos.shape[0]
        hd = q_gain.shape[0]
        wq_loc = w_query.shape[1] // n_dev
        wk_loc = w_key.shape[1] // n_dev
        n_q = wq_loc // hd
        pn32, pre32, post32 = pn_gain.astype(F32), pre_gain.astype(F32), post_gain.astype(F32)
        gq32 = q_gain.astype(F32)[None, :]
        gk32 = k_gain.astype(F32)[None, :]

        patch = jnp.arange(patches)
        patch_cell = (patch // (GRID * POOL)) * SIDE + (patch % GRID) // POOL
        pool_mat = (jnp.arange(BLOCK)[:, None] == patch_cell[None, :]).astype(BF16)
        pooled = jnp.einsum('cp,npd->ncd', pool_mat, vis_loc, preferred_element_type=F32) / (POOL * POOL)
        pooled = pooled.astype(BF16).reshape(img_loc * BLOCK, dim_v)
        normed, norm_pull = jax.vjp(gain_norm, pooled, pn32)
        normed_all = gather(normed)

        q_pos = rank * seq_loc + jnp.arange(seq_loc)
        offset = q_pos[:, None] - img_pos[None, :]
        in_blk = (offset >= 0) & (offset < BLOCK)
        is_img = jnp.any(in_blk, axis=1)
        img_mask = is_img[:, None]
        flat_row = jnp.sum(jnp.where(in_blk, jnp.arange(n_img)[None, :] * BLOCK + offset, 0), axis=1)
        flat_row = jnp.where(is_img, flat_row, -1)
        select = (flat_row[:, None] == jnp.arange(n_img * BLOCK)[None, :]).astype(BF16)
        all_pos = jnp.arange(seq)
        all_off = all_pos[:, None] - img_pos[None, :]
        all_in = (all_off >= 0) & (all_off < BLOCK)
        limit = (all_pos + jnp.sum(jnp.where(all_in, BLOCK - 1 - all_off, 0), axis=1)).astype(jnp.int32).reshape(seq // BQ, 1, BQ)
        n_kb = (jnp.max(limit, axis=(1, 2)) // KB + 1).astype(jnp.int32)
        all_flat = jnp.sum(jnp.where(all_in, jnp.arange(n_img)[None, :] * BLOCK + all_off + 1, 0), axis=1) - 1
        select_all = (all_flat[:, None] == jnp.arange(n_img * BLOCK)[None, :]).astype(BF16)

        normed_rows = dot(select, normed_all).astype(BF16)
        soft_rows = dot(normed_rows, w_proj).astype(BF16)
        merged = jnp.where(img_mask, soft_rows, text_loc)
        hidden, pre_pull = jax.vjp(gain_norm, merged, pre32)
        hidden_all = gather(hidden)

        w_qkv = jnp.concatenate([
            lax.dynamic_slice_in_dim(w_query, rank * wq_loc, wq_loc, 1),
            lax.dynamic_slice_in_dim(w_key, rank * wk_loc, wk_loc, 1),
            lax.dynamic_slice_in_dim(w_value, rank * wk_loc, wk_loc, 1)], axis=1)
        raw = dot(hidden_all, w_qkv).astype(BF16)
        cos_t, sin_t = rope_tables(seq, hd)
        q, k, kt, vt = rope_fwd(raw, cos_t, sin_t, gq32, gk32, hd, n_q)
        rows_of = lambda x, c: x[c * BQ:(c + 1) * BQ]
        fwd = []
        for c in range(HALVES):
            fwd.append(attn_fwd(c, n_kb, limit, q, k, vt, hd, n_dev))
        y_parts, d_o, d_proj_parts, g_post = [], [], [], 0.0
        attn_t = []
        for c in range(HALVES):
            attn_t.append(exchange(fwd[c][0], attn_t[-1] if c else None))
        prev = attn_t[-1]
        for c in range(HALVES):
            attn_c = attn_t[c]
            if c:
                attn_c, _ = lax.optimization_barrier((attn_c, d_attn_t))
            proj_out = dot_tn(attn_c.reshape(n_dev * wq_loc, BQ), w_out).astype(BF16)
            y_part, post_pull = jax.vjp(post_residual, rows_of(merged, c), proj_out, post32)
            _, d_proj, g_post_part = post_pull(rows_of(grad_y, c))
            d_attn_t = dot_nt(w_out, d_proj).astype(BF16).reshape(n_dev, wq_loc, BQ)
            y_parts.append(y_part)
            g_post = g_post + g_post_part
            prev = exchange(d_attn_t, prev)
            d_o.append(prev)
            d_proj_parts.append(gather(d_proj))
        y_loc = jnp.concatenate(y_parts, axis=0)

        dq_halves, carried = [], []
        for c in range(HALVES):
            dq, *carried = attn_bwd(c, n_kb, limit, q, k, kt, raw, d_o[c], fwd[c][1], fwd[c][2], carried, hd, n_dev)
            dq_halves.append(dq)
        dk, dv = carried
        dv_all = gather(dv, 1)
        dq, dk, dq_t, g_q_gain, g_k_gain = rope_bwd(raw, dq_halves, dk, cos_t, sin_t, gq32, gk32, hd, n_q, seq_loc)
        dk_all = gather(dk, 1)
        dq_last = exchange(dq_t, prev)
        g_query = dot_tn(hidden_all, dq).astype(BF16)
        g_query = gather(g_query, 1)

        own_rows = lambda x: lax.dynamic_slice_in_dim(x, rank * seq_loc, seq_loc, 0)
        d_hidden = lax.dot_general(dq_last.reshape(-1, seq_loc), w_query, (((0,), (1,)), ((), ())), preferred_element_type=F32)
        d_hidden = d_hidden + dot_nt(own_rows(dv_all), w_value)
        d_hidden = (d_hidden + dot_nt(own_rows(dk_all), w_key)).astype(BF16)
        d_merged_attn, g_pre = pre_pull(d_hidden)
        d_merged = (grad_y.astype(F32) + d_merged_attn.astype(F32)).astype(BF16)
        grad_text = jnp.where(img_mask, 0.0, d_merged).astype(BF16)

        d_soft_rows = jnp.where(img_mask, d_merged, 0.0).astype(BF16)
        d_normed_rows = dot_nt(d_soft_rows, w_proj).astype(BF16)
        d_normed_all = dot_tn(select, d_normed_rows).astype(BF16)
        d_normed = reduce_to_owner(d_normed_all, rank)
        d_pooled, g_pn = norm_pull(d_normed)
        grad_vis = spread_rows((d_pooled.astype(F32) / (POOL * POOL)).astype(BF16)).reshape(img_loc, patches, dim_v)

        d_soft_t = exchange(d_soft_rows.T.reshape(n_dev, d_model // n_dev, seq_loc), dq_last)
        normed_pos = dot(select_all, normed_all).astype(BF16)
        g_proj = dot(d_soft_t.transpose(1, 0, 2).reshape(-1, seq), normed_pos).astype(BF16)
        g_proj = gather(g_proj)

        g_out = sum(dot_tn(fwd[c][0].transpose(0, 2, 1).reshape(-1, wq_loc), d_proj_parts[c]) for c in range(HALVES)).astype(BF16)
        g_out = gather(g_out)
        g_key = dot_tn(hidden_all, dk_all).astype(BF16)
        g_value = dot_tn(hidden_all, dv_all).astype(BF16)
        g_query = copy_rows(g_query)
        g_out = copy_rows(g_out)
        g_proj = transpose_rows(g_proj)
        small = lax.psum((g_pn, g_pre, g_q_gain[0], g_k_gain[0], g_post), 'cp')
        g_pn, g_pre, g_q_gain, g_k_gain, g_post = [part.astype(BF16) for part in small]
        return (y_loc, grad_text, grad_vis, g_pn, g_proj, g_pre, g_query, g_key, g_value, g_q_gain, g_k_gain, g_out, g_post)

    in_specs = (seq_spec, seq_spec, part_spec, seq_spec) + (rep_spec,) * 10
    out_specs = (seq_spec, seq_spec, seq_spec) + (part_spec,) * 10
    return jax.shard_map(device_step, mesh=mesh, in_specs=in_specs, out_specs=out_specs, check_vma=False)
```

```python
import functools
import math
import jax
import jax.numpy as jnp
from jax import lax
from jax.experimental import pallas as pl
from jax.experimental.pallas import tpu as pltpu
from jax.sharding import PartitionSpec as P

GRID = 64
POOL = 4
SIDE = GRID // POOL
BLOCK = SIDE * SIDE
EPS = 1e-6
ROPE_BASE = 1000000.0
ROPE_SCALE = 8.0
NEG_BIG = -1e30
F32 = jnp.float32
BF16 = jnp.bfloat16
LOG2E = math.log2(math.e)


def rms_scale(values, gain_vec):
    wide_vals = values.astype(F32)
    mean_sq = jnp.mean(wide_vals * wide_vals, axis=-1, keepdims=True)
    return wide_vals * lax.rsqrt(mean_sq + EPS) * (1.0 + gain_vec)


def gain_norm(values, gain_vec):
    return rms_scale(values, gain_vec).astype(BF16)


def post_residual(merged, proj_out, gain_vec):
    return (merged.astype(F32) + rms_scale(proj_out, gain_vec)).astype(BF16)


def dot(a, b):
    return jnp.dot(a, b, preferred_element_type=F32)


def dot_nt(a, b):
    return lax.dot_general(a, b, (((1,), (1,)), ((), ())), preferred_element_type=F32)


def dot_tn(a, b):
    return lax.dot_general(a, b, (((0,), (0,)), ((), ())), preferred_element_type=F32)


def rope_tables(seq, head_dim):
    inv_freq = ROPE_BASE ** (-jnp.arange(0, head_dim, 2).astype(F32) / head_dim)
    rot_angle = (jnp.arange(seq).astype(F32) / ROPE_SCALE)[:, None] * inv_freq[None, :]
    return jnp.cos(rot_angle), jnp.sin(rot_angle)


def rope_fwd_kernel(hd, raw_ref, cos_ref, sin_ref, gq_ref, gk_ref, q_ref, k_ref, kt_ref, vt_ref):
    cos, sin = cos_ref[...], sin_ref[...]
    half = hd // 2
    n_q = q_ref.shape[1] // hd

    def one(col, gain):
        x = raw_ref[:, col:col + hd].astype(F32)
        r = lax.rsqrt(jnp.mean(x * x, axis=-1, keepdims=True) + EPS)
        x = x * r * (1.0 + gain)
        a, b = x[:, :half], x[:, half:]
        return (a * cos - b * sin), (b * cos + a * sin)

    for h in range(n_q):
        a, b = one(h * hd, gq_ref[...])
        q_ref[:, h * hd:h * hd + half] = a.astype(BF16)
        q_ref[:, h * hd + half:(h + 1) * hd] = b.astype(BF16)
    a, b = one(n_q * hd, gk_ref[...])
    k_ref[:, :half] = a.astype(BF16)
    k_ref[:, half:] = b.astype(BF16)
    kt_ref[:half, :] = a.T.astype(BF16)
    kt_ref[half:, :] = b.T.astype(BF16)
    vt_ref[...] = raw_ref[:, (n_q + 1) * hd:].T


def rope_fwd(raw, cos, sin, gq, gk, hd, n_q):
    seq, width = raw.shape
    bm = 512
    row = lambda w: pl.BlockSpec((bm, w), lambda i: (i, 0))
    fix = pl.BlockSpec((1, hd), lambda i: (0, 0))
    return pl.pallas_call(
        functools.partial(rope_fwd_kernel, hd),
        grid=(seq // bm,),
        in_specs=[row(width), row(hd // 2), row(hd // 2), fix, fix],
        out_specs=[row(n_q * hd), row(hd), pl.BlockSpec((hd, bm), lambda i: (0, i)), pl.BlockSpec((hd, bm), lambda i: (0, i))],
        out_shape=[jax.ShapeDtypeStruct((seq, n_q * hd), BF16), jax.ShapeDtypeStruct((seq, hd), BF16)] + [jax.ShapeDtypeStruct((hd, seq), BF16)] * 2,
        cost_estimate=pl.CostEstimate(flops=20 * seq * width, bytes_accessed=4 * seq * width, transcendentals=0),
        name="rope_fwd",
    )(raw, cos, sin, gq, gk)


def rope_bwd_kernel(hd, raw_ref, dq0_ref, dq1_ref, dk_ref, dv_ref, cos_ref, sin_ref, gq_ref, gk_ref, out_ref, qt_ref, kt_ref, vt_ref, sq_ref, sk_ref):
    cos, sin = cos_ref[...], sin_ref[...]
    half = hd // 2
    n_q = dq0_ref.shape[1] // hd

    @pl.when(pl.program_id(0) == 0)
    def _():
        sq_ref[...] = jnp.zeros_like(sq_ref)
        sk_ref[...] = jnp.zeros_like(sk_ref)

    def load(refs, lo, hi):
        return jnp.concatenate([ref[:, lo:hi] for ref in refs], axis=0).astype(F32)

    def one(col, refs, dcol, gain, acc_ref, t_ref):
        da = load(refs, dcol, dcol + half)
        db = load(refs, dcol + half, dcol + hd)
        d = jnp.concatenate([da * cos + db * sin, db * cos - da * sin], axis=1)
        x = raw_ref[:, col:col + hd].astype(F32)
        r = lax.rsqrt(jnp.mean(x * x, axis=-1, keepdims=True) + EPS)
        xr = x * r
        acc_ref[...] += jnp.sum(d * xr, axis=0, keepdims=True)
        gd = d * (1.0 + gain)
        dx = r * (gd - xr * jnp.mean(xr * gd, axis=-1, keepdims=True))
        dx = dx.astype(BF16)
        out_ref[:, col:col + hd] = dx
        t_ref[0, dcol:dcol + hd, :] = dx.T

    for h in range(n_q):
        one(h * hd, (dq0_ref, dq1_ref), h * hd, gq_ref[...], sq_ref, qt_ref)
    one(n_q * hd, (dk_ref,), 0, gk_ref[...], sk_ref, kt_ref)
    out_ref[:, (n_q + 1) * hd:] = dv_ref[...]
    vt_ref[0] = dv_ref[...].T


def rope_bwd(raw, dq_halves, dk, dv, cos, sin, gq, gk, hd, n_q, bm):
    seq, width = raw.shape
    tall = lambda w: pl.BlockSpec((1, w, bm), lambda i: (i, 0, 0))
    tshape = lambda w: jax.ShapeDtypeStruct((seq // bm, w, bm), BF16)
    row = lambda w: pl.BlockSpec((bm, w), lambda i: (i, 0))
    fix = pl.BlockSpec((1, hd), lambda i: (0, 0))
    return pl.pallas_call(
        functools.partial(rope_bwd_kernel, hd),
        grid=(seq // bm,),
        in_specs=[row(width)] + [pl.BlockSpec((bm // 2, n_q * hd), lambda i: (i, 0))] * 2 + [row(hd), row(hd), row(hd // 2), row(hd // 2), fix, fix],
        out_specs=[row(width), tall(n_q * hd), tall(hd), tall(hd), fix, fix],
        out_shape=[jax.ShapeDtypeStruct((seq, width), BF16), tshape(n_q * hd), tshape(hd), tshape(hd), jax.ShapeDtypeStruct((1, hd), F32), jax.ShapeDtypeStruct((1, hd), F32)],
        cost_estimate=pl.CostEstimate(flops=30 * seq * width, bytes_accessed=6 * seq * width, transcendentals=0),
        name="rope_bwd",
    )(raw, *dq_halves, dk, dv, cos, sin, gq, gk)


BQ = 256
KB = 512
HALVES = 2


def stack_heads(blk, hd):
    return jnp.concatenate([blk[:, h * hd:(h + 1) * hd] for h in range(blk.shape[1] // hd)], axis=0)


def wide(blk, hd):
    return jnp.concatenate([blk[h * hd:(h + 1) * hd] for h in range(blk.shape[0] // hd)], axis=1)


def attn_fwd_kernel(hd, part, nkb_ref, lim_ref, q_ref, k_ref, vt_ref, o_ref, o32_ref, lse_ref, s_ref, p_ref, acc_ref):
    qb = HALVES * pl.program_id(0) + part
    coef = hd ** -0.5 * LOG2E
    n_q = q_ref.shape[1] // hd
    rows = n_q * BQ
    qt = stack_heads(q_ref[...], hd).T
    lim2 = jnp.concatenate([lim_ref[0]] * n_q, axis=1)
    n_full = (qb * BQ) // KB
    n_all = nkb_ref[qb]

    @pl.when(pl.program_id(0) == 0)
    def _():
        s_ref[:KB, :] = jnp.full((KB, rows), NEG_BIG, F32)

    def add_sum(m_prev, m, l, t):
        return l * jnp.exp2(m_prev - m) + jnp.sum(jnp.exp2(t.reshape(KB // 8, 8, rows) - m), axis=0)

    def body(masked, kb, stats):
        m_prev, m, l = stats
        pair = s_ref.at[pl.ds(pl.multiple_of(kb * KB, KB), 2 * KB)]
        l = add_sum(m_prev, m, l, pair[:KB])
        t = dot(k_ref[pl.ds(pl.multiple_of(kb * KB, KB), KB), :], qt) * coef
        if masked:
            key = kb * KB + lax.broadcasted_iota(jnp.int32, t.shape, 0)
            t = jnp.where(key <= lim2, t, NEG_BIG)
        pair[KB:] = t
        return m, jnp.maximum(m, jnp.max(t.reshape(KB // 8, 8, rows), axis=0)), l

    low = s_ref[:8, :]
    stats = lax.fori_loop(0, n_full, functools.partial(body, False), (low, low, jnp.zeros((8, rows), F32)))
    m_prev, m8, l8 = lax.fori_loop(n_full, n_all, functools.partial(body, True), stats)
    l8 = add_sum(m_prev, m8, l8, s_ref[pl.ds(pl.multiple_of(n_all * KB, KB), KB), :])
    m = jnp.max(m8, axis=0, keepdims=True)
    lse = m + jnp.log2(jnp.sum(l8 * jnp.exp2(m8 - m), axis=0, keepdims=True))

    def prob(kb):
        return jnp.exp2(s_ref[pl.ds(pl.multiple_of((kb + 1) * KB, KB), KB), :] - lse).astype(BF16)

    def pv(kb, p):
        return dot(vt_ref[:, pl.ds(pl.multiple_of(kb * KB, KB), KB)], p)

    p_ref[:KB] = prob(0)
    acc_ref[...] = jnp.zeros_like(acc_ref)

    def pv_body(kb, carry):
        pair = p_ref.at[pl.ds(pl.multiple_of((kb - 1) * KB, KB), 2 * KB)]
        acc_ref[...] += pv(kb - 1, pair[:KB])
        pair[KB:] = prob(kb)
        return carry

    lax.fori_loop(1, n_all, pv_body, 0)
    acc = acc_ref[...] + pv(n_all - 1, p_ref[pl.ds(pl.multiple_of((n_all - 1) * KB, KB), KB), :])
    for h in range(n_q):
        part = acc[:, h * BQ:(h + 1) * BQ]
        o32_ref[0, h * hd:(h + 1) * hd, :] = part
        o_ref[0, h * hd:(h + 1) * hd, :] = part.astype(BF16)
    lse_ref[0] = jnp.broadcast_to(lse, (8, rows))


def attn_fwd(part, nkb, lim, q, k, vt, hd, n_dev):
    seq, width = q.shape
    n_q = width // hd
    tall = pl.BlockSpec((1, width, BQ), lambda i, *_: (i, 0, 0))
    at = lambda i, *_: HALVES * i + part
    return pl.pallas_call(
        functools.partial(attn_fwd_kernel, hd, part),
        grid_spec=pltpu.PrefetchScalarGridSpec(
            num_scalar_prefetch=1,
            grid=(n_dev,),
            in_specs=[pl.BlockSpec((1, 1, BQ), lambda i, *_: (at(i), 0, 0)), pl.BlockSpec((BQ, width), lambda i, *_: (at(i), 0)),
                      pl.BlockSpec((seq, hd), lambda i, *_: (0, 0)), pl.BlockSpec((hd, seq), lambda i, *_: (0, 0))],
            out_specs=[tall, tall, pl.BlockSpec((1, 8, n_q * BQ), lambda i, *_: (i, 0, 0))],
            scratch_shapes=[pltpu.VMEM((seq + KB, n_q * BQ), F32), pltpu.VMEM((seq, n_q * BQ), BF16), pltpu.VMEM((hd, n_q * BQ), F32)]),
        out_shape=[jax.ShapeDtypeStruct((n_dev, width, BQ), BF16), jax.ShapeDtypeStruct((n_dev, width, BQ), F32),
                   jax.ShapeDtypeStruct((n_dev, 8, n_q * BQ), F32)],
        cost_estimate=pl.CostEstimate(flops=int(1.1 * seq * seq * width), bytes_accessed=4 * seq * width, transcendentals=seq * seq),
        compiler_params=pltpu.CompilerParams(vmem_limit_bytes=40 * 1024 * 1024),
        name="attn_fwd",
    )(nkb, lim, q, k, vt)


def attn_bwd_kernel(hd, part, nkb_ref, lim_ref, q_ref, k_ref, kt_ref, v_ref, do_ref, o32_ref, lse_ref, *refs):
    step = pl.program_id(0)
    qb = HALVES * step + part
    scale = hd ** -0.5
    coef = scale * LOG2E
    n_q = q_ref.shape[1] // hd
    rows = n_q * BQ
    first, last = part == 0, part == HALVES - 1
    if not first:
        dk_in, dv_in, *refs = refs
    dq_ref, dk_ref, dv_ref, *refs = refs
    dk_acc, dv_acc = refs if last else (dk_ref, dv_ref)

    @pl.when(step == 0)
    def _():
        dk_acc[...] = jnp.zeros_like(dk_acc) if first else dk_in[...]
        dv_acc[...] = jnp.zeros_like(dv_acc) if first else dv_in[...]

    q2 = stack_heads(q_ref[...], hd)
    qt = q2.T
    dot_ = wide(do_ref[0], hd)
    do2 = dot_.T
    delta = jnp.sum(dot_.astype(F32) * wide(o32_ref[0], hd), axis=0, keepdims=True)
    lse = lse_ref[0][0:1, :]
    lim2 = jnp.concatenate([lim_ref[0]] * n_q, axis=1)
    n_full = (qb * BQ) // KB
    n_all = nkb_ref[qb]

    def body(masked, kb, dqt):
        keys = pl.ds(pl.multiple_of(kb * KB, KB), KB)
        st = dot(k_ref[keys, :], qt)
        pt = jnp.exp2(st * coef - lse)
        if masked:
            key = kb * KB + lax.broadcasted_iota(jnp.int32, st.shape, 0)
            pt = jnp.where(key <= lim2, pt, 0.0)
        dpt = dot(v_ref[keys, :], dot_)
        dst = (pt * (dpt - delta)).astype(BF16)
        dv_acc[keys, :] += dot(pt.astype(BF16), do2)
        dk_acc[keys, :] += dot(dst, q2)
        return dqt + dot(kt_ref[:, keys], dst)

    dqt = lax.fori_loop(0, n_full, functools.partial(body, False), jnp.zeros((hd, rows), F32))
    dqt = lax.fori_loop(n_full, n_all, functools.partial(body, True), dqt)
    dq = (dqt * scale).T.astype(BF16)
    for h in range(n_q):
        dq_ref[:, h * hd:(h + 1) * hd] = dq[h * BQ:(h + 1) * BQ]

    if last:
        @pl.when(step == pl.num_programs(0) - 1)
        def _():
            dk_ref[...] = (dk_acc[...] * scale).astype(BF16)
            dv_ref[...] = dv_acc[...].astype(BF16)


def attn_bwd(part, nkb, lim, q, k, kt, raw, d_o, o32, lse, carried, hd, n_dev):
    seq, width = q.shape
    n_q = width // hd
    v_col = raw.shape[1] // hd - 1
    at = lambda i, *_: HALVES * i + part
    tall = pl.BlockSpec((1, width, BQ), lambda i, *_: (i, 0, 0))
    whole = pl.BlockSpec((seq, hd), lambda i, *_: (0, 0))
    last = part == HALVES - 1
    acc_type = BF16 if last else F32
    return pl.pallas_call(
        functools.partial(attn_bwd_kernel, hd, part),
        grid_spec=pltpu.PrefetchScalarGridSpec(
            num_scalar_prefetch=1,
            grid=(n_dev,),
            in_specs=[pl.BlockSpec((1, 1, BQ), lambda i, *_: (at(i), 0, 0)), pl.BlockSpec((BQ, width), lambda i, *_: (at(i), 0)), whole,
                      pl.BlockSpec((hd, seq), lambda i, *_: (0, 0)), pl.BlockSpec((seq, hd), lambda i, *_: (0, v_col)), tall, tall,
                      pl.BlockSpec((1, 8, n_q * BQ), lambda i, *_: (i, 0, 0))] + [whole] * len(carried),
            out_specs=[pl.BlockSpec((BQ, width), lambda i, *_: (i, 0)), whole, whole],
            scratch_shapes=[pltpu.VMEM((seq, hd), F32)] * 2 if last else []),
        out_shape=[jax.ShapeDtypeStruct((n_dev * BQ, width), BF16), jax.ShapeDtypeStruct((seq, hd), acc_type), jax.ShapeDtypeStruct((seq, hd), acc_type)],
        cost_estimate=pl.CostEstimate(flops=int(2.7 * seq * seq * width), bytes_accessed=6 * seq * width, transcendentals=seq * seq),
        compiler_params=pltpu.CompilerParams(vmem_limit_bytes=56 * 1024 * 1024),
        name="attn_bwd",
    )(nkb, lim, q, k, kt, raw, d_o, o32, lse, *carried)


def split_kernel(n_dev, x_ref, *o_refs):
    width = x_ref.shape[1] // n_dev
    for g in range(n_dev):
        col = g * width
        for o_ref in o_refs:
            w = o_ref.shape[1] // n_dev
            o_ref[:, g * w:(g + 1) * w] = x_ref[:, col:col + w]
            col += w


def copy_kernel(x_ref, o_ref):
    o_ref[...] = x_ref[...]


def transpose_kernel(x_ref, o_ref):
    o_ref[...] = x_ref[...].T


def stream(body, x, in_spec, shapes, out_specs, grid):
    return pl.pallas_call(
        body,
        grid=(grid,),
        in_specs=[in_spec],
        out_specs=out_specs,
        out_shape=[jax.ShapeDtypeStruct(shape, x.dtype) for shape in shapes],
        cost_estimate=pl.CostEstimate(flops=x.size, bytes_accessed=4 * x.size, transcendentals=0),
        compiler_params=pltpu.CompilerParams(vmem_limit_bytes=60 * 1024 * 1024),
        name="copy_out",
    )(x)


def split_cols(x, n_dev, widths):
    bm = 256
    row = lambda w: pl.BlockSpec((bm, w), lambda i: (i, 0))
    return stream(functools.partial(split_kernel, n_dev), x, row(x.shape[1]), [(x.shape[0], w) for w in widths], [row(w) for w in widths], x.shape[0] // bm)


def copy_rows(x):
    spec = pl.BlockSpec((512, x.shape[1]), lambda i: (i, 0))
    return stream(copy_kernel, x, spec, [x.shape], [spec], x.shape[0] // 512)[0]


def spread_kernel(x_ref, o_ref):
    cell, col = (lax.broadcasted_iota(jnp.int32, (GRID, SIDE), d) for d in (0, 1))
    y = dot((cell // POOL == col).astype(BF16), x_ref[...]).astype(BF16)
    for t in range(POOL):
        o_ref[t * GRID:(t + 1) * GRID, :] = y


def spread_rows(x):
    cols = x.shape[1]
    step = GRID * POOL
    n = x.shape[0] // SIDE
    return stream(spread_kernel, x, pl.BlockSpec((SIDE, cols), lambda i: (i, 0)), [(n * step, cols)], [pl.BlockSpec((step, cols), lambda i: (i, 0))], n)[0]


def transpose_rows(x):
    rows, cols = x.shape
    return stream(transpose_kernel, x, pl.BlockSpec((512, cols), lambda i: (i, 0)), [(cols, rows)], [pl.BlockSpec((cols, 512), lambda i: (0, i))], rows // 512)[0]


def solution(mesh):
    n_dev = mesh.shape['cp']
    seq_spec = P(('dp', 'cp'))
    part_spec = P('dp')
    rep_spec = P()

    def gather(x, axis=0):
        return lax.all_gather(x, 'cp', axis=axis, tiled=True)

    def exchange(x, after=None):
        if after is not None:
            x, _ = lax.optimization_barrier((x, after))
        return lax.all_to_all(x, 'cp', split_axis=0, concat_axis=0, tiled=True)

    def reduce_to_owner(x, rank):
        bits = [rank // 4, (rank // 2) % 2, rank % 2]

        def halve(x, dim, bit):
            pick = lambda b: lax.dynamic_index_in_dim(x, b, dim, keepdims=False)
            got = lax.ppermute(pick(1 - bits[bit]), 'cp', [(i, i ^ (4 >> bit)) for i in range(n_dev)])
            return pick(bits[bit]) + got

        rows, cols = x.shape[0] // n_dev, x.shape[1]
        x = halve(x.reshape(2, 2, 2, rows, cols), 2, 2)
        cut = cols // 256 * 128
        first = halve(halve(x[..., :cut], 1, 1), 0, 0)
        second = halve(halve(x[..., cut:], 0, 0), 0, 1)
        return jnp.concatenate([first, second], axis=-1)

    def device_step(vis_loc, text_loc, img_pos, grad_y, pn_gain, w_proj, pre_gain, w_query, w_key, w_value, q_gain, k_gain, w_out, post_gain):
        rank = lax.axis_index('cp')
        seq_loc, d_model = text_loc.shape
        seq = seq_loc * n_dev
        img_loc, patches, dim_v = vis_loc.shape
        n_img = img_pos.shape[0]
        hd = q_gain.shape[0]
        wq_loc = w_query.shape[1] // n_dev
        wk_loc = w_key.shape[1] // n_dev
        n_q = wq_loc // hd
        pn32, pre32, post32 = pn_gain.astype(F32), pre_gain.astype(F32), post_gain.astype(F32)
        gq32 = q_gain.astype(F32)[None, :]
        gk32 = k_gain.astype(F32)[None, :]

        patch = jnp.arange(patches)
        patch_cell = (patch // (GRID * POOL)) * SIDE + (patch % GRID) // POOL
        pool_mat = (jnp.arange(BLOCK)[:, None] == patch_cell[None, :]).astype(BF16)
        pooled = jnp.einsum('cp,npd->ncd', pool_mat, vis_loc, preferred_element_type=F32) / (POOL * POOL)
        pooled = pooled.astype(BF16).reshape(img_loc * BLOCK, dim_v)
        normed, norm_pull = jax.vjp(gain_norm, pooled, pn32)
        normed_all = gather(normed)

        q_pos = rank * seq_loc + jnp.arange(seq_loc)
        offset = q_pos[:, None] - img_pos[None, :]
        in_blk = (offset >= 0) & (offset < BLOCK)
        is_img = jnp.any(in_blk, axis=1)
        img_mask = is_img[:, None]
        flat_row = jnp.sum(jnp.where(in_blk, jnp.arange(n_img)[None, :] * BLOCK + offset, 0), axis=1)
        flat_row = jnp.where(is_img, flat_row, -1)
        select = (flat_row[:, None] == jnp.arange(n_img * BLOCK)[None, :]).astype(BF16)
        all_pos = jnp.arange(seq)
        all_off = all_pos[:, None] - img_pos[None, :]
        all_in = (all_off >= 0) & (all_off < BLOCK)
        limit = (all_pos + jnp.sum(jnp.where(all_in, BLOCK - 1 - all_off, 0), axis=1)).astype(jnp.int32).reshape(seq // BQ, 1, BQ)
        n_kb = (jnp.max(limit, axis=(1, 2)) // KB + 1).astype(jnp.int32)
        all_flat = jnp.sum(jnp.where(all_in, jnp.arange(n_img)[None, :] * BLOCK + all_off + 1, 0), axis=1) - 1
        select_all = (all_flat[:, None] == jnp.arange(n_img * BLOCK)[None, :]).astype(BF16)

        normed_rows = dot(select, normed_all).astype(BF16)
        soft_rows = dot(normed_rows, w_proj).astype(BF16)
        merged = jnp.where(img_mask, soft_rows, text_loc)
        hidden, pre_pull = jax.vjp(gain_norm, merged, pre32)
        hidden_all = gather(hidden)

        w_qkv = jnp.concatenate([
            lax.dynamic_slice_in_dim(w_query, rank * wq_loc, wq_loc, 1),
            lax.dynamic_slice_in_dim(w_key, rank * wk_loc, wk_loc, 1),
            lax.dynamic_slice_in_dim(w_value, rank * wk_loc, wk_loc, 1)], axis=1)
        raw = dot(hidden_all, w_qkv).astype(BF16)
        cos_t, sin_t = rope_tables(seq, hd)
        q, k, kt, vt = rope_fwd(raw, cos_t, sin_t, gq32, gk32, hd, n_q)
        rows_of = lambda x, c: x[c * BQ:(c + 1) * BQ]
        fwd = []
        for c in range(HALVES):
            fwd.append(attn_fwd(c, n_kb, limit, q, k, vt, hd, n_dev))
        y_parts, d_o, d_proj_parts, g_post = [], [], [], 0.0
        attn_t = []
        for c in range(HALVES):
            attn_t.append(exchange(fwd[c][0], attn_t[-1] if c else None))
        prev = attn_t[-1]
        for c in range(HALVES):
            attn_c = attn_t[c]
            if c:
                attn_c, _ = lax.optimization_barrier((attn_c, d_attn_t))
            proj_out = dot_tn(attn_c.reshape(n_dev * wq_loc, BQ), w_out).astype(BF16)
            y_part, post_pull = jax.vjp(post_residual, rows_of(merged, c), proj_out, post32)
            _, d_proj, g_post_part = post_pull(rows_of(grad_y, c))
            d_attn_t = dot_nt(w_out, d_proj).astype(BF16).reshape(n_dev, wq_loc, BQ)
            y_parts.append(y_part)
            g_post = g_post + g_post_part
            prev = exchange(d_attn_t, prev)
            d_o.append(prev)
            d_proj_parts.append(gather(d_proj))
        y_loc = jnp.concatenate(y_parts, axis=0)

        dq_halves, carried = [], []
        for c in range(HALVES):
            dq, *carried = attn_bwd(c, n_kb, limit, q, k, kt, raw, d_o[c], fwd[c][1], fwd[c][2], carried, hd, n_dev)
            dq_halves.append(dq)
        dk, dv = carried
        d_qkv, dq_t, dk_t, dv_t, g_q_gain, g_k_gain = rope_bwd(raw, dq_halves, dk, dv, cos_t, sin_t, gq32, gk32, hd, n_q, seq_loc)

        g_qkv = dot_tn(hidden_all, d_qkv).astype(BF16)
        g_qkv = gather(g_qkv, 1)

        dq_seq = exchange(dq_t, prev)
        dk_seq = exchange(dk_t, dq_seq)
        dv_last = exchange(dv_t, dk_seq)
        dq_seq, dk_seq, dv_seq = [x.reshape(-1, seq_loc) for x in (dq_seq, dk_seq, dv_last)]
        d_hidden = sum(lax.dot_general(d, w, (((0,), (1,)), ((), ())), preferred_element_type=F32)
                       for d, w in ((dq_seq, w_query), (dk_seq, w_key), (dv_seq, w_value))).astype(BF16)
        d_merged_attn, g_pre = pre_pull(d_hidden)
        d_merged = (grad_y.astype(F32) + d_merged_attn.astype(F32)).astype(BF16)
        grad_text = jnp.where(img_mask, 0.0, d_merged).astype(BF16)

        d_soft_rows = jnp.where(img_mask, d_merged, 0.0).astype(BF16)
        d_normed_rows = dot_nt(d_soft_rows, w_proj).astype(BF16)
        d_normed_all = dot_tn(select, d_normed_rows).astype(BF16)
        d_normed = reduce_to_owner(d_normed_all, rank)
        d_pooled, g_pn = norm_pull(d_normed)
        grad_vis = spread_rows((d_pooled.astype(F32) / (POOL * POOL)).astype(BF16)).reshape(img_loc, patches, dim_v)

        d_soft_t = exchange(d_soft_rows.T.reshape(n_dev, d_model // n_dev, seq_loc), dv_last)
        normed_pos = dot(select_all, normed_all).astype(BF16).reshape(n_dev, seq_loc, dim_v)
        g_proj = sum(dot(d_soft_t[i], normed_pos[i]) for i in range(n_dev)).astype(BF16)
        g_proj = gather(g_proj)

        g_out = sum(dot_tn(fwd[c][0].transpose(0, 2, 1).reshape(-1, wq_loc), d_proj_parts[c]) for c in range(HALVES)).astype(BF16)
        g_out = gather(g_out)
        g_query, g_key, g_value = split_cols(g_qkv, n_dev, (n_dev * wq_loc, n_dev * wk_loc, n_dev * wk_loc))
        g_out = copy_rows(g_out)
        g_proj = transpose_rows(g_proj)
        small = lax.psum((g_pn, g_pre, g_q_gain[0], g_k_gain[0], g_post), 'cp')
        g_pn, g_pre, g_q_gain, g_k_gain, g_post = [part.astype(BF16) for part in small]
        return (y_loc, grad_text, grad_vis, g_pn, g_proj, g_pre, g_query, g_key, g_value, g_q_gain, g_k_gain, g_out, g_post)

    in_specs = (seq_spec, seq_spec, part_spec, seq_spec) + (rep_spec,) * 10
    out_specs = (seq_spec, seq_spec, seq_spec) + (part_spec,) * 10
    return jax.shard_map(device_step, mesh=mesh, in_specs=in_specs, out_specs=out_specs, check_vma=False)
```
